16 devices in a mesh: rep: 2 (over z), nodes: 8 (over y, x, core).
Axes of the slice: x: 2, y: 2, z: 2, core: 2. Of those that a mesh axis runs over, the one named last changes fastest.
Arguments:
- adjacency: bfloat16 [16384, 16384], P('nodes')
- features: bfloat16 [16384, 100], P(('nodes', 'rep'))
- w_one: float32 [100, 256], replicated
- w_two: float32 [256, 47], replicated
- labels: int32 [16384], P(('nodes', 'rep'))
- label_mask: int32 [16384], P(('nodes', 'rep'))
Outputs:
- output 1: float32 [], replicated
- output 2: float32 [100, 256], replicated
- output 3: float32 [256, 47], replicated
All inputs are finite; a program needn't handle non-finite values.
Results may differ from the reference program's by a relative error of at most 0.001.
Values are sent between devices in bfloat16 or wider.
A program may use at most 1 GiB of HBM per device.

```python
import jax
import jax.numpy as jnp
from jax import lax

NUM_NODES = 16384
F_IN = 100
HIDDEN = 256
CLASSES = 47
ROW_BLOCK = 2048
NUM_BLOCKS = NUM_NODES // ROW_BLOCK


def draw_graph(graph_key):
    comm_key, act_key, edge_key = jax.random.split(graph_key, 3)
    community = jax.random.randint(comm_key, (NUM_NODES,), 0, 8)
    activity = jax.random.randint(act_key, (NUM_NODES,), 1, 5)
    node_ids = jnp.arange(NUM_NODES)

    def adj_block(block_index):
        row_start = block_index * ROW_BLOCK
        row_comm = lax.dynamic_slice(community, (row_start,), (ROW_BLOCK,))
        row_act = lax.dynamic_slice(activity, (row_start,), (ROW_BLOCK,))
        edge_draw = jax.random.randint(jax.random.fold_in(edge_key, block_index), (ROW_BLOCK, NUM_NODES), 0, 1000)
        threshold = jnp.where(row_comm[:, None] == community[None, :], 400, 60) * row_act[:, None] // 4
        self_loop = (row_start + jnp.arange(ROW_BLOCK))[:, None] == node_ids[None, :]
        edge_weight = jnp.logical_or(edge_draw < threshold, self_loop).astype(jnp.float32)
        return (edge_weight / jnp.sum(edge_weight, axis=1, keepdims=True)).astype(jnp.bfloat16)

    adjacency = lax.map(adj_block, jnp.arange(NUM_BLOCKS)).reshape(NUM_NODES, NUM_NODES)
    return adjacency, community


def draw_labels(label_key, mask_key):
    labels = jax.random.randint(label_key, (NUM_NODES,), 0, CLASSES)
    mask_draw = (jax.random.randint(mask_key, (NUM_NODES,), 0, 10) < 3).astype(jnp.int32)
    label_mask = jnp.where(jnp.arange(NUM_NODES) == 0, 1, mask_draw).astype(jnp.int32)
    return labels, label_mask


def setup_inputs(seed: int = 0) -> dict:
    root_key = jax.random.key(seed)
    graph_key, mean_key, noise_key, one_key, two_key, label_key, mask_key = jax.random.split(root_key, 7)
    adjacency, community = draw_graph(graph_key)
    comm_mean = jax.random.normal(mean_key, (8, F_IN), jnp.float32)
    feat_noise = jax.random.normal(noise_key, (NUM_NODES, F_IN), jnp.float32)
    features = (comm_mean[community] + feat_noise).astype(jnp.bfloat16)
    w_one = jax.random.normal(one_key, (F_IN, HIDDEN), jnp.float32) * F_IN ** -0.5
    w_two = jax.random.normal(two_key, (HIDDEN, CLASSES), jnp.float32) * HIDDEN ** -0.5
    labels, label_mask = draw_labels(label_key, mask_key)
    return {"adjacency": adjacency, "features": features, "w_one": w_one, "w_two": w_two, "labels": labels, "label_mask": label_mask}


def reference(adjacency, features, w_one, w_two, labels, label_mask):
    adj_blocks = adjacency.reshape(NUM_BLOCKS, ROW_BLOCK, NUM_NODES)

    def aggregate(values):
        def one_block(adj_blk):
            return jnp.dot(adj_blk, values, preferred_element_type=jnp.float32)
        return lax.map(one_block, adj_blocks).reshape(NUM_NODES, values.shape[1])

    def aggregate_t(grad_rows):
        grad_blocks = grad_rows.reshape(NUM_BLOCKS, ROW_BLOCK, grad_rows.shape[1])

        def body(acc, pair):
            adj_blk, grad_blk = pair
            contrib = lax.dot_general(adj_blk, grad_blk, (((0,), (0,)), ((), ())), preferred_element_type=jnp.float32)
            return acc + contrib, None

        init = jnp.zeros((NUM_NODES, grad_rows.shape[1]), jnp.float32)
        return lax.scan(body, init, (adj_blocks, grad_blocks))[0]

    w_one_b = w_one.astype(jnp.bfloat16)
    w_two_b = w_two.astype(jnp.bfloat16)
    y_one = jnp.dot(features, w_one_b, preferred_element_type=jnp.float32).astype(jnp.bfloat16)
    z_one = aggregate(y_one)
    h_one = jnp.maximum(z_one, 0.0).astype(jnp.bfloat16)
    y_two = jnp.dot(h_one, w_two_b, preferred_element_type=jnp.float32).astype(jnp.bfloat16)
    z_two = aggregate(y_two)
    log_probs = jax.nn.log_softmax(z_two, axis=-1)
    onehot = (labels[:, None] == jnp.arange(CLASSES)[None, :]).astype(jnp.float32)
    mask_f = label_mask.astype(jnp.float32)
    label_count = jnp.sum(mask_f)
    loss_value = -jnp.sum(mask_f * jnp.sum(onehot * log_probs, axis=-1)) / label_count
    g_two = ((jnp.exp(log_probs) - onehot) * (mask_f / label_count)[:, None]).astype(jnp.bfloat16)
    dy_two = aggregate_t(g_two).astype(jnp.bfloat16)
    dw_two = lax.dot_general(h_one, dy_two, (((0,), (0,)), ((), ())), preferred_element_type=jnp.float32)
    dh_one = jnp.dot(dy_two, w_two_b.T, preferred_element_type=jnp.float32)
    g_one = jnp.where(z_one > 0, dh_one, 0.0).astype(jnp.bfloat16)
    dy_one = aggregate_t(g_one).astype(jnp.bfloat16)
    dw_one = lax.dot_general(features, dy_one, (((0,), (0,)), ((), ())), preferred_element_type=jnp.float32)
    return (loss_value, dw_one, dw_two)
```

```python
import functools

import jax
import jax.numpy as jnp
from jax import lax
from jax.experimental import pallas as pl
from jax.experimental.pallas import tpu as pltpu
from jax.sharding import PartitionSpec as P

BF16 = jnp.bfloat16
F32 = jnp.float32

POS = {0: 0, 1: 1, 2: 2, 4: 3, 3: 4, 5: 5, 6: 6, 7: 7}
ORDERS = ((1, 2, 4), (2, 4, 1), (4, 1, 2))


def dot(a, b, dims=((1,), (0,))):
    return lax.dot_general(a, b, (dims, ((), ())), preferred_element_type=F32)


def step_kernel(nb, classes, f_in, cpad,
                a_hbm, x_hbm, w1_ref, w2_ref, w2t_ref, lab_ref, msk_ref,
                o1_ref, o2_ref,
                abuf, xg, y1, cnt, z1, h1t, y2g, z2, g2,
                p2out, p2sib, p2sum, p2rcv, d2, g1,
                p6out, p6sib, p6sum, r6f, r6x, r6y, d1,
                part1, part2, rb1, rb2, res1, res2,
                asem, xsem, ssem, rsem):
    r = lax.axis_index("rep")
    n = lax.axis_index("nodes")
    core = n % 2
    xc = (n // 2) % 2
    yc = n // 4
    hid = z1.shape[1]

    def flip(v, f):
        return 1 - v if f else v

    def coords(k, dc):
        rr = flip(r, k // 4)
        nn = flip(yc, (k // 2) % 2) * 4 + flip(xc, k % 2) * 2 + flip(core, dc)
        return rr, nn

    def block_id(k, dc):
        rr, nn = coords(k, dc)
        return nn * 2 + rr

    sent = []

    def send(src, dst, k, dc):
        i = len(sent)
        cp = pltpu.make_async_remote_copy(
            src_ref=src, dst_ref=dst, send_sem=ssem.at[i], recv_sem=rsem.at[i],
            device_id=coords(k, dc), device_id_type=pl.DeviceIdType.MESH)
        cp.start()
        sent.append(cp)
        return cp

    peers = [(k, dc) for k in range(8) for dc in range(2) if (k, dc) != (0, 0)]

    xload = pltpu.make_async_copy(x_hbm, xg.at[0], xsem)
    xload.start()
    loads = {}
    for k in POS:
        for dc in range(2):
            slot = POS[k] * 2 + dc
            col = pl.multiple_of(block_id(k, dc) * nb, nb)
            row = pl.multiple_of(r * nb, nb)
            cp = pltpu.make_async_copy(a_hbm.at[pl.ds(row, nb), pl.ds(col, nb)], abuf.at[slot], asem.at[slot])
            cp.start()
            loads[slot] = cp
    barrier = pltpu.get_barrier_semaphore()
    for k, dc in peers:
        pl.semaphore_signal(barrier, inc=1, device_id=coords(k, dc), device_id_type=pl.DeviceIdType.MESH)
    cnt[...] = jnp.zeros_like(cnt)
    z1[...] = jnp.zeros_like(z1)
    z2[...] = jnp.zeros_like(z2)
    pl.semaphore_wait(barrier, len(peers))
    xload.wait()

    def gather(buf, cuts, consume):
        def at(k, dc):
            return buf.at[POS[k] * 2 + dc]

        def piece(k, p):
            return buf.at[POS[k] * 2, pl.ds(cuts[p], cuts[p + 1] - cuts[p])]

        near = {k: send(at(0, 0), at(k, 0), k, 0) for k in (1, 2, 4)}
        sib = {0: send(at(0, 0), at(0, 1), 0, 1)}
        sib[0].wait_recv()
        consume(0, 2)
        two = {}
        for k in (1, 2, 4):
            near[k].wait_recv()
            for p, (d0, d1_, d2_) in enumerate(ORDERS):
                if k == d0:
                    two[(d0 + d1_, p)] = send(piece(d0, p), piece(d0 + d1_, p), d1_, 0)
                    two[(d0 + d2_, p)] = send(piece(d0, p), piece(d0 + d2_, p), d2_, 0)
                if k == d1_:
                    two[(d1_ + d2_, p)] = send(piece(d1_, p), piece(d1_ + d2_, p), d2_, 0)
            sib[k] = send(at(k, 0), at(k, 1), 0, 1)
        for k in (1, 2, 4):
            sib[k].wait_recv()
        consume(2, 8)
        three = []
        for k in (3, 6, 5):
            for p, (d0, d1_, d2_) in enumerate(ORDERS):
                two[(k, p)].wait_recv()
                if k == d0 + d1_:
                    three.append(send(piece(k, p), piece(7, p), d2_, 0))
            sib[k] = send(at(k, 0), at(k, 1), 0, 1)
        for k in (3, 6, 5):
            sib[k].wait_recv()
        consume(8, 14)
        for cp in three:
            cp.wait_recv()
        sib[7] = send(at(7, 0), at(7, 1), 0, 1)
        sib[7].wait_recv()
        consume(14, 16)

    ones = jnp.ones((16, nb), BF16)
    mrows = 256

    def z1_blocks(lo, hi):
        for s in range(lo, hi):
            loads[s].wait()

        @pl.loop(lo, hi)
        def _(s):
            xb = xg[s]
            cnt[...] += dot(ones, xb)
            y1[...] = dot(xb, w1_ref[...]).astype(BF16)
            yv = y1[...]
            for m in range(0, nb, mrows):
                z1[m:m + mrows, :] += dot(abuf[s, m:m + mrows, :], yv)

    third = (nb // 48) * 16
    gather(xg, (0, nb - 2 * third, nb - third, nb), z1_blocks)

    for m in range(0, nb, mrows):
        h1t[0, :, m:m + mrows] = jnp.maximum(z1[m:m + mrows, :], 0.0).T.astype(BF16)
    y2g[0] = dot(w2t_ref[...], h1t[0]).astype(BF16)

    reload = {}

    def z2_blocks(lo, hi):
        @pl.loop(lo, hi)
        def _(s):
            for m in range(0, nb, mrows):
                z2[m:m + mrows, 0:cpad] += dot(abuf[s, m:m + mrows, :], y2g[s], ((1,), (1,)))

        for k in range(4, 8):
            for dc in range(2):
                slot = POS[k] * 2 + dc
                if lo <= slot < hi:
                    col = pl.multiple_of(block_id(k - 4, dc) * nb, nb)
                    row = pl.multiple_of((1 - r) * nb, nb)
                    cp = pltpu.make_async_copy(a_hbm.at[pl.ds(row, nb), pl.ds(col, nb)], abuf.at[slot], asem.at[slot])
                    cp.start()
                    reload[slot] = cp

    third = cpad // 3
    gather(y2g, (0, third, 2 * third, cpad), z2_blocks)
    h1t_cp = send(h1t.at[0], h1t.at[1], 4, 0)

    z2t = z2[...].T[0:cpad, :]
    cls = lax.broadcasted_iota(jnp.int32, (cpad, nb), 0)
    zm = jnp.where(cls < classes, z2t, -jnp.inf)
    zs = zm - jnp.max(zm, axis=0, keepdims=True)
    logp = zs - jnp.log(jnp.sum(jnp.exp(zs), axis=0, keepdims=True))
    hot = cls == lab_ref[...]
    mask_f = msk_ref[...].astype(F32)
    total_m = cnt[0:1, f_in:f_in + 1]
    loss_v = -mask_f * jnp.sum(jnp.where(hot, logp, 0.0), axis=0, keepdims=True)
    loss_part = jnp.sum(loss_v, axis=1, keepdims=True) / total_m
    g2[0] = ((jnp.exp(logp) - hot.astype(F32)) * (mask_f / total_m)).astype(BF16)
    g2_cp = send(g2.at[0], g2.at[1], 4, 0)
    g2_cp.wait_recv()
    for s in reload:
        reload[s].wait()

    order = (3, 1, 2, 0)
    sib2, rcv2 = {}, {}

    def fin2(q):
        sib2[q].wait_recv()
        p2sum[q] += p2sib[q]
        if q:
            rcv2[q] = send(p2sum.at[q], p2rcv.at[q - 1], q, 0)

    def part2_of(q, dc):
        s, sp = POS[q] * 2 + dc, POS[q + 4] * 2 + dc
        return dot(g2[0], abuf[s]) + dot(g2[1], abuf[sp])

    for i, q in enumerate(order):
        p2out[q] = part2_of(q, 1)
        sib2[q] = send(p2out.at[q], p2sib.at[q], 0, 1)
        p2sum[q] = part2_of(q, 0)
        if i:
            fin2(order[i - 1])
    fin2(0)
    for q in (1, 2, 3):
        rcv2[q].wait_recv()
    d2[0] = (p2sum[0] + p2rcv[0] + p2rcv[1] + p2rcv[2]).astype(BF16)
    d2_cp = send(d2.at[0], d2.at[1], 4, 0)

    rows = hid // 16

    def reduce_start(part, rb):
        return [send(part.at[pl.ds(pl.multiple_of(block_id(k, dc) * rows, rows), rows)], rb.at[i], k, dc)
                for i, (k, dc) in enumerate(peers)]

    def reduce_mid(part, rb, res, cps):
        own = pl.ds(pl.multiple_of(block_id(0, 0) * rows, rows), rows)
        acc = part[own, :]
        for i, cp in enumerate(cps):
            cp.wait_recv()
            acc = acc + rb[i]
        res[own, :] = acc
        return [send(res.at[own], res.at[own], k, dc) for k, dc in peers]

    def g1_of(i):
        g1[i] = jnp.where(h1t[i] > 0, dot(w2_ref[...], d2[i]), 0.0).astype(BF16)

    g1_of(0)
    lane = lax.broadcasted_iota(jnp.int32, (hid, cpad), 1)
    dw2 = dot(h1t[0], d2[0], ((1,), (1,)))
    part2[...] = jnp.zeros_like(part2)
    part2[:, 0:cpad] = jnp.where(lane == classes, loss_part, dw2)
    h1t_cp.wait_recv()
    d2_cp.wait_recv()
    g1_of(1)

    half = nb // 2
    units = ((3, 0), (3, 1), (1, 0), (2, 1), (2, 0), (1, 1), (0, 0), (0, 1))
    sib6, got = {}, {}

    def part6_of(q, h, dc):
        s, sp = POS[q] * 2 + dc, POS[q + 4] * 2 + dc
        lo = h * half
        return dot(g1[0], abuf[s, :, lo:lo + half]) + dot(g1[1], abuf[sp, :, lo:lo + half])

    def fin6(i):
        q, h = units[i]
        sib6[i].wait_recv()
        p6sum[i] += p6sib[i]
        first = 1 if h == 0 else 2
        if q == 3:
            got[("f", h)] = send(p6sum.at[i], r6f.at[h], first, 0)
        elif q == first:
            got[("x", h)] = send(p6sum.at[i], r6x.at[h], first, 0)

    red2 = None
    for i, (q, h) in enumerate(units):
        p6out[i] = part6_of(q, h, 1)
        sib6[i] = send(p6out.at[i], p6sib.at[i], 0, 1)
        p6sum[i] = part6_of(q, h, 0)
        if i:
            fin6(i - 1)
        if i == 3:
            red2 = reduce_start(part2, rb2)
    fin6(len(units) - 1)
    for h, i in ((0, 4), (1, 5)):
        got[("f", h)].wait_recv()
        p6sum[i] += r6f[h]
        got[("y", h)] = send(p6sum.at[i], r6y.at[h], 2 if h == 0 else 1, 0)
    out2 = reduce_mid(part2, rb2, res2, red2)
    for h in (0, 1):
        got[("x", h)].wait_recv()
        p6sum[6 + h] += r6x[h]
    for cp in out2:
        cp.wait_recv()
    o2_ref[...] = res2[...]
    acc = None
    for h in (0, 1):
        got[("y", h)].wait_recv()
        d1[h] = (p6sum[6 + h] + r6y[h]).astype(BF16)
        term = dot(d1[h], xg[0, h * half:(h + 1) * half, :])
        acc = term if acc is None else acc + term
    part1[...] = acc
    red1 = reduce_start(part1, rb1)
    out1 = reduce_mid(part1, rb1, res1, red1)
    for cp in out1:
        cp.wait_recv()
    o1_ref[...] = res1[...]
    for cp in sent:
        cp.wait_send()


def solution(mesh):
    def local_step(adj_rows, features, w_one, w_two, labels, label_mask):
        nb, f_in = features.shape
        total = adj_rows.shape[1]
        hid, classes = w_two.shape
        cpad = 48
        lanes = 128
        xp = jnp.concatenate([features, label_mask[:, None].astype(BF16), jnp.zeros((nb, lanes - f_in - 1), BF16)], axis=1)
        w1p = jnp.pad(w_one.astype(BF16), ((0, lanes - f_in), (0, 0)))
        w2p = jnp.pad(w_two.astype(BF16), ((0, 0), (0, cpad - classes)))
        vmem = pl.BlockSpec(memory_space=pltpu.VMEM)
        anyspec = pl.BlockSpec(memory_space=pl.ANY)
        V = pltpu.VMEM
        nsem = 160
        half = nb // 2
        o1, o2 = pl.pallas_call(
            functools.partial(step_kernel, nb, classes, f_in, cpad),
            out_shape=[jax.ShapeDtypeStruct((hid, lanes), F32), jax.ShapeDtypeStruct((hid, lanes), F32)],
            in_specs=[anyspec, anyspec, vmem, vmem, vmem, vmem, vmem],
            out_specs=[vmem, vmem],
            scratch_shapes=[
                V((total // nb, nb, nb), BF16), V((16, nb, lanes), BF16), V((nb, hid), BF16), V((16, lanes), F32),
                V((nb, hid), F32), V((2, hid, nb), BF16), V((16, cpad, nb), BF16), V((nb, lanes), F32), V((2, cpad, nb), BF16),
                V((4, cpad, nb), F32), V((4, cpad, nb), F32), V((4, cpad, nb), F32), V((3, cpad, nb), F32),
                V((2, cpad, nb), BF16), V((2, hid, nb), BF16),
                V((8, hid, half), F32), V((8, hid, half), F32), V((8, hid, half), F32),
                V((2, hid, half), F32), V((2, hid, half), F32), V((2, hid, half), F32), V((2, hid, half), BF16),
                V((hid, lanes), F32), V((hid, lanes), F32), V((15, hid // 16, lanes), F32), V((15, hid // 16, lanes), F32),
                V((hid, lanes), F32), V((hid, lanes), F32),
                pltpu.SemaphoreType.DMA((16,)), pltpu.SemaphoreType.DMA,
                pltpu.SemaphoreType.DMA((nsem,)), pltpu.SemaphoreType.DMA((nsem,)),
            ],
            compiler_params=pltpu.CompilerParams(collective_id=0, has_side_effects=True, vmem_limit_bytes=67043328),
            name="gcn_step",
        )(adj_rows, xp, w1p, w2p, w2p.T, labels.reshape(1, nb), label_mask.reshape(1, nb))
        return o2[0, classes], o1[:, :f_in].T, o2[:, :classes]

    row_spec = P(("nodes", "rep"))
    return jax.shard_map(local_step, mesh=mesh, in_specs=(P("nodes", None), P(("nodes", "rep"), None), P(), P(), row_spec, row_spec), out_specs=(P(), P(), P()), check_vma=False)
```

```python
import functools

import jax
import jax.numpy as jnp
from jax import lax
from jax.experimental import pallas as pl
from jax.experimental.pallas import tpu as pltpu
from jax.sharding import PartitionSpec as P

BF16 = jnp.bfloat16
scope = jax.named_scope
F32 = jnp.float32

POS = {0: 0, 1: 1, 2: 2, 4: 3, 3: 4, 5: 5, 6: 6, 7: 7}
ORDERS = ((1, 2, 4), (2, 4, 1), (4, 1, 2))


def dot(a, b, dims=((1,), (0,))):
    return lax.dot_general(a, b, (dims, ((), ())), preferred_element_type=F32)


def step_kernel(nb, classes, f_in, cpad,
                a_hbm, x_hbm, w1_ref, w2_ref, w2t_ref, lab_ref, msk_ref,
                o1_ref, o2_ref,
                abuf, xg, y1, cnt, z1, h1t, y2g, z2, g2,
                p2out, p2sib, p2sum, p2rcv, d2, g1,
                p6out, p6sib, p6sum, r6f, r6x, r6y, d1,
                part1, part2, rb1, rb2, res1, res2,
                asem, xsem, ssem, rsem):
    r = lax.axis_index("rep")
    n = lax.axis_index("nodes")
    core = n % 2
    xc = (n // 2) % 2
    yc = n // 4
    hid = z1.shape[1]

    def flip(v, f):
        return 1 - v if f else v

    def coords(k, dc):
        rr = flip(r, k // 4)
        nn = flip(yc, (k // 2) % 2) * 4 + flip(xc, k % 2) * 2 + flip(core, dc)
        return rr, nn

    def block_id(k, dc):
        rr, nn = coords(k, dc)
        return nn * 2 + rr

    sent = []

    def send(src, dst, k, dc):
        i = len(sent)
        cp = pltpu.make_async_remote_copy(
            src_ref=src, dst_ref=dst, send_sem=ssem.at[i], recv_sem=rsem.at[i],
            device_id=coords(k, dc), device_id_type=pl.DeviceIdType.MESH)
        cp.start()
        sent.append(cp)
        return cp

    peers = [(k, dc) for k in range(8) for dc in range(2) if (k, dc) != (0, 0)]

    xload = pltpu.make_async_copy(x_hbm, xg.at[0], xsem)
    xload.start()
    barrier = pltpu.get_barrier_semaphore()
    for k, dc in peers:
        pl.semaphore_signal(barrier, inc=1, device_id=coords(k, dc), device_id_type=pl.DeviceIdType.MESH)
    cnt[...] = jnp.zeros_like(cnt)
    z1[...] = jnp.zeros_like(z1)
    z2[...] = jnp.zeros_like(z2)
    with scope("entry"):
        xload.wait()
        loads = {}
        for k in POS:
            for dc in range(2):
                slot = POS[k] * 2 + dc
                col = pl.multiple_of(block_id(k, dc) * nb, nb)
                row = pl.multiple_of(r * nb, nb)
                cp = pltpu.make_async_copy(a_hbm.at[pl.ds(row, nb), pl.ds(col, nb)], abuf.at[slot], asem.at[slot])
                cp.start()
                loads[slot] = cp
        pl.semaphore_wait(barrier, len(peers))

    def gather(buf, cuts, consume):
        def at(k, dc):
            return buf.at[POS[k] * 2 + dc]

        def piece(k, p):
            return buf.at[POS[k] * 2, pl.ds(cuts[p], cuts[p + 1] - cuts[p])]

        near = {k: send(at(0, 0), at(k, 0), k, 0) for k in (1, 2, 4)}
        sib = {0: send(at(0, 0), at(0, 1), 0, 1)}
        with scope("g0"):
            sib[0].wait_recv()
            consume(0, 2)
        two = {}
        for k in (1, 2, 4):
            with scope("g1_wait"):
                near[k].wait_recv()
            for p, (d0, d1_, d2_) in enumerate(ORDERS):
                if k == d0:
                    two[(d0 + d1_, p)] = send(piece(d0, p), piece(d0 + d1_, p), d1_, 0)
                    two[(d0 + d2_, p)] = send(piece(d0, p), piece(d0 + d2_, p), d2_, 0)
                if k == d1_:
                    two[(d1_ + d2_, p)] = send(piece(d1_, p), piece(d1_ + d2_, p), d2_, 0)
            sib[k] = send(at(k, 0), at(k, 1), 0, 1)
        with scope("g1_sib"):
            for k in (1, 2, 4):
                sib[k].wait_recv()
        with scope("g1_compute"):
            consume(2, 8)
        three = []
        for k in (3, 6, 5):
            for p, (d0, d1_, d2_) in enumerate(ORDERS):
                with scope("g2_wait"):
                    two[(k, p)].wait_recv()
                if k == d0 + d1_:
                    three.append(send(piece(k, p), piece(7, p), d2_, 0))
            sib[k] = send(at(k, 0), at(k, 1), 0, 1)
        with scope("g2_sib"):
            for k in (3, 6, 5):
                sib[k].wait_recv()
        with scope("g2_compute"):
            consume(8, 14)
        with scope("g3_wait"):
            for cp in three:
                cp.wait_recv()
        sib[7] = send(at(7, 0), at(7, 1), 0, 1)
        with scope("g3_sib"):
            sib[7].wait_recv()
        with scope("g3_compute"):
            consume(14, 16)

    ones = jnp.ones((16, nb), BF16)
    mrows = 256

    def z1_blocks(lo, hi):
        for s in range(lo, hi):
            loads[s].wait()

        @pl.loop(lo, hi)
        def _(s):
            xb = xg[s]
            cnt[...] += dot(ones, xb)
            y1[...] = dot(xb, w1_ref[...]).astype(BF16)
            yv = y1[...]
            for m in range(0, nb, mrows):
                z1[m:m + mrows, :] += dot(abuf[s, m:m + mrows, :], yv)

    third = (nb // 48) * 16
    gather(xg, (0, nb - 2 * third, nb - third, nb), z1_blocks)

    with scope("h1y2"):
        for m in range(0, nb, mrows):
            h1t[0, :, m:m + mrows] = jnp.maximum(z1[m:m + mrows, :], 0.0).T.astype(BF16)
        y2g[0] = dot(w2t_ref[...], h1t[0]).astype(BF16)

    reload = {}

    def z2_blocks(lo, hi):
        @pl.loop(lo, hi)
        def _(s):
            for m in range(0, nb, mrows):
                z2[m:m + mrows, 0:cpad] += dot(abuf[s, m:m + mrows, :], y2g[s], ((1,), (1,)))

        for k in range(4, 8):
            for dc in range(2):
                slot = POS[k] * 2 + dc
                if lo <= slot < hi:
                    col = pl.multiple_of(block_id(k - 4, dc) * nb, nb)
                    row = pl.multiple_of((1 - r) * nb, nb)
                    cp = pltpu.make_async_copy(a_hbm.at[pl.ds(row, nb), pl.ds(col, nb)], abuf.at[slot], asem.at[slot])
                    cp.start()
                    reload[slot] = cp

    third = cpad // 3
    gather(y2g, (0, third, 2 * third, cpad), z2_blocks)

    z2t = z2[...].T[0:cpad, :]
    cls = lax.broadcasted_iota(jnp.int32, (cpad, nb), 0)
    zm = jnp.where(cls < classes, z2t, -jnp.inf)
    zs = zm - jnp.max(zm, axis=0, keepdims=True)
    logp = zs - jnp.log(jnp.sum(jnp.exp(zs), axis=0, keepdims=True))
    hot = cls == lab_ref[...]
    mask_f = msk_ref[...].astype(F32)
    total_m = cnt[0:1, f_in:f_in + 1]
    loss_v = -mask_f * jnp.sum(jnp.where(hot, logp, 0.0), axis=0, keepdims=True)
    loss_part = jnp.sum(loss_v, axis=1, keepdims=True) / total_m
    g2[0] = ((jnp.exp(logp) - hot.astype(F32)) * (mask_f / total_m)).astype(BF16)
    g2_cp = send(g2.at[0], g2.at[1], 4, 0)
    h1t_cp = send(h1t.at[0], h1t.at[1], 4, 0)
    with scope("g2z_wait"):
        g2_cp.wait_recv()
        for s in reload:
            reload[s].wait()

    order = (3, 1, 2, 0)
    sib2, rcv2 = {}, {}

    def fin2(q):
        with scope("p2sib"):
            sib2[q].wait_recv()
        p2sum[q] += p2sib[q]
        if q:
            rcv2[q] = send(p2sum.at[q], p2rcv.at[q - 1], q, 0)

    def part2_of(q, dc):
        s, sp = POS[q] * 2 + dc, POS[q + 4] * 2 + dc
        return dot(g2[0], abuf[s]) + dot(g2[1], abuf[sp])

    for i, q in enumerate(order):
        with scope("p2a"):
            p2out[q] = part2_of(q, 1)
        sib2[q] = send(p2out.at[q], p2sib.at[q], 0, 1)
        with scope("p2b"):
            p2sum[q] = part2_of(q, 0)
        if i:
            fin2(order[i - 1])
    fin2(0)
    with scope("p2rcv"):
        for q in (1, 2, 3):
            rcv2[q].wait_recv()
    d2[0] = (p2sum[0] + p2rcv[0] + p2rcv[1] + p2rcv[2]).astype(BF16)
    d2_cp = send(d2.at[0], d2.at[1], 4, 0)

    rows = hid // 16

    def reduce_start(part, rb):
        return [send(part.at[pl.ds(pl.multiple_of(block_id(k, dc) * rows, rows), rows)], rb.at[i], k, dc)
                for i, (k, dc) in enumerate(peers)]

    def reduce_mid(part, rb, res, cps):
        own = pl.ds(pl.multiple_of(block_id(0, 0) * rows, rows), rows)
        acc = part[own, :]
        for i, cp in enumerate(cps):
            cp.wait_recv()
            acc = acc + rb[i]
        res[own, :] = acc
        return [send(res.at[own], res.at[own], k, dc) for k, dc in peers]

    def g1_of(i):
        g1[i] = jnp.where(h1t[i] > 0, dot(w2_ref[...], d2[i]), 0.0).astype(BF16)

    lane = lax.broadcasted_iota(jnp.int32, (hid, cpad), 1)
    dw2 = dot(h1t[0], d2[0], ((1,), (1,)))
    part2[...] = jnp.zeros_like(part2)
    part2[:, 0:cpad] = jnp.where(lane == classes, loss_part, dw2)
    red2 = reduce_start(part2, rb2)
    g1_of(0)
    h1t_cp.wait_recv()
    with scope("d2z_wait"):
        d2_cp.wait_recv()
    with scope("g1b"):
        g1_of(1)

    half = nb // 2
    units = ((3, 0), (3, 1), (1, 0), (2, 1), (2, 0), (1, 1), (0, 0), (0, 1))
    sib6, got = {}, {}

    def part6_of(q, h, dc):
        s, sp = POS[q] * 2 + dc, POS[q + 4] * 2 + dc
        lo = h * half
        return dot(g1[0], abuf[s, :, lo:lo + half]) + dot(g1[1], abuf[sp, :, lo:lo + half])

    def fin6(i):
        q, h = units[i]
        with scope("p6sib"):
            sib6[i].wait_recv()
        p6sum[i] += p6sib[i]
        first = 1 if h == 0 else 2
        if q == 3:
            got[("f", h)] = send(p6sum.at[i], r6f.at[h], first, 0)
        elif q == first:
            got[("x", h)] = send(p6sum.at[i], r6x.at[h], first, 0)

    for i, (q, h) in enumerate(units):
        with scope("p6a"):
            p6out[i] = part6_of(q, h, 1)
        sib6[i] = send(p6out.at[i], p6sib.at[i], 0, 1)
        with scope("p6b"):
            p6sum[i] = part6_of(q, h, 0)
        if i:
            fin6(i - 1)
        if i == 1:
            out2 = reduce_mid(part2, rb2, res2, red2)
    fin6(len(units) - 1)
    for h, i in ((0, 4), (1, 5)):
        with scope("f_wait"):
            got[("f", h)].wait_recv()
        p6sum[i] += r6f[h]
        got[("y", h)] = send(p6sum.at[i], r6y.at[h], 2 if h == 0 else 1, 0)
    for h in (0, 1):
        with scope("x_wait"):
            got[("x", h)].wait_recv()
        p6sum[6 + h] += r6x[h]
    with scope("out2_wait"):
        for cp in out2:
            cp.wait_recv()
    o2_ref[...] = res2[...]
    acc = None
    for h in (0, 1):
        with scope("y_wait"):
            got[("y", h)].wait_recv()
        d1[h] = (p6sum[6 + h] + r6y[h]).astype(BF16)
        term = dot(d1[h], xg[0, h * half:(h + 1) * half, :])
        acc = term if acc is None else acc + term
    part1[...] = acc
    with scope("red1"):
        red1 = reduce_start(part1, rb1)
        out1 = reduce_mid(part1, rb1, res1, red1)
    with scope("out1_wait"):
        for cp in out1:
            cp.wait_recv()
    o1_ref[...] = res1[...]
    with scope("send_wait"):
        for cp in sent:
            cp.wait_send()


def solution(mesh):
    def local_step(adj_rows, features, w_one, w_two, labels, label_mask):
        nb, f_in = features.shape
        total = adj_rows.shape[1]
        hid, classes = w_two.shape
        cpad = 48
        lanes = 128
        xp = jnp.concatenate([features, label_mask[:, None].astype(BF16), jnp.zeros((nb, lanes - f_in - 1), BF16)], axis=1)
        w1p = jnp.pad(w_one.astype(BF16), ((0, lanes - f_in), (0, 0)))
        w2p = jnp.pad(w_two.astype(BF16), ((0, 0), (0, cpad - classes)))
        vmem = pl.BlockSpec(memory_space=pltpu.VMEM)
        anyspec = pl.BlockSpec(memory_space=pl.ANY)
        V = pltpu.VMEM
        nsem = 160
        half = nb // 2
        o1, o2 = pl.pallas_call(
            functools.partial(step_kernel, nb, classes, f_in, cpad),
            out_shape=[jax.ShapeDtypeStruct((hid, lanes), F32), jax.ShapeDtypeStruct((hid, lanes), F32)],
            in_specs=[anyspec, anyspec, vmem, vmem, vmem, vmem, vmem],
            out_specs=[vmem, vmem],
            scratch_shapes=[
                V((total // nb, nb, nb), BF16), V((16, nb, lanes), BF16), V((nb, hid), BF16), V((16, lanes), F32),
                V((nb, hid), F32), V((2, hid, nb), BF16), V((16, cpad, nb), BF16), V((nb, lanes), F32), V((2, cpad, nb), BF16),
                V((4, cpad, nb), F32), V((4, cpad, nb), F32), V((4, cpad, nb), F32), V((3, cpad, nb), F32),
                V((2, cpad, nb), BF16), V((2, hid, nb), BF16),
                V((8, hid, half), F32), V((8, hid, half), F32), V((8, hid, half), F32),
                V((2, hid, half), F32), V((2, hid, half), F32), V((2, hid, half), F32), V((2, hid, half), BF16),
                V((hid, lanes), F32), V((hid, lanes), F32), V((15, hid // 16, lanes), F32), V((15, hid // 16, lanes), F32),
                V((hid, lanes), F32), V((hid, lanes), F32),
                pltpu.SemaphoreType.DMA((16,)), pltpu.SemaphoreType.DMA,
                pltpu.SemaphoreType.DMA((nsem,)), pltpu.SemaphoreType.DMA((nsem,)),
            ],
            compiler_params=pltpu.CompilerParams(collective_id=0, has_side_effects=True, vmem_limit_bytes=67043328),
            name="gcn_step",
        )(adj_rows, xp, w1p, w2p, w2p.T, labels.reshape(1, nb), label_mask.reshape(1, nb))
        return o2[0, classes], o1[:, :f_in].T, o2[:, :classes]

    row_spec = P(("nodes", "rep"))
    return jax.shard_map(local_step, mesh=mesh, in_specs=(P("nodes", None), P(("nodes", "rep"), None), P(), P(), row_spec, row_spec), out_specs=(P(), P(), P()), check_vma=False)
```

```python
import functools

import jax
import jax.numpy as jnp
from jax import lax
from jax.experimental import pallas as pl
from jax.experimental.pallas import tpu as pltpu
from jax.sharding import PartitionSpec as P

BF16 = jnp.bfloat16
F32 = jnp.float32
scope = jax.named_scope

SLOTS = {(0, 0): 0, (0, 1): 1, (1, 0): 2, (2, 0): 3, (4, 0): 4, (1, 1): 5, (2, 1): 6, (4, 1): 7,
         (3, 0): 8, (6, 0): 9, (5, 0): 10, (3, 1): 11, (6, 1): 12, (5, 1): 13, (7, 0): 14, (7, 1): 15}
ORDERS = ((1, 2, 4), (2, 4, 1), (4, 1, 2))
COUNT_BASE = 32.0


def dot(a, b, dims=((1,), (0,))):
    return lax.dot_general(a, b, (dims, ((), ())), preferred_element_type=F32)


def step_kernel(nb, classes, f_in, cpad,
                a_hbm, x_hbm, w1_hbm, w2_hbm, lab_hbm, msk_hbm,
                loss_ref, o1_ref, o2_ref,
                abuf, xg, y1, z1, h1t, y2g, z2, g2,
                xraw, w1raw, w2raw, lab_ref, msk_ref, w1t_ref, w2_ref, w2t_ref, w1f, w2f,
                p2out, p2sib, p2sum, p2rcv, d2, g1,
                p6out, p6sib, p6sum, r6f, r6x, r6y, d1,
                part1, part2, rb1, rb2, res1, res2,
                asem, psem, ssem, rsem):
    r = lax.axis_index("rep")
    n = lax.axis_index("nodes")
    core = n % 2
    xc = (n // 2) % 2
    yc = n // 4
    hid = z1.shape[1]
    fpad = xg.shape[1]

    def flip(v, f):
        return 1 - v if f else v

    def coords(k, dc):
        rr = flip(r, k // 4)
        nn = flip(yc, (k // 2) % 2) * 4 + flip(xc, k % 2) * 2 + flip(core, dc)
        return rr, nn

    def block_id(k, dc):
        rr, nn = coords(k, dc)
        return nn * 2 + rr

    sent = []

    def prepare(src, dst, k, dc):
        i = len(sent)
        cp = pltpu.make_async_remote_copy(
            src_ref=src, dst_ref=dst, send_sem=ssem.at[i], recv_sem=rsem.at[i],
            device_id=coords(k, dc), device_id_type=pl.DeviceIdType.MESH)
        sent.append(cp)
        return cp

    def send(src, dst, k, dc):
        cp = prepare(src, dst, k, dc)
        cp.start()
        return cp

    peers = [(k, dc) for k in range(8) for dc in range(2) if (k, dc) != (0, 0)]

    pre = [pltpu.make_async_copy(src, dst, psem.at[i]) for i, (src, dst) in enumerate(
        ((x_hbm, xraw), (msk_hbm, msk_ref), (w1_hbm, w1raw), (w2_hbm, w2raw), (lab_hbm, lab_ref)))]
    for cp in pre:
        cp.start()
    barrier = pltpu.get_barrier_semaphore()
    for k, dc in peers:
        pl.semaphore_signal(barrier, inc=1, device_id=coords(k, dc), device_id_type=pl.DeviceIdType.MESH)
    z1[...] = jnp.zeros_like(z1)
    z2[...] = jnp.zeros_like(z2)
    part1[...] = jnp.zeros_like(part1)
    part2[...] = jnp.zeros_like(part2)
    w1f[...] = jnp.zeros_like(w1f)
    w2f[...] = jnp.zeros_like(w2f)
    xg[0] = jnp.zeros((fpad, nb), BF16)
    with scope("entry_x"):
        pre[0].wait()
        pre[1].wait()

    def a_rows(group_row, k, dc, slot):
        row = pl.multiple_of(group_row * nb, nb)
        col = pl.multiple_of(block_id(k, dc) * nb, nb)
        return pltpu.make_async_copy(a_hbm.at[pl.ds(row, nb), pl.ds(col, nb)], abuf.at[slot], asem.at[slot])

    for (k, dc), slot in SLOTS.items():
        a_rows(r, k, dc, slot).start()

    xg[0, 0:f_in, :] = xraw[...]
    count = jnp.sum(msk_ref[...].astype(F32), axis=1, keepdims=True)
    hi = jnp.floor(count * (1.0 / COUNT_BASE))
    lo = count - COUNT_BASE * hi
    row16 = lax.broadcasted_iota(jnp.int32, (16, 128), 0) + (fpad - 16)
    tail = xg[0, fpad - 16:fpad, 0:128].astype(F32)
    tail = jnp.where(row16 == f_in, hi, jnp.where(row16 == f_in + 1, lo, tail))
    xg[0, fpad - 16:fpad, 0:128] = tail.astype(BF16)
    with scope("entry_w"):
        for cp in pre[2:]:
            cp.wait()
    w1f[0:f_in, :] = w1raw[...]
    w1t_ref[...] = w1f[...].T[:, 0:fpad].astype(BF16)
    w2f[0:classes, :] = w2raw[...]
    w2t_ref[...] = w2f[0:cpad, :].astype(BF16)
    w2_ref[...] = w2f[...].T[:, 0:cpad].astype(BF16)
    with scope("entry_barrier"):
        pl.semaphore_wait(barrier, len(peers))

    def gather(buf, cuts, by_node, pair_work, after_pair):
        def at(k, dc):
            return buf.at[SLOTS[k, dc]]

        def piece(k, p):
            span = pl.ds(cuts[p], cuts[p + 1] - cuts[p])
            return buf.at[(SLOTS[k, 0], slice(None), span) if by_node else (SLOTS[k, 0], span)]

        sib0 = send(at(0, 0), at(0, 1), 0, 1)
        near, two, three, sib = {}, {}, {}, {0: sib0}
        for j in range(3):
            for p, order in enumerate(ORDERS):
                near[j, p] = send(piece(0, p), piece(order[j], p), order[j], 0)
        for p, (d0, d1_, d2_) in enumerate(ORDERS):
            two[0, p] = prepare(piece(d0, p), piece(d0 + d1_, p), d1_, 0)
            two[1, p] = prepare(piece(d0, p), piece(d0 + d2_, p), d2_, 0)
            two[2, p] = prepare(piece(d1_, p), piece(d1_ + d2_, p), d2_, 0)
            three[p] = prepare(piece(d0 + d1_, p), piece(7, p), d2_, 0)
        for k in range(1, 8):
            sib[k] = prepare(at(k, 0), at(k, 1), 0, 1)

        def wait(*cps):
            for cp in cps:
                cp.wait_recv()

        def start(*cps):
            for cp in cps:
                cp.start()

        def event(t):
            if t == 0:
                wait(sib[0])
            if t == 1:
                for p in range(3):
                    wait(near[0, p])
                    start(two[0, p], two[1, p])
                for p in range(3):
                    wait(near[1, p])
                    start(two[2, p])
                for p in range(3):
                    wait(near[2, p])
                start(sib[1], sib[2], sib[4])
            if t == 2:
                for p in range(3):
                    wait(two[0, p])
                    start(three[p])
                wait(sib[1])
            if t == 3:
                wait(sib[2], sib[4])
            if t == 4:
                for p in range(3):
                    wait(two[1, p], two[2, p])
                start(sib[3], sib[6], sib[5])
            if t == 5:
                wait(sib[3])
            if t == 6:
                for p in range(3):
                    wait(three[p])
                start(sib[7])
                wait(sib[6], sib[5])
            if t == 7:
                wait(sib[7])

        @pl.loop(0, 8)
        def _(t):
            for u in range(8):
                @pl.when(t == u)
                def _():
                    with scope(f"ev{u}"):
                        event(u)
                        if u:
                            after_pair(u - 1)
            with scope("pair"):
                pair_work(t)
        after_pair(7)

    mrows = nb // 2

    def z1_pair(t):
        for j in range(2):
            s = 2 * t + j
            pltpu.make_async_copy(a_hbm.at[pl.ds(0, nb), pl.ds(0, nb)], abuf.at[s], asem.at[s]).wait()
            y1[j] = dot(w1t_ref[...], xg[s]).astype(BF16)
        for m in range(0, nb, mrows):
            z1[m:m + mrows, :] += (dot(abuf[2 * t, m:m + mrows, :], y1[0], ((1,), (1,)))
                                   + dot(abuf[2 * t + 1, m:m + mrows, :], y1[1], ((1,), (1,))))

    third = (nb // 3 // 128 + 1) * 128
    gather(xg, (0, third, 2 * third, nb), True, z1_pair, lambda t: None)

    with scope("h1y2"):
        for m in range(0, nb, 256):
            h1t[0, :, m:m + 256] = jnp.maximum(z1[m:m + 256, :], 0.0).T.astype(BF16)
        y2g[0] = dot(w2t_ref[...], h1t[0]).astype(BF16)

    def z2_pair(t):
        for m in range(0, nb, mrows):
            z2[m:m + mrows, 0:cpad] += (dot(abuf[2 * t, m:m + mrows, :], y2g[2 * t], ((1,), (1,)))
                                        + dot(abuf[2 * t + 1, m:m + mrows, :], y2g[2 * t + 1], ((1,), (1,))))

    def z2_after(t):
        for (k, dc), slot in SLOTS.items():
            if slot // 2 == t and k >= 4:
                a_rows(1 - r, k - 4, dc, slot).start()

    third = cpad // 3
    gather(y2g, (0, third, 2 * third, cpad), False, z2_pair, z2_after)

    tails = xg[0, fpad - 16:fpad, 0:128].astype(F32)
    for s in range(1, 16):
        tails = tails + xg[s, fpad - 16:fpad, 0:128].astype(F32)
    at_hi = f_in - (fpad - 16)
    total_m = COUNT_BASE * tails[at_hi:at_hi + 1, 0:1] + tails[at_hi + 1:at_hi + 2, 0:1]
    z2t = z2[...].T[0:cpad, :]
    cls = lax.broadcasted_iota(jnp.int32, (cpad, nb), 0)
    zm = jnp.where(cls < classes, z2t, -jnp.inf)
    zs = zm - jnp.max(zm, axis=0, keepdims=True)
    logp = zs - jnp.log(jnp.sum(jnp.exp(zs), axis=0, keepdims=True))
    hot = cls == lab_ref[...]
    mask_f = msk_ref[...].astype(F32)
    loss_v = -mask_f * jnp.sum(jnp.where(hot, logp, 0.0), axis=0, keepdims=True)
    loss_part = jnp.sum(loss_v, axis=1, keepdims=True) / total_m
    g2[0] = ((jnp.exp(logp) - hot.astype(F32)) * (mask_f / total_m)).astype(BF16)
    g2_cp = send(g2.at[0], g2.at[1], 4, 0)
    h1t_cp = send(h1t.at[0], h1t.at[1], 4, 0)

    order = (3, 1, 2, 0)
    sib2, rcv2 = {}, {}

    with scope("p2own"):
        for q in order:
            p2out[q] = dot(g2[0], abuf[SLOTS[q, 1]])
            p2sum[q] = dot(g2[0], abuf[SLOTS[q, 0]])
    with scope("g2z_wait"):
        g2_cp.wait_recv()
        for (k, dc), slot in SLOTS.items():
            if k >= 4:
                a_rows(1 - r, k - 4, dc, slot).wait()

    def fin2(q):
        with scope("p2sib"):
            sib2[q].wait_recv()
        p2sum[q] += p2sib[q]
        if q:
            rcv2[q] = send(p2sum.at[q], p2rcv.at[q - 1], q, 0)

    for i, q in enumerate(order):
        with scope("p2a"):
            p2out[q] += dot(g2[1], abuf[SLOTS[q + 4, 1]])
        sib2[q] = send(p2out.at[q], p2sib.at[q], 0, 1)
        with scope("p2b"):
            p2sum[q] += dot(g2[1], abuf[SLOTS[q + 4, 0]])
        if i:
            fin2(order[i - 1])
    fin2(0)
    with scope("p2rcv"):
        for q in (1, 2, 3):
            rcv2[q].wait_recv()
    d2[0] = (p2sum[0] + p2rcv[0] + p2rcv[1] + p2rcv[2]).astype(BF16)
    d2_cp = send(d2.at[0], d2.at[1], 4, 0)

    rows = hid // 16

    def reduce_start(part, rb):
        return [send(part.at[pl.ds(pl.multiple_of(block_id(k, dc) * rows, rows), rows)], rb.at[i], k, dc)
                for i, (k, dc) in enumerate(peers)]

    def reduce_mid(part, rb, res, cps):
        own = pl.ds(pl.multiple_of(block_id(0, 0) * rows, rows), rows)
        acc = part[own, :]
        for i, cp in enumerate(cps):
            cp.wait_recv()
            acc = acc + rb[i]
        res[own, :] = acc
        return [send(res.at[own], res.at[own], k, dc) for k, dc in peers]

    def g1_of(i):
        g1[i] = jnp.where(h1t[i] > 0, dot(w2_ref[...], d2[i]), 0.0).astype(BF16)

    lane = lax.broadcasted_iota(jnp.int32, (hid, cpad), 1)
    dw2 = dot(h1t[0], d2[0], ((1,), (1,)))
    part2[:, 0:cpad] = jnp.where(lane == classes, loss_part, dw2)
    red2 = reduce_start(part2, rb2)
    g1_of(0)

    half = nb // 2
    units = ((3, 0), (3, 1), (1, 0), (2, 1), (2, 0), (1, 1), (0, 0), (0, 1))
    early = 2
    sib6, got = {}, {}

    def own6(q, h, dc):
        return dot(g1[0], abuf[SLOTS[q, dc], :, h * half:(h + 1) * half])

    def partner6(q, h, dc):
        return dot(g1[1], abuf[SLOTS[q + 4, dc], :, h * half:(h + 1) * half])

    def fin6(i):
        q, h = units[i]
        with scope("p6sib"):
            sib6[i].wait_recv()
        p6sum[i] += p6sib[i]
        first = 1 if h == 0 else 2
        if q == 3:
            got["f", h] = send(p6sum.at[i], r6f.at[h], first, 0)
        elif q == first:
            got["x", h] = send(p6sum.at[i], r6x.at[h], first, 0)

    with scope("p6own"):
        for i in range(early):
            p6out[i] = own6(*units[i], 1)
            p6sum[i] = own6(*units[i], 0)
    with scope("d2z_wait"):
        h1t_cp.wait_recv()
        d2_cp.wait_recv()
    with scope("g1b"):
        g1_of(1)
    with scope("p6early"):
        for i in range(early):
            p6out[i] += partner6(*units[i], 1)
            sib6[i] = send(p6out.at[i], p6sib.at[i], 0, 1)
        for i in range(early):
            p6sum[i] += partner6(*units[i], 0)
    for i in range(early):
        fin6(i)
    for i in range(early, len(units)):
        q, h = units[i]
        with scope("p6a"):
            p6out[i] = own6(q, h, 1) + partner6(q, h, 1)
        sib6[i] = send(p6out.at[i], p6sib.at[i], 0, 1)
        with scope("p6b"):
            p6sum[i] = own6(q, h, 0) + partner6(q, h, 0)
        if i > early:
            fin6(i - 1)
        if i == early:
            with scope("red2"):
                out2 = reduce_mid(part2, rb2, res2, red2)
    fin6(len(units) - 1)
    for h, i in ((0, 4), (1, 5)):
        with scope("f_wait"):
            got["f", h].wait_recv()
        p6sum[i] += r6f[h]
        got["y", h] = send(p6sum.at[i], r6y.at[h], 2 if h == 0 else 1, 0)
    for h in (0, 1):
        with scope("x_wait"):
            got["x", h].wait_recv()
        p6sum[6 + h] += r6x[h]
    with scope("out2_wait"):
        for cp in out2:
            cp.wait_recv()
    o2_ref[...] = res2[...].T[0:classes, :]
    loss_ref[...] = res2[0:1, classes:classes + 1]
    acc = None
    for h in (0, 1):
        with scope("y_wait"):
            got["y", h].wait_recv()
        d1[h] = (p6sum[6 + h] + r6y[h]).astype(BF16)
        term = dot(d1[h], xg[0, :, h * half:(h + 1) * half], ((1,), (1,)))
        acc = term if acc is None else acc + term
    part1[:, 0:fpad] = acc
    with scope("red1"):
        red1 = reduce_start(part1, rb1)
        out1 = reduce_mid(part1, rb1, res1, red1)
    with scope("out1_wait"):
        for cp in out1:
            cp.wait_recv()
    o1_ref[...] = res1[...].T[0:f_in, :]
    with scope("send_wait"):
        for cp in sent:
            cp.wait_send()


def solution(mesh):
    def local_step(adj_rows, features, w_one, w_two, labels, label_mask):
        nb, f_in = features.shape
        total = adj_rows.shape[1]
        hid, classes = w_two.shape
        cpad = 48
        lanes = 128
        fpad = 112
        half = nb // 2
        nsem = 144
        vmem = pl.BlockSpec(memory_space=pltpu.VMEM)
        anyspec = pl.BlockSpec(memory_space=pl.ANY)
        V = pltpu.VMEM
        loss, dw1, dw2 = pl.pallas_call(
            functools.partial(step_kernel, nb, classes, f_in, cpad),
            out_shape=[jax.ShapeDtypeStruct((1, 1), F32), jax.ShapeDtypeStruct((f_in, hid), F32),
                       jax.ShapeDtypeStruct((classes, hid), F32)],
            in_specs=[anyspec] * 6,
            out_specs=[vmem] * 3,
            scratch_shapes=[
                V((total // nb, nb, nb), BF16), V((16, fpad, nb), BF16), V((2, hid, nb), BF16),
                V((nb, hid), F32), V((2, hid, nb), BF16), V((16, cpad, nb), BF16), V((nb, lanes), F32), V((2, cpad, nb), BF16),
                V((f_in, nb), BF16), V((f_in, hid), F32), V((classes, hid), F32), V((1, nb), jnp.int32), V((1, nb), jnp.int32),
                V((hid, fpad), BF16), V((hid, cpad), BF16), V((cpad, hid), BF16), V((lanes, hid), F32), V((lanes, hid), F32),
                V((4, cpad, nb), F32), V((4, cpad, nb), F32), V((4, cpad, nb), F32), V((3, cpad, nb), F32),
                V((2, cpad, nb), BF16), V((2, hid, nb), BF16),
                V((8, hid, half), F32), V((8, hid, half), F32), V((8, hid, half), F32),
                V((2, hid, half), F32), V((2, hid, half), F32), V((2, hid, half), F32), V((2, hid, half), BF16),
                V((hid, lanes), F32), V((hid, lanes), F32), V((15, hid // 16, lanes), F32), V((15, hid // 16, lanes), F32),
                V((hid, lanes), F32), V((hid, lanes), F32),
                pltpu.SemaphoreType.DMA((16,)), pltpu.SemaphoreType.DMA((5,)),
                pltpu.SemaphoreType.DMA((nsem,)), pltpu.SemaphoreType.DMA((nsem,)),
            ],
            compiler_params=pltpu.CompilerParams(collective_id=0, has_side_effects=True, vmem_limit_bytes=67043328),
            name="gcn_step",
        )(adj_rows, features.T, w_one, w_two.T, labels.reshape(1, nb), label_mask.reshape(1, nb))
        return loss.reshape(()), dw1, dw2.T

    row_spec = P(("nodes", "rep"))
    return jax.shard_map(local_step, mesh=mesh, in_specs=(P("nodes", None), P(("nodes", "rep"), None), P(), P(), row_spec, row_spec), out_specs=(P(), P(), P()), check_vma=False)
```

```python
import functools

import jax
import jax.numpy as jnp
from jax import lax
from jax.experimental import pallas as pl
from jax.experimental.pallas import tpu as pltpu
from jax.sharding import PartitionSpec as P

BF16 = jnp.bfloat16
F32 = jnp.float32
scope = jax.named_scope

SLOTS = {(0, 0): 0, (0, 1): 1, (1, 0): 2, (2, 0): 3, (4, 0): 4, (1, 1): 5, (2, 1): 6, (4, 1): 7,
         (3, 0): 8, (6, 0): 9, (5, 0): 10, (3, 1): 11, (6, 1): 12, (5, 1): 13, (7, 0): 14, (7, 1): 15}
ORDERS = ((1, 2, 4), (2, 4, 1), (4, 1, 2))
COUNT_BASE = 32.0


def dot(a, b, dims=((1,), (0,))):
    return lax.dot_general(a, b, (dims, ((), ())), preferred_element_type=F32)


def step_kernel(nb, classes, f_in, cpad,
                a_hbm, x_hbm, w1_hbm, w2_hbm, lab_hbm, msk_hbm,
                loss_ref, o1_ref, o2_ref,
                abuf, xg, y1, z1, h1t, y2g, z2, g2,
                xraw, w1raw, w2raw, lab_ref, msk_ref, w1t_ref, w2_ref, w2t_ref, w1f, w2f,
                p2out, p2sib, p2sum, p2fwd, p2far, d2, g1,
                p6out, p6sib, p6sum, p6fwd, p6far, d1,
                part1, part2, rb1, rbc, rbz, sumc, sumz, res1, res2,
                asem, psem, ssem, rsem):
    r = lax.axis_index("rep")
    n = lax.axis_index("nodes")
    core = n % 2
    xc = (n // 2) % 2
    yc = n // 4
    hid = z1.shape[1]
    fpad = xg.shape[1]

    def flip(v, f):
        return 1 - v if f else v

    def coords(k, dc):
        rr = flip(r, k // 4)
        nn = flip(yc, (k // 2) % 2) * 4 + flip(xc, k % 2) * 2 + flip(core, dc)
        return rr, nn

    def block_id(k, dc):
        rr, nn = coords(k, dc)
        return nn * 2 + rr

    sent = []

    def prepare(src, dst, k, dc):
        i = len(sent)
        cp = pltpu.make_async_remote_copy(
            src_ref=src, dst_ref=dst, send_sem=ssem.at[i], recv_sem=rsem.at[i],
            device_id=coords(k, dc), device_id_type=pl.DeviceIdType.MESH)
        sent.append(cp)
        return cp

    def send(src, dst, k, dc):
        cp = prepare(src, dst, k, dc)
        cp.start()
        return cp

    peers = [(k, dc) for k in (7, 3, 5, 6, 1, 2, 4, 0) for dc in range(2) if (k, dc) != (0, 0)]

    pre = [pltpu.make_async_copy(src, dst, psem.at[i]) for i, (src, dst) in enumerate(
        ((x_hbm, xraw), (msk_hbm, msk_ref), (w1_hbm, w1raw), (w2_hbm, w2raw), (lab_hbm, lab_ref)))]
    for cp in pre:
        cp.start()
    barrier = pltpu.get_barrier_semaphore()
    near_peers = ((0, 1), (1, 0), (2, 0), (4, 0))
    for k, dc in near_peers:
        pl.semaphore_signal(barrier, inc=1, device_id=coords(k, dc), device_id_type=pl.DeviceIdType.MESH)
    z1[...] = jnp.zeros_like(z1)
    z2[...] = jnp.zeros_like(z2)
    part1[...] = jnp.zeros_like(part1)
    part2[...] = jnp.zeros_like(part2)
    w1f[...] = jnp.zeros_like(w1f)
    w2f[...] = jnp.zeros_like(w2f)
    xg[0] = jnp.zeros((fpad, nb), BF16)
    with scope("entry_x"):
        pre[0].wait()
        pre[1].wait()

    def a_rows(group_row, k, dc, slot):
        row = pl.multiple_of(group_row * nb, nb)
        col = pl.multiple_of(block_id(k, dc) * nb, nb)
        return pltpu.make_async_copy(a_hbm.at[pl.ds(row, nb), pl.ds(col, nb)], abuf.at[slot], asem.at[slot])

    for (k, dc), slot in SLOTS.items():
        a_rows(r, k, dc, slot).start()

    xg[0, 0:f_in, :] = xraw[...]
    count = jnp.sum(msk_ref[...].astype(F32), axis=1, keepdims=True)
    hi = jnp.floor(count * (1.0 / COUNT_BASE))
    lo = count - COUNT_BASE * hi
    row16 = lax.broadcasted_iota(jnp.int32, (16, 128), 0) + (fpad - 16)
    tail = xg[0, fpad - 16:fpad, 0:128].astype(F32)
    tail = jnp.where(row16 == f_in, hi, jnp.where(row16 == f_in + 1, lo, tail))
    xg[0, fpad - 16:fpad, 0:128] = tail.astype(BF16)
    with scope("entry_w"):
        for cp in pre[2:]:
            cp.wait()
    w1f[0:f_in, :] = w1raw[...]
    w1t_ref[...] = w1f[...].T[:, 0:fpad].astype(BF16)
    w2f[0:classes, :] = w2raw[...]
    w2t_ref[...] = w2f[0:cpad, :].astype(BF16)
    w2_ref[...] = w2f[...].T[:, 0:cpad].astype(BF16)
    with scope("entry_barrier"):
        pl.semaphore_wait(barrier, len(near_peers))

    def gather(buf, cuts, by_node, pair_work, after_pair):
        def at(k, dc):
            return buf.at[SLOTS[k, dc]]

        def piece(k, p):
            span = pl.ds(cuts[p], cuts[p + 1] - cuts[p])
            return buf.at[(SLOTS[k, 0], slice(None), span) if by_node else (SLOTS[k, 0], span)]

        sib0 = send(at(0, 0), at(0, 1), 0, 1)
        near, two, three, sib = {}, {}, {}, {0: sib0}
        for j in range(3):
            for p, order in enumerate(ORDERS):
                near[j, p] = send(piece(0, p), piece(order[j], p), order[j], 0)
        for p, (d0, d1_, d2_) in enumerate(ORDERS):
            two[0, p] = prepare(piece(d0, p), piece(d0 + d1_, p), d1_, 0)
            two[1, p] = prepare(piece(d0, p), piece(d0 + d2_, p), d2_, 0)
            two[2, p] = prepare(piece(d1_, p), piece(d1_ + d2_, p), d2_, 0)
            three[p] = prepare(piece(d0 + d1_, p), piece(7, p), d2_, 0)
        for k in range(1, 8):
            sib[k] = prepare(at(k, 0), at(k, 1), 0, 1)

        def wait(*cps):
            for cp in cps:
                cp.wait_recv()

        def start(*cps):
            for cp in cps:
                cp.start()

        def event(t):
            if t == 0:
                wait(sib[0])
            if t == 1:
                for p in range(3):
                    wait(near[0, p])
                    start(two[0, p], two[1, p])
                for p in range(3):
                    wait(near[1, p])
                    start(two[2, p])
                for p in range(3):
                    wait(near[2, p])
                start(sib[1], sib[2], sib[4])
            if t == 2:
                wait(sib[1])
            if t == 3:
                for p in range(3):
                    wait(two[0, p])
                    start(three[p])
                wait(sib[2], sib[4])
            if t == 4:
                for p in range(3):
                    wait(two[1, p], two[2, p])
                start(sib[3], sib[6], sib[5])
            if t == 5:
                wait(sib[3])
            if t == 6:
                for p in range(3):
                    wait(three[p])
                start(sib[7])
                wait(sib[6], sib[5])
            if t == 7:
                wait(sib[7])

        @pl.loop(0, 8)
        def _(t):
            for u in range(8):
                @pl.when(t == u)
                def _():
                    with scope(f"ev{u}"):
                        event(u)
                        if u:
                            after_pair(u - 1)
            with scope("pair"):
                pair_work(t)
        after_pair(7)

    mrows = nb // 2

    def z1_pair(t):
        for j in range(2):
            s = 2 * t + j
            pltpu.make_async_copy(a_hbm.at[pl.ds(0, nb), pl.ds(0, nb)], abuf.at[s], asem.at[s]).wait()
        for j in range(2):
            s = 2 * t + j
            y1[j] = dot(w1t_ref[...], xg[s]).astype(BF16)
        for m in range(0, nb, mrows):
            z1[m:m + mrows, :] += (dot(abuf[2 * t, m:m + mrows, :], y1[0], ((1,), (1,)))
                                   + dot(abuf[2 * t + 1, m:m + mrows, :], y1[1], ((1,), (1,))))

    third = (nb // 3 // 128 + 1) * 128
    gather(xg, (0, third, 2 * third, nb), True, z1_pair, lambda t: None)

    with scope("h1y2"):
        for m in range(0, nb, 256):
            h1t[0, :, m:m + 256] = jnp.maximum(z1[m:m + 256, :], 0.0).T.astype(BF16)
        y2g[0] = dot(w2t_ref[...], h1t[0]).astype(BF16)

    def z2_pair(t):
        for m in range(0, nb, mrows):
            z2[m:m + mrows, 0:cpad] += (dot(abuf[2 * t, m:m + mrows, :], y2g[2 * t], ((1,), (1,)))
                                        + dot(abuf[2 * t + 1, m:m + mrows, :], y2g[2 * t + 1], ((1,), (1,))))

    def z2_after(t):
        for (k, dc), slot in SLOTS.items():
            if slot // 2 == t and k >= 4:
                a_rows(1 - r, k - 4, dc, slot).start()

    third = cpad // 3
    gather(y2g, (0, third, 2 * third, cpad), False, z2_pair, z2_after)

    tails = xg[0, fpad - 16:fpad, 0:128].astype(F32)
    for s in range(1, 16):
        tails = tails + xg[s, fpad - 16:fpad, 0:128].astype(F32)
    at_hi = f_in - (fpad - 16)
    total_m = COUNT_BASE * tails[at_hi:at_hi + 1, 0:1] + tails[at_hi + 1:at_hi + 2, 0:1]
    z2t = z2[...].T[0:cpad, :]
    cls = lax.broadcasted_iota(jnp.int32, (cpad, nb), 0)
    zm = jnp.where(cls < classes, z2t, -jnp.inf)
    zs = zm - jnp.max(zm, axis=0, keepdims=True)
    logp = zs - jnp.log(jnp.sum(jnp.exp(zs), axis=0, keepdims=True))
    hot = cls == lab_ref[...]
    mask_f = msk_ref[...].astype(F32)
    loss_v = -mask_f * jnp.sum(jnp.where(hot, logp, 0.0), axis=0, keepdims=True)
    loss_part = jnp.sum(loss_v, axis=1, keepdims=True) / total_m
    g2[0] = ((jnp.exp(logp) - hot.astype(F32)) * (mask_f / total_m)).astype(BF16)
    g2_cp = send(g2.at[0], g2.at[1], 4, 0)
    h1t_cp = send(h1t.at[0], h1t.at[1], 4, 0)

    half = nb // 2
    units = ((3, 0), (3, 1), (1, 0), (2, 1), (2, 0), (1, 1), (0, 0), (0, 1))

    def tree(name, g, out, sibb, summ, rfwd, rfar, early):
        sibs, got = {}, {}

        def cols(h):
            return slice(h * half, (h + 1) * half)

        def own(q, h, dc):
            return dot(g[0], abuf[SLOTS[q, dc], :, cols(h)])

        def partner(q, h, dc):
            return dot(g[1], abuf[SLOTS[q + 4, dc], :, cols(h)])

        def first_dim(h):
            return 1 if h == 0 else 2

        def begin():
            for i in range(early):
                out[i] = own(*units[i], 1)
                summ[i] = own(*units[i], 0)

        def finish(i):
            q, h = units[i]
            with scope(name + "_sib"):
                sibs[i].wait_recv()
            summ[i] += sibb[i]
            if q == 3:
                got["f", h] = send(summ.at[i], rfwd.at[h], first_dim(h), 0)
            elif q == first_dim(h):
                got["x", h] = send(summ.at[i], rfar.at[h], first_dim(h), 0)

        def group(j):
            pair = (2 * j, 2 * j + 1)
            with scope(name + "_group"):
                for i in pair:
                    if i < early:
                        out[i] += partner(*units[i], 1)
                    else:
                        out[i] = own(*units[i], 1) + partner(*units[i], 1)
                    sibs[i] = send(out.at[i], sibb.at[i], 0, 1)
                for i in pair:
                    if i < early:
                        summ[i] += partner(*units[i], 0)
                    else:
                        summ[i] = own(*units[i], 0) + partner(*units[i], 0)
            return lambda: [finish(i) for i in pair]

        def forward():
            for h, i in ((0, 4), (1, 5)):
                with scope(name + "_fwait"):
                    got["f", h].wait_recv()
                summ[i] += rfwd[h]
                got["y", h] = send(summ.at[i], rfar.at[2 + h], 3 - first_dim(h), 0)
            for h in (0, 1):
                with scope(name + "_xwait"):
                    got["x", h].wait_recv()
                summ[6 + h] += rfar[h]

        def last(h):
            with scope(name + "_ywait"):
                got["y", h].wait_recv()
            return (summ[6 + h] + rfar[2 + h]).astype(BF16)

        return begin, group, forward, last

    begin, group, forward, last = tree("p2", g2, p2out, p2sib, p2sum, p2fwd, p2far, 8)
    with scope("p2own"):
        begin()
    with scope("g2z_wait"):
        g2_cp.wait_recv()
        for (k, dc), slot in SLOTS.items():
            if k >= 4:
                a_rows(1 - r, k - 4, dc, slot).wait()
    for j in range(4):
        group(j)()
    forward()
    for h in (0, 1):
        d2[0, :, h * half:(h + 1) * half] = last(h)
    d2_cp = send(d2.at[0], d2.at[1], 4, 0)

    def g1_of(i):
        g1[i] = jnp.where(h1t[i] > 0, dot(w2_ref[...], d2[i]), 0.0).astype(BF16)

    lane = lax.broadcasted_iota(jnp.int32, (hid, cpad), 1)
    dw2 = dot(h1t[0], d2[0], ((1,), (1,)))
    part2[:, 0:cpad] = jnp.where(lane == classes, loss_part, dw2)
    hc, hz = hid // 2, hid // 4

    def span(start, size):
        return pl.ds(pl.multiple_of(start, size), size)

    cp_c = send(part2.at[span((1 - core) * hc, hc)], rbc, 0, 1)
    g1_of(0)

    begin, group, forward, last = tree("p6", g1, p6out, p6sib, p6sum, p6fwd, p6far, 2)
    with scope("p6own"):
        begin()
    cp_c.wait_recv()
    sumc[...] = part2[span(core * hc, hc), :] + rbc[...]
    cp_z = send(sumc.at[span((1 - r) * hz, hz)], rbz.at[0], 4, 0)
    with scope("d2z_wait"):
        h1t_cp.wait_recv()
        d2_cp.wait_recv()
    with scope("g1b"):
        g1_of(1)
    fin0 = group(0)
    cp_z.wait_recv()
    sumz[0] = sumc[span(r * hz, hz), :] + rbz[0]
    cp_x = send(sumz.at[0], rbz.at[1], 1, 0)
    fin0()
    fin1 = group(1)
    cp_x.wait_recv()
    sumz[1] = sumz[0] + rbz[1]
    cp_y = send(sumz.at[1], rbz.at[2], 2, 0)
    fin1()
    group(2)()
    group(3)()
    forward()
    mine = span(core * hc + r * hz, hz)
    cp_y.wait_recv()
    res2[mine, :] = sumz[1] + rbz[2]
    cp_z = send(res2.at[mine], res2.at[mine], 4, 0)
    cp_z.wait_recv()
    mine = span(core * hc, hc)
    cp_c = send(res2.at[mine], res2.at[mine], 0, 1)
    cp_c.wait_recv()
    o2_ref[...] = res2[...].T[0:classes, :]
    loss_ref[...] = res2[0:1, classes:classes + 1]

    rows = hid // 16

    def reduce_start(part, rb):
        return [send(part.at[pl.ds(pl.multiple_of(block_id(k, dc) * rows, rows), rows)], rb.at[i], k, dc)
                for i, (k, dc) in enumerate(peers)]

    def reduce_mid(part, rb, res, cps):
        own = pl.ds(pl.multiple_of(block_id(0, 0) * rows, rows), rows)
        acc = part[own, :]
        for i, cp in enumerate(cps):
            cp.wait_recv()
            acc = acc + rb[i]
        res[own, :] = acc
        return [send(res.at[own], res.at[own], k, dc) for k, dc in peers]

    acc = None
    for h in (0, 1):
        d1[h] = last(h)
        term = dot(d1[h], xg[0, :, h * half:(h + 1) * half], ((1,), (1,)))
        acc = term if acc is None else acc + term
    part1[:, 0:fpad] = acc
    with scope("red1"):
        red1 = reduce_start(part1, rb1)
        out1 = reduce_mid(part1, rb1, res1, red1)
    with scope("out1_wait"):
        for cp in out1:
            cp.wait_recv()
    o1_ref[...] = res1[...].T[0:f_in, :]
    with scope("send_wait"):
        for cp in sent:
            cp.wait_send()


def solution(mesh):
    def local_step(adj_rows, features, w_one, w_two, labels, label_mask):
        nb, f_in = features.shape
        total = adj_rows.shape[1]
        hid, classes = w_two.shape
        cpad = 48
        lanes = 128
        fpad = 112
        half = nb // 2
        nsem = 144
        vmem = pl.BlockSpec(memory_space=pltpu.VMEM)
        anyspec = pl.BlockSpec(memory_space=pl.ANY)
        V = pltpu.VMEM
        loss, dw1, dw2 = pl.pallas_call(
            functools.partial(step_kernel, nb, classes, f_in, cpad),
            out_shape=[jax.ShapeDtypeStruct((1, 1), F32), jax.ShapeDtypeStruct((f_in, hid), F32),
                       jax.ShapeDtypeStruct((classes, hid), F32)],
            in_specs=[anyspec] * 6,
            out_specs=[vmem] * 3,
            scratch_shapes=[
                V((total // nb, nb, nb), BF16), V((16, fpad, nb), BF16), V((2, hid, nb), BF16),
                V((nb, hid), F32), V((2, hid, nb), BF16), V((16, cpad, nb), BF16), V((nb, lanes), F32), V((2, cpad, nb), BF16),
                V((f_in, nb), BF16), V((f_in, hid), F32), V((classes, hid), F32), V((1, nb), jnp.int32), V((1, nb), jnp.int32),
                V((hid, fpad), BF16), V((hid, cpad), BF16), V((cpad, hid), BF16), V((lanes, hid), F32), V((lanes, hid), F32),
                V((8, cpad, half), F32), V((8, cpad, half), F32), V((8, cpad, half), F32), V((2, cpad, half), F32), V((4, cpad, half), F32),
                V((2, cpad, nb), BF16), V((2, hid, nb), BF16),
                V((8, hid, half), F32), V((8, hid, half), F32), V((8, hid, half), F32),
                V((2, hid, half), F32), V((4, hid, half), F32), V((2, hid, half), BF16),
                V((hid, lanes), F32), V((hid, lanes), F32), V((15, hid // 16, lanes), F32), V((hid // 2, lanes), F32),
                V((3, hid // 4, lanes), F32), V((hid // 2, lanes), F32), V((2, hid // 4, lanes), F32),
                V((hid, lanes), F32), V((hid, lanes), F32),
                pltpu.SemaphoreType.DMA((16,)), pltpu.SemaphoreType.DMA((5,)),
                pltpu.SemaphoreType.DMA((nsem,)), pltpu.SemaphoreType.DMA((nsem,)),
            ],
            compiler_params=pltpu.CompilerParams(collective_id=0, has_side_effects=True, vmem_limit_bytes=67043328),
            name="gcn_step",
        )(adj_rows, features.T, w_one, w_two.T, labels.reshape(1, nb), label_mask.reshape(1, nb))
        return loss.reshape(()), dw1, dw2.T

    row_spec = P(("nodes", "rep"))
    return jax.shard_map(local_step, mesh=mesh, in_specs=(P("nodes", None), P(("nodes", "rep"), None), P(), P(), row_spec, row_spec), out_specs=(P(), P(), P()), check_vma=False)
```

```python
import functools

import jax
import jax.numpy as jnp
from jax import lax
from jax.experimental import pallas as pl
from jax.experimental.pallas import tpu as pltpu
from jax.sharding import PartitionSpec as P

BF16 = jnp.bfloat16
F32 = jnp.float32
scope = jax.named_scope

ORDERS = ((1, 2, 4), (2, 4, 1), (4, 1, 2))
STAGES = (((0,) * 3,) + tuple(tuple(o[j] for o in ORDERS) for j in range(3))
          + tuple(tuple(o[a] + o[b] for o in ORDERS) for a, b in ((0, 1), (0, 2), (1, 2))) + ((7,) * 3,))
BACK = {key: slot for slot, key in enumerate(
    [(0, 0, 0), (0, 0, 1)] + [(0, k, dc) for k in (3, 1, 2) for dc in (1, 0)] + [(1, k, dc) for k in (3, 1, 2, 0) for dc in (1, 0)])}
COUNT_BASE = 32.0


def dot(a, b, dims=((1,), (0,))):
    return lax.dot_general(a, b, (dims, ((), ())), preferred_element_type=F32)


def step_kernel(nb, classes, f_in, cpad,
                a_hbm, x_hbm, w1_hbm, w2_hbm, lab_hbm, msk_hbm,
                loss_hbm, o1_hbm, o2_hbm,
                abuf, xg, y1, z1, h1t, y2g, z2, g2,
                xraw, w1raw, w2raw, lab_ref, msk_ref, w1t_ref, w2_ref, w2t_ref, w1f, w2f,
                p2out, p2sib, p2sum, p2fwd, p2far, d2, g1,
                p6out, p6sib, p6sum, p6fwd, p6far,
                part1, part2, rb1, rbc, rbz, sumc, sumz, res1, res2, loss_ref, o1_ref, o2_ref,
                asem, psem, osem, ssem, rsem):
    r = lax.axis_index("rep")
    n = lax.axis_index("nodes")
    core = n % 2
    xc = (n // 2) % 2
    yc = n // 4
    hid = z1.shape[1]
    fpad = xg.shape[1]

    def flip(v, f):
        return 1 - v if f else v

    def coords(k, dc):
        rr = flip(r, k // 4)
        nn = flip(yc, (k // 2) % 2) * 4 + flip(xc, k % 2) * 2 + flip(core, dc)
        return rr, nn

    def block_id(k, dc):
        rr, nn = coords(k, dc)
        return nn * 2 + rr

    used = {"send": 0, "recv": 0}
    drains = []

    def new(kind):
        used[kind] += 1
        return used[kind] - 1

    def prepare(src, dst, k, dc, ss, rs):
        return pltpu.make_async_remote_copy(
            src_ref=src, dst_ref=dst, send_sem=ssem.at[ss], recv_sem=rsem.at[rs],
            device_id=coords(k, dc), device_id_type=pl.DeviceIdType.MESH)

    def send(*args):
        prepare(*args).start()

    def landed(ref, rs):
        pltpu.make_async_copy(ref, ref, rsem.at[rs]).wait()

    def drain(ref, ss):
        drains.append((ref, ss))

    peers = [(k, dc) for k in (7, 3, 5, 6, 1, 2, 4, 0) for dc in range(2) if (k, dc) != (0, 0)]

    pre = [pltpu.make_async_copy(src, dst, psem.at[i]) for i, (src, dst) in enumerate(
        ((x_hbm, xraw), (msk_hbm, msk_ref), (w1_hbm, w1raw), (w2_hbm, w2raw), (lab_hbm, lab_ref)))]
    for cp in pre:
        cp.start()
    barrier = pltpu.get_barrier_semaphore()
    near_peers = ((0, 1), (1, 0), (2, 0), (4, 0))
    for k, dc in near_peers:
        pl.semaphore_signal(barrier, inc=1, device_id=coords(k, dc), device_id_type=pl.DeviceIdType.MESH)
    z1[...] = jnp.zeros_like(z1)
    z2[...] = jnp.zeros_like(z2)
    part1[...] = jnp.zeros_like(part1)
    part2[...] = jnp.zeros_like(part2)
    w1f[...] = jnp.zeros_like(w1f)
    w2f[...] = jnp.zeros_like(w2f)
    xg[0] = jnp.zeros((fpad, nb), BF16)
    with scope("entry_x"):
        pre[0].wait()
        pre[1].wait()

    third = (nb // 3 // 128 + 1) * 128
    cuts = [slice(0, third), slice(third, 2 * third), slice(2 * third, nb)]

    def a_load(rows, k, dc, slot, cut=slice(0, nb)):
        row = pl.multiple_of(rows * nb, nb)
        col = pl.multiple_of(block_id(k, dc) * nb + cut.start, 128)
        size = cut.stop - cut.start
        pltpu.make_async_copy(a_hbm.at[pl.ds(row, nb), pl.ds(col, size)], abuf.at[slot, :, cut], asem.at[(slot + 1) // 2]).start()

    def a_wait(base, count, sem):
        pltpu.make_async_copy(a_hbm.at[pl.ds(0, count * nb), pl.ds(0, nb)], a_hbm.at[pl.ds(0, count * nb), pl.ds(0, nb)], asem.at[sem]).wait()

    for slot in range(16):
        t, dc = slot // 2, slot % 2
        if t in (0, 7):
            a_load(r, STAGES[t][0], dc, slot)
        else:
            for p in range(3):
                a_load(r, STAGES[t][p], dc, slot, cuts[p])

    xg[0, 0:f_in, :] = xraw[...]
    count = jnp.sum(msk_ref[...].astype(F32), axis=1, keepdims=True)
    hi = jnp.floor(count * (1.0 / COUNT_BASE))
    lo = count - COUNT_BASE * hi
    row16 = lax.broadcasted_iota(jnp.int32, (16, 128), 0) + (fpad - 16)
    tail = xg[0, fpad - 16:fpad, 0:128].astype(F32)
    tail = jnp.where(row16 == f_in, hi, jnp.where(row16 == f_in + 1, lo, tail))
    xg[0, fpad - 16:fpad, 0:128] = tail.astype(BF16)
    with scope("entry_w"):
        for cp in pre[2:]:
            cp.wait()
    w1f[0:f_in, :] = w1raw[...]
    w1t_ref[...] = w1f[...].T[:, 0:fpad].astype(BF16)
    w2f[0:classes, :] = w2raw[...]
    w2t_ref[...] = w2f[0:cpad, :].astype(BF16)
    w2_ref[...] = w2f[...].T[:, 0:cpad].astype(BF16)
    with scope("entry_barrier"):
        pl.semaphore_wait(barrier, len(near_peers))

    def gather(buf, work, event):
        ss = new("send")
        on = [new("recv") for _ in STAGES]
        ons = [new("recv") for _ in STAGES]

        def piece(slot, p):
            return buf.at[slot, :, cuts[p]]

        for j in range(3):
            for p, order in enumerate(ORDERS):
                send(piece(0, p), piece(2 * (1 + j), p), order[j], 0, ss, on[1 + j])
        sib = [prepare(buf.at[2 * t], buf.at[2 * t + 1], 0, 1, ss, ons[t]) for t in range(8)]
        sib[0].start()
        hops = {1: ((4, 1), (5, 2)), 2: ((6, 2),), 4: ((7, 2),)}
        onward = {t: [prepare(piece(2 * t, p), piece(2 * to, p), order[d], 0, ss, on[to]) for to, d in nxt for p, order in enumerate(ORDERS)]
                  for t, nxt in hops.items()}
        drain(buf.at[pl.ds(0, 15)], ss)
        work(0, 1)

        @pl.loop(1, 8)
        def _(t):
            for u in range(1, 8):
                @pl.when(t == u)
                def _():
                    with scope(f"ev{u}"):
                        landed(buf.at[0], on[u])
                        for cp in onward.get(u, ()):
                            cp.start()
                        sib[u].start()
                        event(u)
                        landed(buf.at[0], ons[u - 1])
            with scope("pair"):
                work(2 * t - 1, 2)
        event(8)
        with scope("ev8"):
            landed(buf.at[0], ons[7])
        work(15, 1)
        event(9)

    mrows = nb // 2

    def z1_work(base, count):
        a_wait(base, count, (base + 1) // 2)
        for j in range(count):
            y1[j] = dot(w1t_ref[...], xg[base + j]).astype(BF16)
        for m in range(0, nb, mrows):
            z1[m:m + mrows, :] += sum(dot(abuf[base + j, m:m + mrows, :], y1[j], ((1,), (1,))) for j in range(count))

    gather(xg, z1_work, lambda t: None)

    with scope("h1y2"):
        for m in range(0, nb, 256):
            h1t[0, :, m:m + 256] = jnp.maximum(z1[m:m + 256, :], 0.0).T.astype(BF16)
        y2g[0] = dot(w2t_ref[...], h1t[0]).astype(BF16)

    def z2_work(base, count):
        for m in range(0, nb, mrows):
            z2[m:m + mrows, 0:cpad] += sum(dot(abuf[base + j, m:m + mrows, :], y2g[base + j], ((1,), (1,))) for j in range(count))

    chunk = hid // 4
    h1t_ss, h1t_rs = new("send"), new("recv")
    h1t_cps = [prepare(h1t.at[0, pl.ds(i * chunk, chunk)], h1t.at[1, pl.ds(i * chunk, chunk)], 4, 0, h1t_ss, h1t_rs) for i in range(4)]
    drain(h1t.at[0], h1t_ss)

    def z2_event(t):
        for (which, k, dc), slot in BACK.items():
            if slot > 1 and (slot + 1) // 2 == t - 1:
                a_load(flip(r, which), k, dc, slot)
        if t == 5:
            h1t_cps[0].start()

    gather(y2g, z2_work, z2_event)

    tails = xg[0, fpad - 16:fpad, 0:128].astype(F32)
    for s in range(1, 16):
        tails = tails + xg[s, fpad - 16:fpad, 0:128].astype(F32)
    at_hi = f_in - (fpad - 16)
    total_m = COUNT_BASE * tails[at_hi:at_hi + 1, 0:1] + tails[at_hi + 1:at_hi + 2, 0:1]
    z2t = z2[...].T[0:cpad, :]
    cls = lax.broadcasted_iota(jnp.int32, (cpad, nb), 0)
    zm = jnp.where(cls < classes, z2t, -jnp.inf)
    zs = zm - jnp.max(zm, axis=0, keepdims=True)
    logp = zs - jnp.log(jnp.sum(jnp.exp(zs), axis=0, keepdims=True))
    hot = cls == lab_ref[...]
    mask_f = msk_ref[...].astype(F32)
    loss_v = -mask_f * jnp.sum(jnp.where(hot, logp, 0.0), axis=0, keepdims=True)
    loss_part = jnp.sum(loss_v, axis=1, keepdims=True) / total_m
    g2[0] = ((jnp.exp(logp) - hot.astype(F32)) * (mask_f / total_m)).astype(BF16)
    g2_rs, g2_ss = new("recv"), new("send")
    send(g2.at[0], g2.at[1], 4, 0, g2_ss, g2_rs)
    drain(g2.at[0], g2_ss)
    for cp in h1t_cps[1:]:
        cp.start()

    half = nb // 2
    units = ((3, 0), (3, 1), (1, 0), (2, 1), (2, 0), (1, 1), (0, 0), (0, 1))

    def tree(name, g, out, sibb, summ, rfwd, rfar, early):
        sib_ss, ss = new("send"), new("send")
        sib_rs = [new("recv") for _ in range(5)]
        f_rs = [new("recv") for _ in range(2)]
        x_rs = new("recv")
        y_rs = [new("recv") for _ in range(2)]
        drain(out, sib_ss)
        drain(summ.at[pl.ds(0, 6)], ss)

        def cols(h):
            return slice(h * half, (h + 1) * half)

        def own(q, h, dc):
            return dot(g[0], abuf[BACK[0, q, dc], :, cols(h)])

        def partner(q, h, dc):
            return dot(g[1], abuf[BACK[1, q, dc], :, cols(h)])

        def first_dim(h):
            return 1 if h == 0 else 2

        def begin():
            for i in range(early):
                out[i] = own(*units[i], 1)
                summ[i] = own(*units[i], 0)

        def finish(i):
            q, h = units[i]
            with scope(name + "_sib"):
                if i < 2:
                    landed(sibb.at[i], sib_rs[i])
                elif i % 2 == 0:
                    landed(sibb.at[pl.ds(i, 2)], sib_rs[1 + i // 2])
            summ[i] += sibb[i]
            if q == 3:
                send(summ.at[i], rfwd.at[h], first_dim(h), 0, ss, f_rs[h])
            elif q == first_dim(h):
                send(summ.at[i], rfar.at[h], first_dim(h), 0, ss, x_rs)

        def group(j):
            pair = (2 * j, 2 * j + 1)
            with scope(name + "_group"):
                for i in pair:
                    if i < early:
                        out[i] += partner(*units[i], 1)
                    else:
                        out[i] = own(*units[i], 1) + partner(*units[i], 1)
                    send(out.at[i], sibb.at[i], 0, 1, sib_ss, sib_rs[i if i < 2 else 1 + i // 2])
                for i in pair:
                    if i < early:
                        summ[i] += partner(*units[i], 0)
                    else:
                        summ[i] = own(*units[i], 0) + partner(*units[i], 0)
            return lambda: [finish(i) for i in pair]

        def forward():
            for h, i in ((0, 4), (1, 5)):
                with scope(name + "_fwait"):
                    landed(rfwd.at[h], f_rs[h])
                summ[i] += rfwd[h]
                for c in range(2):
                    part = (slice(None), slice(c * half // 2, (c + 1) * half // 2))
                    send(summ.at[(i,) + part], rfar.at[(2 + h,) + part], 3 - first_dim(h), 0, ss, y_rs[c])

        def collect():
            with scope(name + "_xwait"):
                landed(rfar.at[pl.ds(0, 2)], x_rs)
            for h in (0, 1):
                summ[6 + h] += rfar[h]

        def last(h, c):
            if h == 0:
                with scope(name + "_ywait"):
                    landed(rfar.at[0], y_rs[c])
            part = (slice(None), slice(c * half // 2, (c + 1) * half // 2))
            return (summ[(6 + h,) + part] + rfar[(2 + h,) + part]).astype(BF16)

        return begin, group, forward, collect, last

    begin, group, forward, collect, last = tree("p2", g2, p2out, p2sib, p2sum, p2fwd, p2far, 8)
    with scope("p2own"):
        for sem in range(1, 5):
            a_wait(0, 1 if sem == 1 else 2, sem)
        begin()
    with scope("g2z_wait"):
        landed(g2.at[1], g2_rs)
        for sem in range(5, 9):
            a_wait(0, 1 if sem == 8 else 2, sem)
    for j in range(3):
        group(j)()
    forward()
    group(3)()
    collect()
    quarters = [(h, c, slice(h * half + c * half // 2, h * half + (c + 1) * half // 2)) for c in (0, 1) for h in (0, 1)]
    d2_rs, d2_ss = new("recv"), new("send")
    for h, c, at in quarters:
        d2[0, :, at] = last(h, c)
        send(d2.at[0, :, at], d2.at[1, :, at], 4, 0, d2_ss, d2_rs)
    drain(d2.at[0], d2_ss)

    def g1_of(i):
        g1[i] = jnp.where(h1t[i] > 0, dot(w2_ref[...], d2[i]), 0.0).astype(BF16)

    lane = lax.broadcasted_iota(jnp.int32, (hid, cpad), 1)
    dw2 = dot(h1t[0], d2[0], ((1,), (1,)))
    part2[:, 0:cpad] = jnp.where(lane == classes, loss_part, dw2)
    hc, hz = hid // 2, hid // 4

    def span(start, size):
        return pl.ds(pl.multiple_of(start, size), size)

    w_ss = new("send")
    w_rs = [new("recv") for _ in range(6)]
    drain(p6out.at[0, :, 0:2 * res2.shape[1]], w_ss)
    send(part2.at[span((1 - core) * hc, hc)], rbc, 0, 1, w_ss, w_rs[0])
    g1_of(0)

    begin, group, forward, collect, last = tree("p6", g1, p6out, p6sib, p6sum, p6fwd, p6far, 2)
    with scope("p6own"):
        begin()
    landed(rbc, w_rs[0])
    sumc[...] = part2[span(core * hc, hc), :] + rbc[...]
    send(sumc.at[span((1 - r) * hz, hz)], rbz.at[0], 4, 0, w_ss, w_rs[1])
    with scope("d2z_wait"):
        landed(h1t.at[1], h1t_rs)
        landed(d2.at[1], d2_rs)
    with scope("g1b"):
        g1_of(1)
    fin0 = group(0)
    landed(rbz.at[0], w_rs[1])
    sumz[0] = sumc[span(r * hz, hz), :] + rbz[0]
    send(sumz.at[0], rbz.at[1], 1, 0, w_ss, w_rs[2])
    fin0()
    fin1 = group(1)
    landed(rbz.at[1], w_rs[2])
    sumz[1] = sumz[0] + rbz[1]
    send(sumz.at[1], rbz.at[2], 2, 0, w_ss, w_rs[3])
    fin1()
    group(2)()
    forward()
    group(3)()
    collect()
    mine = span(core * hc + r * hz, hz)
    landed(rbz.at[2], w_rs[3])
    res2[mine, :] = sumz[1] + rbz[2]
    send(res2.at[mine], res2.at[mine], 4, 0, w_ss, w_rs[4])
    landed(rbz.at[0], w_rs[4])
    mine = span(core * hc, hc)
    send(res2.at[mine], res2.at[mine], 0, 1, w_ss, w_rs[5])
    landed(rbc, w_rs[5])
    o2_ref[...] = res2[...].T[0:classes, :]
    loss_ref[...] = res2[0:1, classes:classes + 1]
    outs = [pltpu.make_async_copy(src, dst, osem.at[i]) for i, (src, dst) in enumerate(
        ((loss_ref, loss_hbm), (o2_ref, o2_hbm), (o1_ref, o1_hbm)))]
    outs[0].start()
    outs[1].start()

    rows = hid // 16

    acc = None
    for h, c, at in quarters:
        term = dot(last(h, c), xg[0, :, at], ((1,), (1,)))
        acc = term if acc is None else acc + term
    part1[:, 0:fpad] = acc
    red_ss = [new("send") for _ in range(2)]
    red_rs = [new("recv") for _ in range(2)]
    with scope("red1"):
        for i, (k, dc) in enumerate(peers):
            send(part1.at[span(block_id(k, dc) * rows, rows)], rb1.at[i], k, dc, red_ss[0], red_rs[0])
        mine = span(block_id(0, 0) * rows, rows)
        landed(rb1, red_rs[0])
        res1[mine, :] = part1[mine, :] + sum(rb1[i] for i in range(len(peers)))
        for k, dc in peers:
            send(res1.at[mine], res1.at[mine], k, dc, red_ss[1], red_rs[1])
    with scope("out1_wait"):
        landed(rb1, red_rs[1])
    drain(rb1, red_ss[0])
    drain(rb1, red_ss[1])
    o1_ref[...] = res1[...].T[0:f_in, :]
    outs[2].start()
    with scope("send_wait"):
        for ref, ss in drains:
            pltpu.make_async_copy(ref, ref, ssem.at[ss]).wait()
        for cp in outs:
            cp.wait()
    assert used == {"send": ssem.shape[0], "recv": rsem.shape[0]}, used


def solution(mesh):
    def local_step(adj_rows, features, w_one, w_two, labels, label_mask):
        nb, f_in = features.shape
        total = adj_rows.shape[1]
        hid, classes = w_two.shape
        cpad = 48
        lanes = 128
        fpad = 112
        half = nb // 2
        nsend, nrecv = 12, 63
        anyspec = pl.BlockSpec(memory_space=pl.ANY)
        V = pltpu.VMEM
        loss, dw1, dw2 = pl.pallas_call(
            functools.partial(step_kernel, nb, classes, f_in, cpad),
            out_shape=[jax.ShapeDtypeStruct((1, 1), F32), jax.ShapeDtypeStruct((f_in, hid), F32),
                       jax.ShapeDtypeStruct((classes, hid), F32)],
            in_specs=[anyspec] * 6,
            out_specs=[anyspec] * 3,
            scratch_shapes=[
                V((total // nb, nb, nb), BF16), V((16, fpad, nb), BF16), V((2, hid, nb), BF16),
                V((nb, hid), F32), V((2, hid, nb), BF16), V((16, cpad, nb), BF16), V((nb, lanes), F32), V((2, cpad, nb), BF16),
                V((f_in, nb), BF16), V((f_in, hid), F32), V((classes, hid), F32), V((1, nb), jnp.int32), V((1, nb), jnp.int32),
                V((hid, fpad), BF16), V((hid, cpad), BF16), V((cpad, hid), BF16), V((lanes, hid), F32), V((lanes, hid), F32),
                V((8, cpad, half), F32), V((8, cpad, half), F32), V((8, cpad, half), F32), V((2, cpad, half), F32), V((4, cpad, half), F32),
                V((2, cpad, nb), BF16), V((2, hid, nb), BF16),
                V((8, hid, half), F32), V((8, hid, half), F32), V((8, hid, half), F32),
                V((2, hid, half), F32), V((4, hid, half), F32),
                V((hid, lanes), F32), V((hid, lanes), F32), V((15, hid // 16, lanes), F32), V((hid // 2, lanes), F32),
                V((3, hid // 4, lanes), F32), V((hid // 2, lanes), F32), V((2, hid // 4, lanes), F32),
                V((hid, lanes), F32), V((hid, lanes), F32), V((1, 1), F32), V((f_in, hid), F32), V((classes, hid), F32),
                pltpu.SemaphoreType.DMA((9,)), pltpu.SemaphoreType.DMA((5,)), pltpu.SemaphoreType.DMA((3,)),
                pltpu.SemaphoreType.DMA((nsend,)), pltpu.SemaphoreType.DMA((nrecv,)),
            ],
            compiler_params=pltpu.CompilerParams(collective_id=0, has_side_effects=True, vmem_limit_bytes=67043328),
            name="gcn_step",
        )(adj_rows, features.T, w_one, w_two.T, labels.reshape(1, nb), label_mask.reshape(1, nb))
        return loss.reshape(()), dw1, dw2.T

    row_spec = P(("nodes", "rep"))
    return jax.shard_map(local_step, mesh=mesh, in_specs=(P("nodes", None), P(("nodes", "rep"), None), P(), P(), row_spec, row_spec), out_specs=(P(), P(), P()), check_vma=False)
```

```python
import functools

import jax
import jax.numpy as jnp
from jax import lax
from jax.experimental import pallas as pl
from jax.experimental.pallas import tpu as pltpu
from jax.sharding import PartitionSpec as P

BF16 = jnp.bfloat16
F32 = jnp.float32
scope = jax.named_scope

ORDERS = ((1, 2, 4), (2, 4, 1), (4, 1, 2))
STAGES = (((0,) * 3,) + tuple(tuple(o[j] for o in ORDERS) for j in range(3))
          + tuple(tuple(o[a] + o[b] for o in ORDERS) for a, b in ((0, 1), (0, 2), (1, 2))) + ((7,) * 3,))
BACK = {key: slot for slot, key in enumerate(
    [(0, 0, 0), (0, 0, 1)] + [(0, k, dc) for k in (3, 1, 2) for dc in (1, 0)] + [(1, k, dc) for k in (3, 1, 2, 0) for dc in (1, 0)])}
COUNT_BASE = 32.0


def dot(a, b, dims=((1,), (0,))):
    return lax.dot_general(a, b, (dims, ((), ())), preferred_element_type=F32)


def step_kernel(nb, classes, f_in, cpad,
                a_hbm, x_hbm, w1_hbm, w2_hbm, lab_hbm, msk_hbm,
                loss_hbm, o1_hbm, o2_hbm,
                abuf, xg, y1, z1, h1t, y2g, z2, g2,
                xraw, w1raw, w2raw, lab_ref, msk_ref, w1t_ref, w2_ref, w2t_ref, w1f, w2f,
                p2out, p2sib, p2sum, p2fwd, p2far, d2, g1,
                p6out, p6sib, p6sum, p6fwd, p6far,
                part1, part2, rb1, rbc, rbz, sumc, sumz, res1, res2, loss_ref, o1_ref, o2_ref,
                asem, psem, osem, ssem, rsem):
    r = lax.axis_index("rep")
    n = lax.axis_index("nodes")
    core = n % 2
    xc = (n // 2) % 2
    yc = n // 4
    hid = z1.shape[1]
    fpad = xg.shape[1]

    def flip(v, f):
        return 1 - v if f else v

    def coords(k, dc):
        rr = flip(r, k // 4)
        nn = flip(yc, (k // 2) % 2) * 4 + flip(xc, k % 2) * 2 + flip(core, dc)
        return rr, nn

    def block_id(k, dc):
        rr, nn = coords(k, dc)
        return nn * 2 + rr

    used = {"send": 0, "recv": 0}
    drains = []

    def new(kind):
        used[kind] += 1
        return used[kind] - 1

    def prepare(src, dst, k, dc, ss, rs):
        return pltpu.make_async_remote_copy(
            src_ref=src, dst_ref=dst, send_sem=ssem.at[ss], recv_sem=rsem.at[rs],
            device_id=coords(k, dc), device_id_type=pl.DeviceIdType.MESH)

    def send(*args):
        prepare(*args).start()

    def landed(ref, rs):
        pltpu.make_async_copy(ref, ref, rsem.at[rs]).wait()

    def drain(ref, ss):
        drains.append((ref, ss))

    peers = [(k, dc) for k in (7, 3, 5, 6, 1, 2, 4, 0) for dc in range(2) if (k, dc) != (0, 0)]

    pre = [pltpu.make_async_copy(src, dst, psem.at[i]) for i, (src, dst) in enumerate(
        ((x_hbm, xraw), (msk_hbm, msk_ref), (w1_hbm, w1raw), (w2_hbm, w2raw), (lab_hbm, lab_ref)))]
    for cp in pre:
        cp.start()
    barrier = pltpu.get_barrier_semaphore()
    near_peers = ((0, 1), (1, 0), (2, 0), (4, 0))
    for k, dc in near_peers:
        pl.semaphore_signal(barrier, inc=1, device_id=coords(k, dc), device_id_type=pl.DeviceIdType.MESH)
    z1[...] = jnp.zeros_like(z1)
    z2[...] = jnp.zeros_like(z2)
    part1[...] = jnp.zeros_like(part1)
    part2[...] = jnp.zeros_like(part2)
    w1f[...] = jnp.zeros_like(w1f)
    w2f[...] = jnp.zeros_like(w2f)
    xg[0] = jnp.zeros((fpad, nb), BF16)
    with scope("entry_x"):
        pre[0].wait()
        pre[1].wait()

    third = (nb // 3 // 128 + 1) * 128
    cuts = [slice(0, third), slice(third, 2 * third), slice(2 * third, nb)]

    def a_load(rows, k, dc, slot, cut=slice(0, nb)):
        row = pl.multiple_of(rows * nb, nb)
        col = pl.multiple_of(block_id(k, dc) * nb + cut.start, 128)
        size = cut.stop - cut.start
        pltpu.make_async_copy(a_hbm.at[pl.ds(row, nb), pl.ds(col, size)], abuf.at[slot, :, cut], asem.at[0 if slot < 2 else (slot + 1) // 2]).start()

    def a_wait(base, count, sem):
        pltpu.make_async_copy(a_hbm.at[pl.ds(0, count * nb), pl.ds(0, nb)], a_hbm.at[pl.ds(0, count * nb), pl.ds(0, nb)], asem.at[sem]).wait()

    for slot in range(16):
        t, dc = slot // 2, slot % 2
        if t in (0, 7):
            a_load(r, STAGES[t][0], dc, slot)
        else:
            for p in range(3):
                a_load(r, STAGES[t][p], dc, slot, cuts[p])

    xg[0, 0:f_in, :] = xraw[...]
    count = jnp.sum(msk_ref[...].astype(F32), axis=1, keepdims=True)
    hi = jnp.floor(count * (1.0 / COUNT_BASE))
    lo = count - COUNT_BASE * hi
    row16 = lax.broadcasted_iota(jnp.int32, (16, 128), 0) + (fpad - 16)
    tail = xg[0, fpad - 16:fpad, 0:128].astype(F32)
    tail = jnp.where(row16 == f_in, hi, jnp.where(row16 == f_in + 1, lo, tail))
    xg[0, fpad - 16:fpad, 0:128] = tail.astype(BF16)
    with scope("entry_w"):
        for cp in pre[2:]:
            cp.wait()
    w1f[0:f_in, :] = w1raw[...]
    w1t_ref[...] = w1f[...].T[:, 0:fpad].astype(BF16)
    w2f[0:classes, :] = w2raw[...]
    w2t_ref[...] = w2f[0:cpad, :].astype(BF16)
    w2_ref[...] = w2f[...].T[:, 0:cpad].astype(BF16)
    with scope("entry_barrier"):
        pl.semaphore_wait(barrier, len(near_peers))

    def gather(buf, work, event):
        ss = new("send")
        on = [new("recv") for _ in STAGES]
        ons = [new("recv") for _ in STAGES]

        def piece(slot, p):
            return buf.at[slot, :, cuts[p]]

        for j in range(3):
            for p, order in enumerate(ORDERS):
                send(piece(0, p), piece(2 * (1 + j), p), order[j], 0, ss, on[1 + j])
        sib = [prepare(buf.at[2 * t], buf.at[2 * t + 1], 0, 1, ss, ons[t]) for t in range(8)]
        sib[0].start()
        hops = {1: ((4, 1), (5, 2)), 2: ((6, 2),), 4: ((7, 2),)}
        onward = {t: [prepare(piece(2 * t, p), piece(2 * to, p), order[d], 0, ss, on[to]) for to, d in nxt for p, order in enumerate(ORDERS)]
                  for t, nxt in hops.items()}
        drain(buf.at[pl.ds(0, 15)], ss)

        def arrive(u):
            with scope(f"ev{u}"):
                landed(buf.at[0], on[u])
                for cp in onward.get(u, ()):
                    cp.start()
                sib[u].start()
                event(u)
                if u > 1:
                    landed(buf.at[0], ons[u - 1])

        with scope("ev0"):
            landed(buf.at[0], ons[0])
        work(0, 2)
        arrive(1)
        work(2, 1)

        @pl.loop(2, 8)
        def _(t):
            for u in range(2, 8):
                @pl.when(t == u)
                def _():
                    arrive(u)
            with scope("pair"):
                work(2 * t - 1, 2)
        event(8)
        with scope("ev8"):
            landed(buf.at[0], ons[7])
        work(15, 1)
        event(9)

    mrows = nb // 2

    def z1_work(base, count):
        a_wait(base, count, 0 if isinstance(base, int) and base == 0 else (base + 1) // 2)
        for j in range(count):
            y1[j] = dot(w1t_ref[...], xg[base + j]).astype(BF16)
        for m in range(0, nb, mrows):
            z1[m:m + mrows, :] += sum(dot(abuf[base + j, m:m + mrows, :], y1[j], ((1,), (1,))) for j in range(count))

    gather(xg, z1_work, lambda t: None)

    with scope("h1y2"):
        for m in range(0, nb, 256):
            h1t[0, :, m:m + 256] = jnp.maximum(z1[m:m + 256, :], 0.0).T.astype(BF16)
        y2g[0] = dot(w2t_ref[...], h1t[0]).astype(BF16)

    def z2_work(base, count):
        for m in range(0, nb, mrows):
            z2[m:m + mrows, 0:cpad] += sum(dot(abuf[base + j, m:m + mrows, :], y2g[base + j], ((1,), (1,))) for j in range(count))

    chunk = hid // 4
    h1t_ss, h1t_rs = new("send"), new("recv")
    h1t_cps = [prepare(h1t.at[0, pl.ds(i * chunk, chunk)], h1t.at[1, pl.ds(i * chunk, chunk)], 4, 0, h1t_ss, h1t_rs) for i in range(4)]
    drain(h1t.at[0], h1t_ss)

    def z2_event(t):
        for (which, k, dc), slot in BACK.items():
            if slot > 1 and (slot + 1) // 2 == t - 1:
                a_load(flip(r, which), k, dc, slot)
        if t == 5:
            h1t_cps[0].start()

    gather(y2g, z2_work, z2_event)

    tails = xg[0, fpad - 16:fpad, 0:128].astype(F32)
    for s in range(1, 16):
        tails = tails + xg[s, fpad - 16:fpad, 0:128].astype(F32)
    at_hi = f_in - (fpad - 16)
    total_m = COUNT_BASE * tails[at_hi:at_hi + 1, 0:1] + tails[at_hi + 1:at_hi + 2, 0:1]
    z2t = z2[...].T[0:cpad, :]
    cls = lax.broadcasted_iota(jnp.int32, (cpad, nb), 0)
    zm = jnp.where(cls < classes, z2t, -jnp.inf)
    zs = zm - jnp.max(zm, axis=0, keepdims=True)
    logp = zs - jnp.log(jnp.sum(jnp.exp(zs), axis=0, keepdims=True))
    hot = cls == lab_ref[...]
    mask_f = msk_ref[...].astype(F32)
    loss_v = -mask_f * jnp.sum(jnp.where(hot, logp, 0.0), axis=0, keepdims=True)
    loss_part = jnp.sum(loss_v, axis=1, keepdims=True) / total_m
    g2[0] = ((jnp.exp(logp) - hot.astype(F32)) * (mask_f / total_m)).astype(BF16)
    g2_rs, g2_ss = new("recv"), new("send")
    send(g2.at[0], g2.at[1], 4, 0, g2_ss, g2_rs)
    drain(g2.at[0], g2_ss)
    for cp in h1t_cps[1:]:
        cp.start()

    half = nb // 2
    units = ((3, 0), (3, 1), (1, 0), (2, 1), (2, 0), (1, 1), (0, 0), (0, 1))

    def tree(name, g, out, sibb, summ, rfwd, rfar, early):
        sib_ss, ss = new("send"), new("send")
        sib_rs = [new("recv") for _ in range(3)]
        sibf_rs = {(h, c): new("recv") for h in range(2) for c in range(2)}
        f_rs = {(h, c): new("recv") for h in range(2) for c in range(2)}
        x_rs = new("recv")
        y_rs = [new("recv") for _ in range(2)]
        drain(out, sib_ss)
        drain(summ.at[pl.ds(0, 6)], ss)

        def cols(h):
            return slice(h * half, (h + 1) * half)

        def own(q, h, dc):
            return dot(g[0], abuf[BACK[0, q, dc], :, cols(h)])

        def partner(q, h, dc):
            return dot(g[1], abuf[BACK[1, q, dc], :, cols(h)])

        def partner_piece(i, dc, c):
            q, h = units[i]
            lo = h * half + c * half // 2
            return dot(g[1], abuf[BACK[1, q, dc], :, lo:lo + half // 2])

        def piece(i, c):
            return (i, slice(None), slice(c * half // 2, (c + 1) * half // 2))

        def first_dim(h):
            return 1 if h == 0 else 2

        def begin():
            for i in range(early):
                out[i] = own(*units[i], 1)
                summ[i] = own(*units[i], 0)

        def first_group(between):
            with scope(name + "_group"):
                for c in range(2):
                    for i in range(2):
                        out[piece(i, c)] += partner_piece(i, 1, c)
                    for i in range(2):
                        send(out.at[piece(i, c)], sibb.at[piece(i, c)], 0, 1, sib_ss, sibf_rs[i, c])
                for i in range(2):
                    summ[i] += partner(*units[i], 0)
            for c in range(2):
                for i in range(2):
                    with scope(name + "_sib"):
                        landed(sibb.at[piece(i, c)], sibf_rs[i, c])
                    summ[piece(i, c)] += sibb[piece(i, c)]
                    send(summ.at[piece(i, c)], rfwd.at[piece(i, c)], first_dim(i), 0, ss, f_rs[i, c])
                if c == 0:
                    between()

        def group(j):
            pair = (2 * j, 2 * j + 1)
            with scope(name + "_group"):
                for i in pair:
                    if i < early:
                        out[i] += partner(*units[i], 1)
                    else:
                        out[i] = own(*units[i], 1) + partner(*units[i], 1)
                for i in pair:
                    send(out.at[i], sibb.at[i], 0, 1, sib_ss, sib_rs[j - 1])
                for i in pair:
                    if i < early:
                        summ[i] += partner(*units[i], 0)
                    else:
                        summ[i] = own(*units[i], 0) + partner(*units[i], 0)
            with scope(name + "_sib"):
                landed(sibb.at[pl.ds(2 * j, 2)], sib_rs[j - 1])
            for i in pair:
                q, h = units[i]
                summ[i] += sibb[i]
                if q == first_dim(h):
                    send(summ.at[i], rfar.at[h], first_dim(h), 0, ss, x_rs)

        def forward():
            for c in range(2):
                for h in range(2):
                    with scope(name + "_fwait"):
                        landed(rfwd.at[piece(h, c)], f_rs[h, c])
                    summ[piece(4 + h, c)] += rfwd[piece(h, c)]
                    send(summ.at[piece(4 + h, c)], rfar.at[piece(2 + h, c)], 3 - first_dim(h), 0, ss, y_rs[c])

        def collect():
            with scope(name + "_xwait"):
                landed(rfar.at[pl.ds(0, 2)], x_rs)
            for h in (0, 1):
                summ[6 + h] += rfar[h]

        def last(h, c):
            if h == 0:
                with scope(name + "_ywait"):
                    landed(rfar.at[0], y_rs[c])
            return (summ[piece(6 + h, c)] + rfar[piece(2 + h, c)]).astype(BF16)

        return begin, first_group, group, forward, collect, last

    begin, first_group, group, forward, collect, last = tree("p2", g2, p2out, p2sib, p2sum, p2fwd, p2far, 8)
    with scope("p2own"):
        for sem in range(1, 5):
            a_wait(0, 1 if sem == 1 else 2, sem)
        begin()
    with scope("g2z_wait"):
        landed(g2.at[1], g2_rs)
        for sem in range(5, 9):
            a_wait(0, 1 if sem == 8 else 2, sem)
    first_group(lambda: None)
    group(1)
    group(2)
    forward()
    group(3)
    collect()
    quarters = [(h, c, slice(h * half + c * half // 2, h * half + (c + 1) * half // 2)) for c in (0, 1) for h in (0, 1)]
    d2_rs, d2_ss = new("recv"), new("send")
    for h, c, at in quarters:
        d2[0, :, at] = last(h, c)
        send(d2.at[0, :, at], d2.at[1, :, at], 4, 0, d2_ss, d2_rs)
    drain(d2.at[0], d2_ss)

    def g1_of(i):
        g1[i] = jnp.where(h1t[i] > 0, dot(w2_ref[...], d2[i]), 0.0).astype(BF16)

    lane = lax.broadcasted_iota(jnp.int32, (hid, cpad), 1)
    dw2 = dot(h1t[0], d2[0], ((1,), (1,)))
    part2[:, 0:cpad] = jnp.where(lane == classes, loss_part, dw2)
    hc, hz = hid // 2, hid // 4

    def span(start, size):
        return pl.ds(pl.multiple_of(start, size), size)

    w_ss = new("send")
    w_rs = [new("recv") for _ in range(6)]
    drain(p6out.at[0, :, 0:2 * res2.shape[1]], w_ss)
    send(part2.at[span((1 - core) * hc, hc)], rbc, 0, 1, w_ss, w_rs[0])
    g1_of(0)

    begin, first_group, group, forward, collect, last = tree("p6", g1, p6out, p6sib, p6sum, p6fwd, p6far, 2)
    with scope("p6own"):
        begin()
    landed(rbc, w_rs[0])
    sumc[...] = part2[span(core * hc, hc), :] + rbc[...]
    send(sumc.at[span((1 - r) * hz, hz)], rbz.at[0], 4, 0, w_ss, w_rs[1])
    with scope("d2z_wait"):
        landed(h1t.at[1], h1t_rs)
        landed(d2.at[1], d2_rs)
    with scope("g1b"):
        g1_of(1)

    def exchange_x():
        landed(rbz.at[0], w_rs[1])
        sumz[0] = sumc[span(r * hz, hz), :] + rbz[0]
        send(sumz.at[0], rbz.at[1], 1, 0, w_ss, w_rs[2])

    first_group(exchange_x)
    group(1)
    group(2)
    with scope("exchange_y"):
        landed(rbz.at[1], w_rs[2])
    sumz[1] = sumz[0] + rbz[1]
    send(sumz.at[1], rbz.at[2], 2, 0, w_ss, w_rs[3])
    forward()
    group(3)
    collect()
    mine = span(core * hc + r * hz, hz)
    landed(rbz.at[2], w_rs[3])
    res2[mine, :] = sumz[1] + rbz[2]
    send(res2.at[mine], res2.at[mine], 4, 0, w_ss, w_rs[4])
    landed(rbz.at[0], w_rs[4])
    mine = span(core * hc, hc)
    send(res2.at[mine], res2.at[mine], 0, 1, w_ss, w_rs[5])
    landed(rbc, w_rs[5])
    o2_ref[...] = res2[...].T[0:classes, :]
    loss_ref[...] = res2[0:1, classes:classes + 1]
    outs = [pltpu.make_async_copy(src, dst, osem.at[i]) for i, (src, dst) in enumerate(
        ((loss_ref, loss_hbm), (o2_ref, o2_hbm), (o1_ref, o1_hbm)))]
    outs[0].start()
    outs[1].start()

    rows = hid // 16

    acc = None
    for h, c, at in quarters:
        term = dot(last(h, c), xg[0, :, at], ((1,), (1,)))
        acc = term if acc is None else acc + term
    part1[:, 0:fpad] = acc
    red_ss = [new("send") for _ in range(2)]
    red_rs = [new("recv") for _ in range(2)]
    with scope("red1"):
        for i, (k, dc) in enumerate(peers):
            send(part1.at[span(block_id(k, dc) * rows, rows)], rb1.at[i], k, dc, red_ss[0], red_rs[0])
        mine = span(block_id(0, 0) * rows, rows)
        landed(rb1, red_rs[0])
        res1[mine, :] = part1[mine, :] + sum(rb1[i] for i in range(len(peers)))
        for k, dc in peers:
            send(res1.at[mine], res1.at[mine], k, dc, red_ss[1], red_rs[1])
    with scope("out1_wait"):
        landed(rb1, red_rs[1])
    drain(rb1, red_ss[0])
    drain(rb1, red_ss[1])
    o1_ref[...] = res1[...].T[0:f_in, :]
    outs[2].start()
    with scope("send_wait"):
        for ref, ss in drains:
            pltpu.make_async_copy(ref, ref, ssem.at[ss]).wait()
        for cp in outs:
            cp.wait()
    assert used == {"send": ssem.shape[0], "recv": rsem.shape[0]}, used


def copy_kernel(*refs):
    for src, dst in zip(refs[:3], refs[3:]):
        dst[...] = src[...]


def solution(mesh):
    def local_step(adj_rows, features, w_one, w_two, labels, label_mask):
        nb, f_in = features.shape
        total = adj_rows.shape[1]
        hid, classes = w_two.shape
        cpad = 48
        lanes = 128
        fpad = 112
        half = nb // 2
        nsend, nrecv = 12, 71
        anyspec = pl.BlockSpec(memory_space=pl.ANY)
        V = pltpu.VMEM
        loss, dw1, dw2 = pl.pallas_call(
            functools.partial(step_kernel, nb, classes, f_in, cpad),
            out_shape=[jax.ShapeDtypeStruct((1, 1), F32), jax.ShapeDtypeStruct((f_in, hid), F32),
                       jax.ShapeDtypeStruct((classes, hid), F32)],
            in_specs=[anyspec] * 6,
            out_specs=[anyspec] * 3,
            scratch_shapes=[
                V((total // nb, nb, nb), BF16), V((16, fpad, nb), BF16), V((2, hid, nb), BF16),
                V((nb, hid), F32), V((2, hid, nb), BF16), V((16, cpad, nb), BF16), V((nb, lanes), F32), V((2, cpad, nb), BF16),
                V((f_in, nb), BF16), V((f_in, hid), F32), V((classes, hid), F32), V((1, nb), jnp.int32), V((1, nb), jnp.int32),
                V((hid, fpad), BF16), V((hid, cpad), BF16), V((cpad, hid), BF16), V((lanes, hid), F32), V((lanes, hid), F32),
                V((8, cpad, half), F32), V((8, cpad, half), F32), V((8, cpad, half), F32), V((2, cpad, half), F32), V((4, cpad, half), F32),
                V((2, cpad, nb), BF16), V((2, hid, nb), BF16),
                V((8, hid, half), F32), V((8, hid, half), F32), V((8, hid, half), F32),
                V((2, hid, half), F32), V((4, hid, half), F32),
                V((hid, lanes), F32), V((hid, lanes), F32), V((15, hid // 16, lanes), F32), V((hid // 2, lanes), F32),
                V((3, hid // 4, lanes), F32), V((hid // 2, lanes), F32), V((2, hid // 4, lanes), F32),
                V((hid, lanes), F32), V((hid, lanes), F32), V((1, 1), F32), V((f_in, hid), F32), V((classes, hid), F32),
                pltpu.SemaphoreType.DMA((9,)), pltpu.SemaphoreType.DMA((5,)), pltpu.SemaphoreType.DMA((3,)),
                pltpu.SemaphoreType.DMA((nsend,)), pltpu.SemaphoreType.DMA((nrecv,)),
            ],
            compiler_params=pltpu.CompilerParams(collective_id=0, has_side_effects=True, vmem_limit_bytes=67043328),
            name="gcn_step",
        )(adj_rows, features.T, w_one, w_two.T, labels.reshape(1, nb), label_mask.reshape(1, nb))
        loss, dw1, dw2 = pl.pallas_call(
            copy_kernel,
            out_shape=[jax.ShapeDtypeStruct(v.shape, F32) for v in (loss, dw1, dw2)],
            name="outputs",
        )(loss, dw1, dw2)
        return loss.reshape(()), dw1, dw2.T

    row_spec = P(("nodes", "rep"))
    return jax.shard_map(local_step, mesh=mesh, in_specs=(P("nodes", None), P(("nodes", "rep"), None), P(), P(), row_spec, row_spec), out_specs=(P(), P(), P()), check_vma=False)
```

```python
import functools

import jax
import jax.numpy as jnp
from jax import lax
from jax.experimental import pallas as pl
from jax.experimental.pallas import tpu as pltpu
from jax.sharding import PartitionSpec as P

BF16 = jnp.bfloat16
F32 = jnp.float32
scope = jax.named_scope

ORDERS = ((1, 2, 4), (2, 4, 1), (4, 1, 2))
STAGES = (((0,) * 3,) + tuple(tuple(o[j] for o in ORDERS) for j in range(3))
          + tuple(tuple(o[a] + o[b] for o in ORDERS) for a, b in ((0, 1), (0, 2), (1, 2))) + ((7,) * 3,))
BACK = {key: slot for slot, key in enumerate(
    [(0, 0, 0), (0, 0, 1)] + [(0, k, dc) for k in (3, 1, 2) for dc in (1, 0)] + [(1, k, dc) for k in (3, 1, 2, 0) for dc in (1, 0)])}
COUNT_BASE = 32.0


def dot(a, b, dims=((1,), (0,))):
    return lax.dot_general(a, b, (dims, ((), ())), preferred_element_type=F32)


def step_kernel(nb, classes, f_in, cpad,
                a_hbm, x_hbm, w1_hbm, w2_hbm, lab_hbm, msk_hbm,
                o1_hbm, o2_hbm,
                abuf, xg, y1, z1, h1t, y2g, z2, g2,
                xraw, w1raw, w2raw, lab_ref, msk_ref, w1t_ref, w2_ref, w2t_ref, w1f, w2f,
                p2out, p2sib, p2sum, p2fwd, p2far, d2, g1,
                p6out, p6sib, p6sum, p6fwd, p6far,
                part1, part2, rb1, rbc, rbz, sumc, sumz, res1, res2,
                asem, psem, osem, ssem, rsem):
    r = lax.axis_index("rep")
    n = lax.axis_index("nodes")
    core = n % 2
    xc = (n // 2) % 2
    yc = n // 4
    hid = z1.shape[1]
    fpad = xg.shape[1]

    def flip(v, f):
        return 1 - v if f else v

    def coords(k, dc):
        rr = flip(r, k // 4)
        nn = flip(yc, (k // 2) % 2) * 4 + flip(xc, k % 2) * 2 + flip(core, dc)
        return rr, nn

    def block_id(k, dc):
        rr, nn = coords(k, dc)
        return nn * 2 + rr

    used = {"send": 0, "recv": 0}
    drains = []

    def new(kind):
        used[kind] += 1
        return used[kind] - 1

    def prepare(src, dst, k, dc, ss, rs):
        return pltpu.make_async_remote_copy(
            src_ref=src, dst_ref=dst, send_sem=ssem.at[ss], recv_sem=rsem.at[rs],
            device_id=coords(k, dc), device_id_type=pl.DeviceIdType.MESH)

    def send(*args):
        prepare(*args).start()

    def landed(ref, rs):
        pltpu.make_async_copy(ref, ref, rsem.at[rs]).wait()

    def drain(ref, ss):
        drains.append((ref, ss))

    peers = [(k, dc) for k in (7, 3, 5, 6, 1, 2, 4, 0) for dc in range(2) if (k, dc) != (0, 0)]

    pre = [pltpu.make_async_copy(src, dst, psem.at[i]) for i, (src, dst) in enumerate(
        ((x_hbm, xraw), (msk_hbm, msk_ref), (w1_hbm, w1raw), (w2_hbm, w2raw), (lab_hbm, lab_ref)))]
    for cp in pre:
        cp.start()
    barrier = pltpu.get_barrier_semaphore()
    near_peers = ((0, 1), (1, 0), (2, 0), (4, 0))
    for k, dc in near_peers:
        pl.semaphore_signal(barrier, inc=1, device_id=coords(k, dc), device_id_type=pl.DeviceIdType.MESH)
    z1[...] = jnp.zeros_like(z1)
    z2[...] = jnp.zeros_like(z2)
    part1[...] = jnp.zeros_like(part1)
    w1f[...] = jnp.zeros_like(w1f)
    w2f[...] = jnp.zeros_like(w2f)
    xg[0] = jnp.zeros((fpad, nb), BF16)
    with scope("entry_x"):
        pre[0].wait()
        pre[1].wait()

    third = (nb // 3 // 128 + 1) * 128
    cuts = [slice(0, third), slice(third, 2 * third), slice(2 * third, nb)]

    def a_load(rows, k, dc, slot, cut=slice(0, nb)):
        row = pl.multiple_of(rows * nb, nb)
        col = pl.multiple_of(block_id(k, dc) * nb + cut.start, 128)
        size = cut.stop - cut.start
        pltpu.make_async_copy(a_hbm.at[pl.ds(row, nb), pl.ds(col, size)], abuf.at[slot, :, cut], asem.at[0 if slot < 2 else (slot + 1) // 2]).start()

    def a_wait(base, count, sem):
        pltpu.make_async_copy(a_hbm.at[pl.ds(0, count * nb), pl.ds(0, nb)], a_hbm.at[pl.ds(0, count * nb), pl.ds(0, nb)], asem.at[sem]).wait()

    for slot in range(16):
        t, dc = slot // 2, slot % 2
        if t in (0, 7):
            a_load(r, STAGES[t][0], dc, slot)
        else:
            for p in range(3):
                a_load(r, STAGES[t][p], dc, slot, cuts[p])

    xg[0, 0:f_in, :] = xraw[...]
    count = jnp.sum(msk_ref[...].astype(F32), axis=1, keepdims=True)
    hi = jnp.floor(count * (1.0 / COUNT_BASE))
    lo = count - COUNT_BASE * hi
    row16 = lax.broadcasted_iota(jnp.int32, (8, 128), 0) + (fpad - 8)
    tail = xg[0, fpad - 8:fpad, 0:128].astype(F32)
    tail = jnp.where(row16 == f_in, hi, jnp.where(row16 == f_in + 1, lo, tail))
    xg[0, fpad - 8:fpad, 0:128] = tail.astype(BF16)
    with scope("entry_w"):
        for cp in pre[2:]:
            cp.wait()
    w1f[0:f_in, :] = w1raw[...]
    w1t_ref[...] = w1f[...].T[:, 0:fpad].astype(BF16)
    w2f[0:classes, :] = w2raw[...]
    w2t_ref[...] = w2f[0:cpad, :].astype(BF16)
    w2_ref[...] = w2f[...].T[:, 0:cpad].astype(BF16)
    with scope("entry_barrier"):
        pl.semaphore_wait(barrier, len(near_peers))

    def gather(buf, work, event):
        ss = new("send")
        on = [new("recv") for _ in STAGES]
        ons = [new("recv") for _ in STAGES]

        def piece(slot, p):
            return buf.at[slot, :, cuts[p]]

        for j in range(3):
            for p, order in enumerate(ORDERS):
                send(piece(0, p), piece(2 * (1 + j), p), order[j], 0, ss, on[1 + j])
        sib = [prepare(buf.at[2 * t], buf.at[2 * t + 1], 0, 1, ss, ons[t]) for t in range(8)]
        sib[0].start()
        hops = {1: ((4, 1), (5, 2)), 2: ((6, 2),), 4: ((7, 2),)}
        onward = {t: [prepare(piece(2 * t, p), piece(2 * to, p), order[d], 0, ss, on[to]) for to, d in nxt for p, order in enumerate(ORDERS)]
                  for t, nxt in hops.items()}
        drain(buf.at[pl.ds(0, 15)], ss)

        def arrive(u):
            with scope(f"ev{u}"):
                landed(buf.at[0], on[u])
                for cp in onward.get(u, ()):
                    cp.start()
                sib[u].start()
                event(u)
                if u > 1:
                    landed(buf.at[0], ons[u - 1])

        with scope("ev0"):
            landed(buf.at[0], ons[0])
        work(0, 2)
        arrive(1)
        work(2, 1)

        @pl.loop(2, 8)
        def _(t):
            for u in range(2, 8):
                @pl.when(t == u)
                def _():
                    arrive(u)
            with scope("pair"):
                work(2 * t - 1, 2)
        event(8)
        with scope("ev8"):
            landed(buf.at[0], ons[7])
        work(15, 1)
        event(9)

    mrows = nb // 2

    def z1_work(base, count):
        a_wait(base, count, 0 if isinstance(base, int) and base == 0 else (base + 1) // 2)
        for j in range(count):
            y1[j] = dot(w1t_ref[...], xg[base + j]).astype(BF16)
        for m in range(0, nb, mrows):
            z1[m:m + mrows, :] += sum(dot(abuf[base + j, m:m + mrows, :], y1[j], ((1,), (1,))) for j in range(count))

    gather(xg, z1_work, lambda t: None)

    with scope("h1y2"):
        for m in range(0, nb, 256):
            h1t[0, :, m:m + 256] = jnp.maximum(z1[m:m + 256, :], 0.0).T.astype(BF16)
        y2g[0] = dot(w2t_ref[...], h1t[0]).astype(BF16)

    def z2_work(base, count):
        for m in range(0, nb, mrows):
            z2[m:m + mrows, 0:cpad] += sum(dot(abuf[base + j, m:m + mrows, :], y2g[base + j], ((1,), (1,))) for j in range(count))

    chunk = hid // 4
    h1t_ss, h1t_rs = new("send"), new("recv")
    h1t_cps = [prepare(h1t.at[0, pl.ds(i * chunk, chunk)], h1t.at[1, pl.ds(i * chunk, chunk)], 4, 0, h1t_ss, h1t_rs) for i in range(4)]
    drain(h1t.at[0], h1t_ss)

    def z2_event(t):
        for (which, k, dc), slot in BACK.items():
            if slot > 1 and (slot + 1) // 2 == t - 1:
                a_load(flip(r, which), k, dc, slot)
        if t == 5:
            h1t_cps[0].start()

    gather(y2g, z2_work, z2_event)

    tails = xg[0, fpad - 8:fpad, 0:128].astype(F32)
    for s in range(1, 16):
        tails = tails + xg[s, fpad - 8:fpad, 0:128].astype(F32)
    at_hi = f_in - (fpad - 8)
    total_m = COUNT_BASE * tails[at_hi:at_hi + 1, 0:1] + tails[at_hi + 1:at_hi + 2, 0:1]
    z2t = z2[...].T[0:cpad, :]
    cls = lax.broadcasted_iota(jnp.int32, (cpad, nb), 0)
    zm = jnp.where(cls < classes, z2t, -jnp.inf)
    zs = zm - jnp.max(zm, axis=0, keepdims=True)
    logp = zs - jnp.log(jnp.sum(jnp.exp(zs), axis=0, keepdims=True))
    hot = cls == lab_ref[...]
    mask_f = msk_ref[...].astype(F32)
    loss_v = -mask_f * jnp.sum(jnp.where(hot, logp, 0.0), axis=0, keepdims=True)
    loss_part = jnp.sum(loss_v, axis=1, keepdims=True) / total_m
    g2[0] = ((jnp.exp(logp) - hot.astype(F32)) * (mask_f / total_m)).astype(BF16)
    g2_rs, g2_ss = new("recv"), new("send")
    send(g2.at[0], g2.at[1], 4, 0, g2_ss, g2_rs)
    drain(g2.at[0], g2_ss)
    for cp in h1t_cps[1:]:
        cp.start()

    half = nb // 2
    units = ((3, 0), (3, 1), (1, 0), (2, 1), (2, 0), (1, 1), (0, 0), (0, 1))

    def tree(name, g, out, sibb, summ, rfwd, rfar, early):
        sib_ss, ss = new("send"), new("send")
        sib_rs = [new("recv") for _ in range(3)]
        sibf_rs = {(h, c): new("recv") for h in range(2) for c in range(2)}
        f_rs = {(h, c): new("recv") for h in range(2) for c in range(2)}
        x_rs = new("recv")
        y_rs = [new("recv") for _ in range(2)]
        drain(out, sib_ss)
        drain(summ.at[pl.ds(0, 6)], ss)

        def cols(h):
            return slice(h * half, (h + 1) * half)

        def own(q, h, dc):
            return dot(g[0], abuf[BACK[0, q, dc], :, cols(h)])

        def partner(q, h, dc):
            return dot(g[1], abuf[BACK[1, q, dc], :, cols(h)])

        def partner_piece(i, dc, c):
            q, h = units[i]
            lo = h * half + c * half // 2
            return dot(g[1], abuf[BACK[1, q, dc], :, lo:lo + half // 2])

        def piece(i, c):
            return (i, slice(None), slice(c * half // 2, (c + 1) * half // 2))

        def first_dim(h):
            return 1 if h == 0 else 2

        def begin():
            for i in range(early):
                out[i] = own(*units[i], 1)
                summ[i] = own(*units[i], 0)

        def first_group(between):
            with scope(name + "_group"):
                for c in range(2):
                    for i in range(2):
                        out[piece(i, c)] += partner_piece(i, 1, c)
                    for i in range(2):
                        send(out.at[piece(i, c)], sibb.at[piece(i, c)], 0, 1, sib_ss, sibf_rs[i, c])
                for i in range(2):
                    summ[i] += partner(*units[i], 0)
            for c in range(2):
                for i in range(2):
                    with scope(name + "_sib"):
                        landed(sibb.at[piece(i, c)], sibf_rs[i, c])
                    summ[piece(i, c)] += sibb[piece(i, c)]
                    send(summ.at[piece(i, c)], rfwd.at[piece(i, c)], first_dim(i), 0, ss, f_rs[i, c])
                if c == 0:
                    between()

        def group(j):
            pair = (2 * j, 2 * j + 1)
            with scope(name + "_group"):
                for i in pair:
                    if i < early:
                        out[i] += partner(*units[i], 1)
                    else:
                        out[i] = own(*units[i], 1) + partner(*units[i], 1)
                for i in pair:
                    send(out.at[i], sibb.at[i], 0, 1, sib_ss, sib_rs[j - 1])
                for i in pair:
                    if i < early:
                        summ[i] += partner(*units[i], 0)
                    else:
                        summ[i] = own(*units[i], 0) + partner(*units[i], 0)
            with scope(name + "_sib"):
                landed(sibb.at[pl.ds(2 * j, 2)], sib_rs[j - 1])
            for i in pair:
                q, h = units[i]
                summ[i] += sibb[i]
                if q == first_dim(h):
                    send(summ.at[i], rfar.at[h], first_dim(h), 0, ss, x_rs)

        def forward():
            for c in range(2):
                for h in range(2):
                    with scope(name + "_fwait"):
                        landed(rfwd.at[piece(h, c)], f_rs[h, c])
                    summ[piece(4 + h, c)] += rfwd[piece(h, c)]
                    send(summ.at[piece(4 + h, c)], rfar.at[piece(2 + h, c)], 3 - first_dim(h), 0, ss, y_rs[c])

        def collect():
            with scope(name + "_xwait"):
                landed(rfar.at[pl.ds(0, 2)], x_rs)
            for h in (0, 1):
                summ[6 + h] += rfar[h]

        def last(h, c):
            if h == 0:
                with scope(name + "_ywait"):
                    landed(rfar.at[0], y_rs[c])
            return (summ[piece(6 + h, c)] + rfar[piece(2 + h, c)]).astype(BF16)

        return begin, first_group, group, forward, collect, last

    begin, first_group, group, forward, collect, last = tree("p2", g2, p2out, p2sib, p2sum, p2fwd, p2far, 8)
    with scope("p2own"):
        for sem in range(1, 5):
            a_wait(0, 1 if sem == 1 else 2, sem)
        begin()
    with scope("g2z_wait"):
        landed(g2.at[1], g2_rs)
        for sem in range(5, 9):
            a_wait(0, 1 if sem == 8 else 2, sem)
    first_group(lambda: None)
    group(1)
    group(2)
    forward()
    group(3)
    collect()
    quarters = [(h, c, slice(h * half + c * half // 2, h * half + (c + 1) * half // 2)) for c in (0, 1) for h in (0, 1)]
    d2_rs, d2_ss = new("recv"), new("send")
    for h, c, at in quarters:
        d2[0, :, at] = last(h, c)
        send(d2.at[0, :, at], d2.at[1, :, at], 4, 0, d2_ss, d2_rs)
    drain(d2.at[0], d2_ss)

    def g1_of(i):
        g1[i] = jnp.where(h1t[i] > 0, dot(w2_ref[...], d2[i]), 0.0).astype(BF16)

    cls_row = lax.broadcasted_iota(jnp.int32, (cpad, hid), 0)
    part2[...] = jnp.where(cls_row == classes, loss_part, dot(d2[0], h1t[0], ((1,), (1,))))
    hc, hz = hid // 2, cpad // 2

    def span(start, size):
        return pl.ds(pl.multiple_of(start, size), size)

    w_ss = new("send")
    w_rs = [new("recv") for _ in range(6)]
    drain(p2out.at[0], w_ss)
    send(part2.at[:, span((1 - core) * hc, hc)], rbc, 0, 1, w_ss, w_rs[0])
    g1_of(0)

    begin, first_group, group, forward, collect, last = tree("p6", g1, p6out, p6sib, p6sum, p6fwd, p6far, 2)
    with scope("p6own"):
        begin()
    landed(rbc, w_rs[0])
    sumc[...] = part2[:, span(core * hc, hc)] + rbc[...]
    send(sumc.at[span((1 - r) * hz, hz)], rbz.at[0], 4, 0, w_ss, w_rs[1])
    with scope("d2z_wait"):
        landed(h1t.at[1], h1t_rs)
        landed(d2.at[1], d2_rs)
    with scope("g1b"):
        g1_of(1)

    def exchange_x():
        landed(rbz.at[0], w_rs[1])
        sumz[0] = sumc[span(r * hz, hz), :] + rbz[0]
        send(sumz.at[0], rbz.at[1], 1, 0, w_ss, w_rs[2])

    first_group(exchange_x)
    group(1)
    group(2)
    with scope("exchange_y"):
        landed(rbz.at[1], w_rs[2])
    sumz[1] = sumz[0] + rbz[1]
    send(sumz.at[1], rbz.at[2], 2, 0, w_ss, w_rs[3])
    forward()
    group(3)
    collect()
    mine = (span(r * hz, hz), span(core * hc, hc))
    landed(rbz.at[2], w_rs[3])
    res2[mine] = sumz[1] + rbz[2]
    send(res2.at[mine], res2.at[mine], 4, 0, w_ss, w_rs[4])
    landed(rbz.at[0], w_rs[4])
    mine = (slice(None), span(core * hc, hc))
    send(res2.at[mine], res2.at[mine], 0, 1, w_ss, w_rs[5])
    landed(rbc, w_rs[5])
    outs = [pltpu.make_async_copy(src, dst, osem.at[i]) for i, (src, dst) in enumerate(((res2, o2_hbm), (res1, o1_hbm)))]
    outs[0].start()

    rows = part1.shape[0] // 16

    acc = None
    for h, c, at in quarters:
        term = dot(xg[0, :, at], last(h, c), ((1,), (1,)))
        acc = term if acc is None else acc + term
    part1[0:fpad, :] = acc
    red_ss = [new("send") for _ in range(2)]
    red_rs = [new("recv") for _ in range(2)]
    with scope("red1"):
        for i, (k, dc) in enumerate(peers):
            send(part1.at[span(block_id(k, dc) * rows, rows)], rb1.at[i], k, dc, red_ss[0], red_rs[0])
        mine = span(block_id(0, 0) * rows, rows)
        landed(rb1, red_rs[0])
        res1[mine, :] = part1[mine, :] + sum(rb1[i] for i in range(len(peers)))
        for k, dc in peers:
            send(res1.at[mine], res1.at[mine], k, dc, red_ss[1], red_rs[1])
    with scope("out1_wait"):
        landed(rb1, red_rs[1])
    drain(rb1, red_ss[0])
    drain(rb1, red_ss[1])
    outs[1].start()
    with scope("send_wait"):
        for ref, ss in drains:
            pltpu.make_async_copy(ref, ref, ssem.at[ss]).wait()
        for cp in outs:
            cp.wait()
    assert used == {"send": ssem.shape[0], "recv": rsem.shape[0]}, used


def output_kernel(in1_ref, in2_ref, loss_ref, o1_ref, o2_ref):
    f_in, classes = o1_ref.shape[0], o2_ref.shape[0]
    o1_ref[...] = in1_ref[0:f_in, :]
    o2_ref[...] = in2_ref[0:classes, :]
    loss_ref[...] = in2_ref[classes:classes + 1, 0:1]


def solution(mesh):
    def local_step(adj_rows, features, w_one, w_two, labels, label_mask):
        nb, f_in = features.shape
        total = adj_rows.shape[1]
        hid, classes = w_two.shape
        cpad = 48
        lanes = 128
        fpad = 104
        half = nb // 2
        nsend, nrecv = 12, 71
        anyspec = pl.BlockSpec(memory_space=pl.ANY)
        V = pltpu.VMEM
        dw1, dw2 = pl.pallas_call(
            functools.partial(step_kernel, nb, classes, f_in, cpad),
            out_shape=[jax.ShapeDtypeStruct((lanes, hid), F32), jax.ShapeDtypeStruct((cpad, hid), F32)],
            in_specs=[anyspec] * 6,
            out_specs=[anyspec] * 2,
            scratch_shapes=[
                V((total // nb, nb, nb), BF16), V((16, fpad, nb), BF16), V((2, hid, nb), BF16),
                V((nb, hid), F32), V((2, hid, nb), BF16), V((16, cpad, nb), BF16), V((nb, lanes), F32), V((2, cpad, nb), BF16),
                V((f_in, nb), BF16), V((f_in, hid), F32), V((classes, hid), F32), V((1, nb), jnp.int32), V((1, nb), jnp.int32),
                V((hid, fpad), BF16), V((hid, cpad), BF16), V((cpad, hid), BF16), V((lanes, hid), F32), V((lanes, hid), F32),
                V((8, cpad, half), F32), V((8, cpad, half), F32), V((8, cpad, half), F32), V((2, cpad, half), F32), V((4, cpad, half), F32),
                V((2, cpad, nb), BF16), V((2, hid, nb), BF16),
                V((8, hid, half), F32), V((8, hid, half), F32), V((8, hid, half), F32),
                V((2, hid, half), F32), V((4, hid, half), F32),
                V((lanes, hid), F32), V((cpad, hid), F32), V((15, lanes // 16, hid), F32), V((cpad, hid // 2), F32),
                V((3, cpad // 2, hid // 2), F32), V((cpad, hid // 2), F32), V((2, cpad // 2, hid // 2), F32),
                V((lanes, hid), F32), V((cpad, hid), F32),
                pltpu.SemaphoreType.DMA((9,)), pltpu.SemaphoreType.DMA((5,)), pltpu.SemaphoreType.DMA((2,)),
                pltpu.SemaphoreType.DMA((nsend,)), pltpu.SemaphoreType.DMA((nrecv,)),
            ],
            compiler_params=pltpu.CompilerParams(collective_id=0, has_side_effects=True, vmem_limit_bytes=67043328),
            name="gcn_step",
        )(adj_rows, features.T, w_one, w_two.T, labels.reshape(1, nb), label_mask.reshape(1, nb))
        loss, dw1, dw2 = pl.pallas_call(
            output_kernel,
            out_shape=[jax.ShapeDtypeStruct((1, 1), F32), jax.ShapeDtypeStruct((f_in, hid), F32),
                       jax.ShapeDtypeStruct((classes, hid), F32)],
            name="outputs",
        )(dw1, dw2)
        return loss.reshape(()), dw1, dw2.T

    row_spec = P(("nodes", "rep"))
    return jax.shard_map(local_step, mesh=mesh, in_specs=(P("nodes", None), P(("nodes", "rep"), None), P(), P(), row_spec, row_spec), out_specs=(P(), P(), P()), check_vma=False)
```

```python
import functools

import jax
import jax.numpy as jnp
from jax import lax
from jax.experimental import pallas as pl
from jax.experimental.pallas import tpu as pltpu
from jax.sharding import PartitionSpec as P

BF16 = jnp.bfloat16
F32 = jnp.float32
scope = jax.named_scope

ORDERS = ((1, 2, 4), (2, 4, 1), (4, 1, 2))
STAGES = (((0,) * 3,) + tuple(tuple(o[j] for o in ORDERS) for j in range(3))
          + tuple(tuple(o[a] + o[b] for o in ORDERS) for a, b in ((0, 1), (0, 2), (1, 2))) + ((7,) * 3,))
BACK = {key: slot for slot, key in enumerate(
    [(0, 0, 0), (0, 0, 1)] + [(0, k, dc) for k in (3, 1, 2) for dc in (1, 0)] + [(1, k, dc) for k in (3, 1, 2, 0) for dc in (1, 0)])}
COUNT_BASE = 32.0


def dot(a, b, dims=((1,), (0,))):
    return lax.dot_general(a, b, (dims, ((), ())), preferred_element_type=F32)


def step_kernel(nb, classes, f_in, cpad,
                a_hbm, x_hbm, w1_hbm, w2_hbm, lab_hbm, msk_hbm,
                o1_ref, o2_ref,
                abuf, xg, y1, z1, h1t, y2g, z2, g2,
                xraw, w1raw, w2raw, lab_ref, msk_ref, w1t_ref, w2_ref, w2t_ref, w1f, w2f,
                p2out, p2sib, p2sum, p2fwd, p2far, d2,
                p6out, p6sib, p6sum, p6fwd, p6far,
                part1, part2, rb1, rbc, rbz, sumc, sumz, res1, res2,
                asem, psem, ssem, rsem):
    r = lax.axis_index("rep")
    n = lax.axis_index("nodes")
    core = n % 2
    xc = (n // 2) % 2
    yc = n // 4
    hid = z1.shape[1]
    fpad = xg.shape[1]

    def flip(v, f):
        return 1 - v if f else v

    def coords(k, dc):
        rr = flip(r, k // 4)
        nn = flip(yc, (k // 2) % 2) * 4 + flip(xc, k % 2) * 2 + flip(core, dc)
        return rr, nn

    def block_id(k, dc):
        rr, nn = coords(k, dc)
        return nn * 2 + rr

    used = {"send": 0, "recv": 0}
    drains = []

    def new(kind):
        used[kind] += 1
        return used[kind] - 1

    def prepare(src, dst, k, dc, ss, rs):
        return pltpu.make_async_remote_copy(
            src_ref=src, dst_ref=dst, send_sem=ssem.at[ss], recv_sem=rsem.at[rs],
            device_id=coords(k, dc), device_id_type=pl.DeviceIdType.MESH)

    def send(*args):
        prepare(*args).start()

    def landed(ref, rs):
        pltpu.make_async_copy(ref, ref, rsem.at[rs]).wait()

    def drain(ref, ss):
        drains.append((ref, ss))

    peers = [(k, dc) for k in (7, 3, 5, 6, 1, 2, 4, 0) for dc in range(2) if (k, dc) != (0, 0)]

    pre = [pltpu.make_async_copy(src, dst, psem.at[i]) for i, (src, dst) in enumerate(
        ((x_hbm, xraw), (msk_hbm, msk_ref), (w1_hbm, w1raw), (w2_hbm, w2raw), (lab_hbm, lab_ref)))]
    for cp in pre:
        cp.start()
    barrier = pltpu.get_barrier_semaphore()
    near_peers = ((0, 1), (1, 0), (2, 0), (4, 0))
    for k, dc in near_peers:
        pl.semaphore_signal(barrier, inc=1, device_id=coords(k, dc), device_id_type=pl.DeviceIdType.MESH)
    z1[...] = jnp.zeros_like(z1)
    z2[...] = jnp.zeros_like(z2)
    part1[...] = jnp.zeros_like(part1)
    w1f[...] = jnp.zeros_like(w1f)
    w2f[...] = jnp.zeros_like(w2f)
    xg[0] = jnp.zeros((fpad, nb), BF16)
    with scope("entry_x"):
        pre[0].wait()
        pre[1].wait()

    third = (nb // 3 // 128 + 1) * 128
    cuts = [slice(0, third), slice(third, 2 * third), slice(2 * third, nb)]

    def a_load(rows, k, dc, slot, cut=slice(0, nb)):
        row = pl.multiple_of(rows * nb, nb)
        col = pl.multiple_of(block_id(k, dc) * nb + cut.start, 128)
        size = cut.stop - cut.start
        pltpu.make_async_copy(a_hbm.at[pl.ds(row, nb), pl.ds(col, size)], abuf.at[slot, :, cut], asem.at[0 if slot < 2 else (slot + 1) // 2]).start()

    def a_wait(base, count, sem):
        pltpu.make_async_copy(a_hbm.at[pl.ds(0, count * nb), pl.ds(0, nb)], a_hbm.at[pl.ds(0, count * nb), pl.ds(0, nb)], asem.at[sem]).wait()

    for slot in range(16):
        t, dc = slot // 2, slot % 2
        if t in (0, 7):
            a_load(r, STAGES[t][0], dc, slot)
        else:
            for p in range(3):
                a_load(r, STAGES[t][p], dc, slot, cuts[p])

    xg[0, 0:f_in, :] = xraw[...]
    count = jnp.sum(msk_ref[...].astype(F32), axis=1, keepdims=True)
    hi = jnp.floor(count * (1.0 / COUNT_BASE))
    lo = count - COUNT_BASE * hi
    row16 = lax.broadcasted_iota(jnp.int32, (8, 128), 0) + (fpad - 8)
    tail = xg[0, fpad - 8:fpad, 0:128].astype(F32)
    tail = jnp.where(row16 == f_in, hi, jnp.where(row16 == f_in + 1, lo, tail))
    xg[0, fpad - 8:fpad, 0:128] = tail.astype(BF16)
    with scope("entry_w"):
        for cp in pre[2:]:
            cp.wait()
    w1f[0:f_in, :] = w1raw[...]
    w1t_ref[...] = w1f[...].T[:, 0:fpad].astype(BF16)
    w2f[0:classes, :] = w2raw[...]
    w2t_ref[...] = w2f[0:cpad, :].astype(BF16)
    w2_ref[...] = w2f[...].T[:, 0:cpad].astype(BF16)
    with scope("entry_barrier"):
        pl.semaphore_wait(barrier, len(near_peers))

    def gather(buf, work, event):
        ss = new("send")
        on = [new("recv") for _ in STAGES]
        ons = [new("recv") for _ in STAGES]

        def piece(slot, p):
            return buf.at[slot, :, cuts[p]]

        for j in range(3):
            for p, order in enumerate(ORDERS):
                send(piece(0, p), piece(2 * (1 + j), p), order[j], 0, ss, on[1 + j])
        sib = [prepare(buf.at[2 * t], buf.at[2 * t + 1], 0, 1, ss, ons[t]) for t in range(8)]
        sib[0].start()
        hops = {1: ((4, 1), (5, 2)), 2: ((6, 2),), 4: ((7, 2),)}
        onward = {t: [prepare(piece(2 * t, p), piece(2 * to, p), order[d], 0, ss, on[to]) for to, d in nxt for p, order in enumerate(ORDERS)]
                  for t, nxt in hops.items()}
        drain(buf.at[pl.ds(0, 15)], ss)

        def arrive(u):
            with scope(f"ev{u}"):
                landed(buf.at[0], on[u])
                for cp in onward.get(u, ()):
                    cp.start()
                sib[u].start()
                event(u)
                if u > 1:
                    landed(buf.at[0], ons[u - 1])

        with scope("ev0"):
            landed(buf.at[0], ons[0])
        work(0, 2)
        arrive(1)
        work(2, 1)

        @pl.loop(2, 8)
        def _(t):
            for u in range(2, 8):
                @pl.when(t == u)
                def _():
                    arrive(u)
            with scope("pair"):
                work(2 * t - 1, 2)
        event(8)
        with scope("ev8"):
            landed(buf.at[0], ons[7])
        work(15, 1)
        event(9)

    mrows = nb // 2

    def z1_work(base, count):
        a_wait(base, count, 0 if isinstance(base, int) and base == 0 else (base + 1) // 2)
        for j in range(count):
            y1[j] = dot(w1t_ref[...], xg[base + j]).astype(BF16)
        for m in range(0, nb, mrows):
            total = z1[m:m + mrows, :]
            for j in range(count):
                total = total + dot(abuf[base + j, m:m + mrows, :], y1[j], ((1,), (1,)))
            z1[m:m + mrows, :] = total

    gather(xg, z1_work, lambda t: None)

    with scope("h1y2"):
        for m in range(0, nb, 256):
            h1t[0, :, m:m + 256] = jnp.maximum(z1[m:m + 256, :], 0.0).T.astype(BF16)
        y2g[0] = dot(w2t_ref[...], h1t[0]).astype(BF16)

    def z2_work(base, count):
        for m in range(0, nb, mrows):
            total = z2[m:m + mrows, 0:cpad]
            for j in range(count):
                total = total + dot(abuf[base + j, m:m + mrows, :], y2g[base + j], ((1,), (1,)))
            z2[m:m + mrows, 0:cpad] = total

    chunk = hid // 4
    h1t_ss, h1t_rs = new("send"), new("recv")
    h1t_cps = [prepare(h1t.at[0, pl.ds(i * chunk, chunk)], h1t.at[1, pl.ds(i * chunk, chunk)], 4, 0, h1t_ss, h1t_rs) for i in range(4)]
    drain(h1t.at[0], h1t_ss)

    def z2_event(t):
        for (which, k, dc), slot in BACK.items():
            if slot > 1 and (slot + 1) // 2 == t - 1:
                a_load(flip(r, which), k, dc, slot)
        if t == 5:
            h1t_cps[0].start()

    gather(y2g, z2_work, z2_event)

    tails = xg[0, fpad - 8:fpad, 0:128].astype(F32)
    for s in range(1, 16):
        tails = tails + xg[s, fpad - 8:fpad, 0:128].astype(F32)
    at_hi = f_in - (fpad - 8)
    total_m = COUNT_BASE * tails[at_hi:at_hi + 1, 0:1] + tails[at_hi + 1:at_hi + 2, 0:1]
    z2t = z2[...].T[0:cpad, :]
    cls = lax.broadcasted_iota(jnp.int32, (cpad, nb), 0)
    zm = jnp.where(cls < classes, z2t, -jnp.inf)
    zs = zm - jnp.max(zm, axis=0, keepdims=True)
    logp = zs - jnp.log(jnp.sum(jnp.exp(zs), axis=0, keepdims=True))
    hot = cls == lab_ref[...]
    mask_f = msk_ref[...].astype(F32)
    loss_v = -mask_f * jnp.sum(jnp.where(hot, logp, 0.0), axis=0, keepdims=True)
    loss_part = jnp.sum(loss_v, axis=1, keepdims=True) / total_m
    g2[0] = ((jnp.exp(logp) - hot.astype(F32)) * (mask_f / total_m)).astype(BF16)
    g2_rs, g2_ss = new("recv"), new("send")
    send(g2.at[0], g2.at[1], 4, 0, g2_ss, g2_rs)
    drain(g2.at[0], g2_ss)
    for cp in h1t_cps[1:]:
        cp.start()

    half = nb // 2
    units = ((3, 0), (3, 1), (1, 0), (2, 1), (2, 0), (1, 1), (0, 0), (0, 1))

    def tree(name, g, out, sibb, summ, rfwd, rfar, early):
        sib_ss, ss = new("send"), new("send")
        sib_rs = [new("recv") for _ in range(3)]
        sibf_rs = {(h, c): new("recv") for h in range(2) for c in range(2)}
        f_rs = {(h, c): new("recv") for h in range(2) for c in range(2)}
        x_rs = new("recv")
        y_rs = [new("recv") for _ in range(2)]
        drain(out, sib_ss)
        drain(summ.at[pl.ds(0, 6)], ss)

        def cols(h):
            return slice(h * half, (h + 1) * half)

        def own(q, h, dc):
            return dot(g[0], abuf[BACK[0, q, dc], :, cols(h)])

        def partner(q, h, dc):
            return dot(g[1], abuf[BACK[1, q, dc], :, cols(h)])

        def partner_piece(i, dc, c):
            q, h = units[i]
            lo = h * half + c * half // 2
            return dot(g[1], abuf[BACK[1, q, dc], :, lo:lo + half // 2])

        def piece(i, c):
            return (i, slice(None), slice(c * half // 2, (c + 1) * half // 2))

        def first_dim(h):
            return 1 if h == 0 else 2

        def begin():
            for i in range(early):
                out[i] = own(*units[i], 1)
                summ[i] = own(*units[i], 0)

        def first_group(between):
            with scope(name + "_group"):
                for c in range(2):
                    for i in range(2):
                        out[piece(i, c)] += partner_piece(i, 1, c)
                    for i in range(2):
                        send(out.at[piece(i, c)], sibb.at[piece(i, c)], 0, 1, sib_ss, sibf_rs[i, c])
            for c in range(2):
                with scope(name + "_group"):
                    for i in range(2):
                        summ[piece(i, c)] += partner_piece(i, 0, c)
                for i in range(2):
                    with scope(name + "_sib"):
                        landed(sibb.at[piece(i, c)], sibf_rs[i, c])
                    summ[piece(i, c)] += sibb[piece(i, c)]
                    send(summ.at[piece(i, c)], rfwd.at[piece(i, c)], first_dim(i), 0, ss, f_rs[i, c])
                if c == 0:
                    between()

        def group(j):
            pair = (2 * j, 2 * j + 1)
            with scope(name + "_group"):
                for i in pair:
                    if i < early:
                        out[i] += partner(*units[i], 1)
                    else:
                        out[i] = own(*units[i], 1) + partner(*units[i], 1)
                for i in pair:
                    send(out.at[i], sibb.at[i], 0, 1, sib_ss, sib_rs[j - 1])
                for i in pair:
                    if i < early:
                        summ[i] += partner(*units[i], 0)
                    else:
                        summ[i] = own(*units[i], 0) + partner(*units[i], 0)
            with scope(name + "_sib"):
                landed(sibb.at[pl.ds(2 * j, 2)], sib_rs[j - 1])
            for i in pair:
                q, h = units[i]
                summ[i] += sibb[i]
                if q == first_dim(h):
                    send(summ.at[i], rfar.at[h], first_dim(h), 0, ss, x_rs)

        def forward():
            for c in range(2):
                for h in range(2):
                    with scope(name + "_fwait"):
                        landed(rfwd.at[piece(h, c)], f_rs[h, c])
                    summ[piece(4 + h, c)] += rfwd[piece(h, c)]
                    send(summ.at[piece(4 + h, c)], rfar.at[piece(2 + h, c)], 3 - first_dim(h), 0, ss, y_rs[c])

        def collect():
            with scope(name + "_xwait"):
                landed(rfar.at[pl.ds(0, 2)], x_rs)
            for h in (0, 1):
                summ[6 + h] += rfar[h]

        def last(h, c):
            if h == 0:
                with scope(name + "_ywait"):
                    landed(rfar.at[0], y_rs[c])
            return (summ[piece(6 + h, c)] + rfar[piece(2 + h, c)]).astype(BF16)

        return begin, first_group, group, forward, collect, last

    begin, first_group, group, forward, collect, last = tree("p2", g2, p2out, p2sib, p2sum, p2fwd, p2far, 8)
    with scope("p2own"):
        for sem in range(1, 5):
            a_wait(0, 1 if sem == 1 else 2, sem)
        begin()
    with scope("g2z_wait"):
        landed(g2.at[1], g2_rs)
        for sem in range(5, 9):
            a_wait(0, 1 if sem == 8 else 2, sem)
    first_group(lambda: None)
    group(1)
    group(2)
    forward()
    group(3)
    collect()
    quarters = [(h, c, slice(h * half + c * half // 2, h * half + (c + 1) * half // 2)) for c in (0, 1) for h in (0, 1)]
    d2_rs, d2_ss = new("recv"), new("send")
    for h, c, at in quarters:
        d2[0, :, at] = last(h, c)
        send(d2.at[0, :, at], d2.at[1, :, at], 4, 0, d2_ss, d2_rs)
    drain(d2.at[0], d2_ss)

    g1 = y1

    def g1_of(i):
        g1[i] = jnp.where(h1t[i] > 0, dot(w2_ref[...], d2[i]), 0.0).astype(BF16)

    cls_row = lax.broadcasted_iota(jnp.int32, (cpad, hid), 0)
    part2[...] = jnp.where(cls_row == classes, loss_part, dot(d2[0], h1t[0], ((1,), (1,))))
    hc, hz = hid // 2, cpad // 2

    def span(start, size):
        return pl.ds(pl.multiple_of(start, size), size)

    w_ss = new("send")
    w_rs = [new("recv") for _ in range(6)]
    drain(p2out.at[0], w_ss)
    send(part2.at[:, span((1 - core) * hc, hc)], rbc, 0, 1, w_ss, w_rs[0])
    g1_of(0)

    begin, first_group, group, forward, collect, last = tree("p6", g1, p6out, p6sib, p6sum, p6fwd, p6far, 2)
    with scope("p6own"):
        begin()
    landed(rbc, w_rs[0])
    sumc[...] = part2[:, span(core * hc, hc)] + rbc[...]
    send(sumc.at[span((1 - r) * hz, hz)], rbz.at[0], 4, 0, w_ss, w_rs[1])
    with scope("d2z_wait"):
        landed(h1t.at[1], h1t_rs)
        landed(d2.at[1], d2_rs)
    with scope("g1b"):
        g1_of(1)

    def exchange_x():
        landed(rbz.at[0], w_rs[1])
        sumz[0] = sumc[span(r * hz, hz), :] + rbz[0]
        send(sumz.at[0], rbz.at[1], 1, 0, w_ss, w_rs[2])

    first_group(exchange_x)
    group(1)
    group(2)
    with scope("exchange_y"):
        landed(rbz.at[1], w_rs[2])
    sumz[1] = sumz[0] + rbz[1]
    send(sumz.at[1], rbz.at[2], 2, 0, w_ss, w_rs[3])
    forward()
    group(3)
    collect()
    mine = (span(r * hz, hz), span(core * hc, hc))
    landed(rbz.at[2], w_rs[3])
    res2[mine] = sumz[1] + rbz[2]
    send(res2.at[mine], res2.at[mine], 4, 0, w_ss, w_rs[4])
    landed(rbz.at[0], w_rs[4])
    mine = (slice(None), span(core * hc, hc))
    send(res2.at[mine], res2.at[mine], 0, 1, w_ss, w_rs[5])
    landed(rbc, w_rs[5])
    o2_ref[...] = res2[...]

    rows = part1.shape[0] // 16

    acc = None
    for h, c, at in quarters:
        term = dot(xg[0, :, at], last(h, c), ((1,), (1,)))
        acc = term if acc is None else acc + term
    part1[0:fpad, :] = acc
    red_ss = [new("send") for _ in range(2)]
    red_rs = [new("recv") for _ in range(2)]
    with scope("red1"):
        for i, (k, dc) in enumerate(peers):
            send(part1.at[span(block_id(k, dc) * rows, rows)], rb1.at[i], k, dc, red_ss[0], red_rs[0])
        mine = span(block_id(0, 0) * rows, rows)
        landed(rb1, red_rs[0])
        res1[mine, :] = part1[mine, :] + sum(rb1[i] for i in range(len(peers)))
        for k, dc in peers:
            send(res1.at[mine], res1.at[mine], k, dc, red_ss[1], red_rs[1])
    with scope("out1_wait"):
        landed(rb1, red_rs[1])
    drain(rb1, red_ss[0])
    drain(rb1, red_ss[1])
    o1_ref[...] = res1[...]
    with scope("send_wait"):
        for ref, ss in drains:
            pltpu.make_async_copy(ref, ref, ssem.at[ss]).wait()
    assert used == {"send": ssem.shape[0], "recv": rsem.shape[0]}, used


def output_kernel(in1_ref, in2_ref, loss_ref, o1_ref, o2_ref):
    f_in, classes = o1_ref.shape[0], o2_ref.shape[0]
    o1_ref[...] = in1_ref[0:f_in, :]
    o2_ref[...] = in2_ref[0:classes, :]
    loss_ref[...] = in2_ref[classes:classes + 1, 0:1]


def solution(mesh):
    def local_step(adj_rows, features, w_one, w_two, labels, label_mask):
        nb, f_in = features.shape
        total = adj_rows.shape[1]
        hid, classes = w_two.shape
        cpad = 48
        lanes = 128
        fpad = 104
        half = nb // 2
        nsend, nrecv = 12, 71
        anyspec = pl.BlockSpec(memory_space=pl.ANY)
        V = pltpu.VMEM
        dw1, dw2 = pl.pallas_call(
            functools.partial(step_kernel, nb, classes, f_in, cpad),
            out_shape=[V((lanes, hid), F32), V((cpad, hid), F32)],
            in_specs=[anyspec] * 6,
            out_specs=[pl.BlockSpec(memory_space=pltpu.VMEM)] * 2,
            scratch_shapes=[
                V((total // nb, nb, nb), BF16), V((16, fpad, nb), BF16), V((2, hid, nb), BF16),
                V((nb, hid), F32), V((2, hid, nb), BF16), V((16, cpad, nb), BF16), V((nb, lanes), F32), V((2, cpad, nb), BF16),
                V((f_in, nb), BF16), V((f_in, hid), F32), V((classes, hid), F32), V((1, nb), jnp.int32), V((1, nb), jnp.int32),
                V((hid, fpad), BF16), V((hid, cpad), BF16), V((cpad, hid), BF16), V((lanes, hid), F32), V((lanes, hid), F32),
                V((8, cpad, half), F32), V((8, cpad, half), F32), V((8, cpad, half), F32), V((2, cpad, half), F32), V((4, cpad, half), F32),
                V((2, cpad, nb), BF16),
                V((8, hid, half), F32), V((8, hid, half), F32), V((8, hid, half), F32),
                V((2, hid, half), F32), V((4, hid, half), F32),
                V((lanes, hid), F32), V((cpad, hid), F32), V((15, lanes // 16, hid), F32), V((cpad, hid // 2), F32),
                V((3, cpad // 2, hid // 2), F32), V((cpad, hid // 2), F32), V((2, cpad // 2, hid // 2), F32),
                V((lanes, hid), F32), V((cpad, hid), F32),
                pltpu.SemaphoreType.DMA((9,)), pltpu.SemaphoreType.DMA((5,)),
                pltpu.SemaphoreType.DMA((nsend,)), pltpu.SemaphoreType.DMA((nrecv,)),
            ],
            compiler_params=pltpu.CompilerParams(collective_id=0, has_side_effects=True, vmem_limit_bytes=64 * 1000 * 1000),
            name="gcn_step",
        )(adj_rows, features.T, w_one, w_two.T, labels.reshape(1, nb), label_mask.reshape(1, nb))
        loss, dw1, dw2 = pl.pallas_call(
            output_kernel,
            out_shape=[jax.ShapeDtypeStruct((1, 1), F32), jax.ShapeDtypeStruct((f_in, hid), F32),
                       jax.ShapeDtypeStruct((classes, hid), F32)],
            name="outputs",
        )(*(pltpu.with_memory_space_constraint(v, pltpu.VMEM) for v in (dw1, dw2)))
        return loss.reshape(()), dw1, dw2.T

    row_spec = P(("nodes", "rep"))
    return jax.shard_map(local_step, mesh=mesh, in_specs=(P("nodes", None), P(("nodes", "rep"), None), P(), P(), row_spec, row_spec), out_specs=(P(), P(), P()), check_vma=False)
```

```python
import functools

import jax
import jax.numpy as jnp
from jax import lax
from jax.experimental import pallas as pl
from jax.experimental.pallas import tpu as pltpu
from jax.sharding import PartitionSpec as P

BF16 = jnp.bfloat16
F32 = jnp.float32
scope = jax.named_scope

ORDERS = ((1, 2, 4), (2, 4, 1), (4, 1, 2))
STAGES = (((0,) * 3,) + tuple(tuple(o[j] for o in ORDERS) for j in range(3))
          + tuple(tuple(o[a] + o[b] for o in ORDERS) for a, b in ((0, 1), (0, 2), (1, 2))) + ((7,) * 3,))
BACK = {key: slot for slot, key in enumerate(
    [(0, 0, 0), (0, 0, 1)] + [(0, k, dc) for k in (3, 1, 2) for dc in (1, 0)] + [(1, k, dc) for k in (3, 1, 2, 0) for dc in (1, 0)])}
COUNT_BASE = 32.0


def dot(a, b, dims=((1,), (0,))):
    return lax.dot_general(a, b, (dims, ((), ())), preferred_element_type=F32)


def step_kernel(nb, classes, f_in, cpad,
                a_hbm, x_hbm, w1_hbm, w2_hbm, lab_hbm, msk_hbm,
                o1_ref, o2_ref,
                abuf, xg, y1, z1, h1t, y2g, z2, g2,
                xraw, w1raw, w2raw, lab_ref, msk_ref, w1t_ref, w2_ref, w2t_ref, w1f, w2f,
                p2out, p2sib, p2sum, p2fwd, p2far, d2,
                p6out, p6sib, p6sum, p6fwd, p6far,
                part1, part2, rb1, rbc, rbz, sumc, sumz, res1, res2,
                asem, psem, ssem, rsem):
    r = lax.axis_index("rep")
    n = lax.axis_index("nodes")
    core = n % 2
    xc = (n // 2) % 2
    yc = n // 4
    hid = z1.shape[1]
    fpad = xg.shape[1]

    def flip(v, f):
        return 1 - v if f else v

    def coords(k, dc):
        rr = flip(r, k // 4)
        nn = flip(yc, (k // 2) % 2) * 4 + flip(xc, k % 2) * 2 + flip(core, dc)
        return rr, nn

    def block_id(k, dc):
        rr, nn = coords(k, dc)
        return nn * 2 + rr

    used = {"send": 0, "recv": 0}
    drains = []

    def new(kind):
        used[kind] += 1
        return used[kind] - 1

    def prepare(src, dst, k, dc, ss, rs):
        return pltpu.make_async_remote_copy(
            src_ref=src, dst_ref=dst, send_sem=ssem.at[ss], recv_sem=rsem.at[rs],
            device_id=coords(k, dc), device_id_type=pl.DeviceIdType.MESH)

    def send(*args):
        prepare(*args).start()

    def landed(ref, rs):
        pltpu.make_async_copy(ref, ref, rsem.at[rs]).wait()

    def drain(ref, ss):
        drains.append((ref, ss))

    peers = [(k, dc) for k in (7, 3, 5, 6, 1, 2, 4, 0) for dc in range(2) if (k, dc) != (0, 0)]

    pre = [pltpu.make_async_copy(src, dst, psem.at[i]) for i, (src, dst) in enumerate(
        ((x_hbm, xraw), (msk_hbm, msk_ref), (w1_hbm, w1raw), (w2_hbm, w2raw), (lab_hbm, lab_ref)))]
    for cp in pre:
        cp.start()
    barrier = pltpu.get_barrier_semaphore()
    near_peers = ((0, 1), (1, 0), (2, 0), (4, 0))
    for k, dc in near_peers:
        pl.semaphore_signal(barrier, inc=1, device_id=coords(k, dc), device_id_type=pl.DeviceIdType.MESH)
    z1[...] = jnp.zeros_like(z1)
    z2[...] = jnp.zeros_like(z2)
    part1[...] = jnp.zeros_like(part1)
    w1f[...] = jnp.zeros_like(w1f)
    w2f[...] = jnp.zeros_like(w2f)
    xg[0] = jnp.zeros((fpad, nb), BF16)
    with scope("entry_x"):
        pre[0].wait()
        pre[1].wait()

    third = (nb // 3 // 128 + 1) * 128
    cuts = [slice(0, third), slice(third, 2 * third), slice(2 * third, nb)]

    def a_load(rows, k, dc, slot, cut=slice(0, nb)):
        row = pl.multiple_of(rows * nb, nb)
        col = pl.multiple_of(block_id(k, dc) * nb + cut.start, 128)
        size = cut.stop - cut.start
        pltpu.make_async_copy(a_hbm.at[pl.ds(row, nb), pl.ds(col, size)], abuf.at[slot, :, cut], asem.at[0 if slot < 2 else (slot + 1) // 2]).start()

    def a_wait(base, count, sem):
        pltpu.make_async_copy(a_hbm.at[pl.ds(0, count * nb), pl.ds(0, nb)], a_hbm.at[pl.ds(0, count * nb), pl.ds(0, nb)], asem.at[sem]).wait()

    for slot in range(16):
        t, dc = slot // 2, slot % 2
        if t in (0, 7):
            a_load(r, STAGES[t][0], dc, slot)
        else:
            for p in range(3):
                a_load(r, STAGES[t][p], dc, slot, cuts[p])

    xg[0, 0:f_in, :] = xraw[...]
    count = jnp.sum(msk_ref[...].astype(F32), axis=1, keepdims=True)
    hi = jnp.floor(count * (1.0 / COUNT_BASE))
    lo = count - COUNT_BASE * hi
    row16 = lax.broadcasted_iota(jnp.int32, (8, 128), 0) + (fpad - 8)
    tail = xg[0, fpad - 8:fpad, 0:128].astype(F32)
    tail = jnp.where(row16 == f_in, hi, jnp.where(row16 == f_in + 1, lo, tail))
    xg[0, fpad - 8:fpad, 0:128] = tail.astype(BF16)
    with scope("entry_w"):
        for cp in pre[2:]:
            cp.wait()
    w1f[0:f_in, :] = w1raw[...]
    w1t_ref[...] = w1f[...].T[:, 0:fpad].astype(BF16)
    w2f[0:classes, :] = w2raw[...]
    w2t_ref[...] = w2f[0:cpad, :].astype(BF16)
    w2_ref[...] = w2f[...].T[:, 0:cpad].astype(BF16)
    with scope("entry_barrier"):
        pl.semaphore_wait(barrier, len(near_peers))

    def gather(buf, work, event, tail=None):
        ss = new("send")
        on = [new("recv") for _ in STAGES]
        ons = [new("recv") for _ in STAGES]

        def piece(slot, p):
            return buf.at[slot, :, cuts[p]]

        for j in range(3):
            for p, order in enumerate(ORDERS):
                send(piece(0, p), piece(2 * (1 + j), p), order[j], 0, ss, on[1 + j])
        sib = [prepare(buf.at[2 * t], buf.at[2 * t + 1], 0, 1, ss, ons[t]) for t in range(8)]
        sib[0].start()
        hops = {1: ((4, 1), (5, 2)), 2: ((6, 2),), 4: ((7, 2),)}
        onward = {t: [prepare(piece(2 * t, p), piece(2 * to, p), order[d], 0, ss, on[to]) for to, d in nxt for p, order in enumerate(ORDERS)]
                  for t, nxt in hops.items()}
        drain(buf.at[pl.ds(0, 15)], ss)

        def arrive(u):
            with scope(f"ev{u}"):
                landed(buf.at[0], on[u])
                for cp in onward.get(u, ()):
                    cp.start()
                sib[u].start()
                if u > 1:
                    landed(buf.at[0], ons[u - 1])

        with scope("ev0"):
            landed(buf.at[0], ons[0])
        work(0, 2)
        arrive(1)
        work(2, 1)


        @pl.loop(2, 8)
        def _(t):
            for u in range(2, 8):
                @pl.when(t == u)
                def _():
                    arrive(u)
                    event(u)
            with scope("pair"):
                work(2 * t - 1, 2)
        event(8)
        with scope("ev8"):
            landed(buf.at[0], ons[7])
        if tail:
            tail()
        else:
            work(15, 1)
        event(9)

    mrows = nb // 2

    def z1_work(base, count):
        a_wait(base, count, 0 if isinstance(base, int) and base == 0 else (base + 1) // 2)
        for j in range(count):
            y1[j] = dot(w1t_ref[...], xg[base + j]).astype(BF16)
        for m in range(0, nb, mrows):
            total = z1[m:m + mrows, :]
            for j in range(count):
                total = total + dot(abuf[base + j, m:m + mrows, :], y1[j], ((1,), (1,)))
            z1[m:m + mrows, :] = total

    gather(xg, z1_work, lambda t: None)

    with scope("h1y2"):
        for m in range(0, nb, 256):
            h1t[0, :, m:m + 256] = jnp.maximum(z1[m:m + 256, :], 0.0).T.astype(BF16)
        y2g[0] = dot(w2t_ref[...], h1t[0]).astype(BF16)

    def z2_work(base, count):
        for m in range(0, nb, mrows):
            total = z2[m:m + mrows, 0:cpad]
            for j in range(count):
                total = total + dot(abuf[base + j, m:m + mrows, :], y2g[base + j], ((1,), (1,)))
            z2[m:m + mrows, 0:cpad] = total

    chunk = hid // 4
    h1t_ss, h1t_rs = new("send"), new("recv")
    h1t_cps = [prepare(h1t.at[0, pl.ds(i * chunk, chunk)], h1t.at[1, pl.ds(i * chunk, chunk)], 4, 0, h1t_ss, h1t_rs) for i in range(4)]
    drain(h1t.at[0], h1t_ss)

    def z2_event(t):
        for (which, k, dc), slot in BACK.items():
            if slot > 1 and (slot + 1) // 2 == t - 1:
                a_load(flip(r, which), k, dc, slot)
        if t == 5:
            h1t_cps[0].start()

    tails = xg[0, fpad - 8:fpad, 0:128].astype(F32)
    for s in range(1, 16):
        tails = tails + xg[s, fpad - 8:fpad, 0:128].astype(F32)
    at_hi = f_in - (fpad - 8)
    total_m = COUNT_BASE * tails[at_hi:at_hi + 1, 0:1] + tails[at_hi + 1:at_hi + 2, 0:1]
    g2_rs, g2_ss = new("recv"), new("send")
    losses = []

    def z2_tail():
        for m in range(0, nb, mrows):
            at = slice(m, m + mrows)
            total = z2[at, 0:cpad]
            total = total + dot(abuf[15, at, :], y2g[15], ((1,), (1,)))
            z2[at, 0:cpad] = total
            z2t = z2[at, :].T[0:cpad, :]
            cls = lax.broadcasted_iota(jnp.int32, (cpad, mrows), 0)
            zm = jnp.where(cls < classes, z2t, -jnp.inf)
            zs = zm - jnp.max(zm, axis=0, keepdims=True)
            logp = zs - jnp.log(jnp.sum(jnp.exp(zs), axis=0, keepdims=True))
            hot = cls == lab_ref[:, at]
            mask_f = msk_ref[:, at].astype(F32)
            loss_v = -mask_f * jnp.sum(jnp.where(hot, logp, 0.0), axis=0, keepdims=True)
            losses.append(jnp.sum(loss_v, axis=1, keepdims=True))
            g2[0, :, at] = ((jnp.exp(logp) - hot.astype(F32)) * (mask_f / total_m)).astype(BF16)
            send(g2.at[0, :, at], g2.at[1, :, at], 4, 0, g2_ss, g2_rs)

    gather(y2g, z2_work, z2_event, z2_tail)
    drain(g2.at[0], g2_ss)
    loss_part = (losses[0] + losses[1]) / total_m
    for cp in h1t_cps[1:]:
        cp.start()

    half = nb // 2
    units = ((3, 0), (3, 1), (1, 0), (2, 1), (2, 0), (1, 1), (0, 0), (0, 1))

    def tree(name, g, out, sibb, summ, rfwd, rfar, early):
        sib_ss, ss = new("send"), new("send")
        sib_rs = [new("recv") for _ in range(3)]
        sibf_rs = {(h, c): new("recv") for h in range(2) for c in range(2)}
        f_rs = {(h, c): new("recv") for h in range(2) for c in range(2)}
        x_rs = new("recv")
        y_rs = [new("recv") for _ in range(2)]
        drain(out, sib_ss)
        drain(summ.at[pl.ds(0, 6)], ss)

        def cols(h):
            return slice(h * half, (h + 1) * half)

        def own(q, h, dc):
            return dot(g[0], abuf[BACK[0, q, dc], :, cols(h)])

        def partner(q, h, dc):
            return dot(g[1], abuf[BACK[1, q, dc], :, cols(h)])

        def partner_piece(i, dc, c):
            q, h = units[i]
            lo = h * half + c * half // 2
            return dot(g[1], abuf[BACK[1, q, dc], :, lo:lo + half // 2])

        def piece(i, c):
            return (i, slice(None), slice(c * half // 2, (c + 1) * half // 2))

        def first_dim(h):
            return 1 if h == 0 else 2

        def begin():
            for i in range(early):
                out[i] = own(*units[i], 1)
                summ[i] = own(*units[i], 0)

        def first_group(between):
            with scope(name + "_group"):
                for c in range(2):
                    for i in range(2):
                        out[piece(i, c)] += partner_piece(i, 1, c)
                    for i in range(2):
                        send(out.at[piece(i, c)], sibb.at[piece(i, c)], 0, 1, sib_ss, sibf_rs[i, c])
            for c in range(2):
                with scope(name + "_group"):
                    for i in range(2):
                        summ[piece(i, c)] += partner_piece(i, 0, c)
                for i in range(2):
                    with scope(name + "_sib"):
                        landed(sibb.at[piece(i, c)], sibf_rs[i, c])
                    summ[piece(i, c)] += sibb[piece(i, c)]
                    send(summ.at[piece(i, c)], rfwd.at[piece(i, c)], first_dim(i), 0, ss, f_rs[i, c])
                if c == 0:
                    between()

        def group(j):
            pair = (2 * j, 2 * j + 1)
            with scope(name + "_group"):
                for i in pair:
                    if i < early:
                        out[i] += partner(*units[i], 1)
                    else:
                        out[i] = own(*units[i], 1) + partner(*units[i], 1)
                for i in pair:
                    send(out.at[i], sibb.at[i], 0, 1, sib_ss, sib_rs[j - 1])
                for i in pair:
                    if i < early:
                        summ[i] += partner(*units[i], 0)
                    else:
                        summ[i] = own(*units[i], 0) + partner(*units[i], 0)
            with scope(name + "_sib"):
                landed(sibb.at[pl.ds(2 * j, 2)], sib_rs[j - 1])
            for i in pair:
                q, h = units[i]
                summ[i] += sibb[i]
                if q == first_dim(h):
                    send(summ.at[i], rfar.at[h], first_dim(h), 0, ss, x_rs)

        def forward():
            for c in range(2):
                for h in range(2):
                    with scope(name + "_fwait"):
                        landed(rfwd.at[piece(h, c)], f_rs[h, c])
                    summ[piece(4 + h, c)] += rfwd[piece(h, c)]
                    send(summ.at[piece(4 + h, c)], rfar.at[piece(2 + h, c)], 3 - first_dim(h), 0, ss, y_rs[c])

        def collect():
            with scope(name + "_xwait"):
                landed(rfar.at[pl.ds(0, 2)], x_rs)
            for h in (0, 1):
                summ[6 + h] += rfar[h]

        def last(h, c):
            if h == 0:
                with scope(name + "_ywait"):
                    landed(rfar.at[0], y_rs[c])
            return (summ[piece(6 + h, c)] + rfar[piece(2 + h, c)]).astype(BF16)

        return begin, first_group, group, forward, collect, last

    begin, first_group, group, forward, collect, last = tree("p2", g2, p2out, p2sib, p2sum, p2fwd, p2far, 8)
    with scope("p2own"):
        for sem in range(1, 5):
            a_wait(0, 1 if sem == 1 else 2, sem)
        begin()
    with scope("g2z_wait"):
        landed(g2.at[1], g2_rs)
        a_wait(0, 2, 5)
    first_group(lambda: None)
    for sem in (6, 7):
        a_wait(0, 2, sem)
    group(1)
    group(2)
    forward()
    a_wait(0, 1, 8)
    group(3)
    collect()
    quarters = [(h, c, slice(h * half + c * half // 2, h * half + (c + 1) * half // 2)) for c in (0, 1) for h in (0, 1)]
    d2_rs, d2_ss = new("recv"), new("send")
    for h, c, at in quarters:
        d2[0, :, at] = last(h, c)
        send(d2.at[0, :, at], d2.at[1, :, at], 4, 0, d2_ss, d2_rs)
    drain(d2.at[0], d2_ss)

    g1 = y1

    def g1_of(i):
        g1[i] = jnp.where(h1t[i] > 0, dot(w2_ref[...], d2[i]), 0.0).astype(BF16)

    cls_row = lax.broadcasted_iota(jnp.int32, (cpad, hid), 0)
    part2[...] = jnp.where(cls_row == classes, loss_part, dot(d2[0], h1t[0], ((1,), (1,))))
    hc, hz = hid // 2, cpad // 2

    def span(start, size):
        return pl.ds(pl.multiple_of(start, size), size)

    w_ss = new("send")
    w_rs = [new("recv") for _ in range(6)]
    drain(p2out.at[0], w_ss)
    send(part2.at[:, span((1 - core) * hc, hc)], rbc, 0, 1, w_ss, w_rs[0])
    g1_of(0)

    begin, first_group, group, forward, collect, last = tree("p6", g1, p6out, p6sib, p6sum, p6fwd, p6far, 2)
    with scope("p6own"):
        begin()
    landed(rbc, w_rs[0])
    sumc[...] = part2[:, span(core * hc, hc)] + rbc[...]
    send(sumc.at[span((1 - r) * hz, hz)], rbz.at[0], 4, 0, w_ss, w_rs[1])
    with scope("d2z_wait"):
        landed(h1t.at[1], h1t_rs)
        landed(d2.at[1], d2_rs)
    with scope("g1b"):
        g1_of(1)

    def exchange_x():
        landed(rbz.at[0], w_rs[1])
        sumz[0] = sumc[span(r * hz, hz), :] + rbz[0]
        send(sumz.at[0], rbz.at[1], 1, 0, w_ss, w_rs[2])

    first_group(exchange_x)
    group(1)
    group(2)
    with scope("exchange_y"):
        landed(rbz.at[1], w_rs[2])
    sumz[1] = sumz[0] + rbz[1]
    send(sumz.at[1], rbz.at[2], 2, 0, w_ss, w_rs[3])
    forward()
    group(3)
    collect()
    mine = (span(r * hz, hz), span(core * hc, hc))
    landed(rbz.at[2], w_rs[3])
    res2[mine] = sumz[1] + rbz[2]
    send(res2.at[mine], res2.at[mine], 4, 0, w_ss, w_rs[4])
    landed(rbz.at[0], w_rs[4])
    mine = (slice(None), span(core * hc, hc))
    send(res2.at[mine], res2.at[mine], 0, 1, w_ss, w_rs[5])
    landed(rbc, w_rs[5])
    o2_ref[...] = res2[...]

    rows = rb1.shape[1]
    owners = part1.shape[0] // rows

    def owner(k, dc):
        rr, nn = coords(k, dc)
        chip = rr * 4 + nn // 2
        return chip, jnp.logical_and(nn % 2 == 1, chip < owners)

    own_id, owns = owner(0, 0)

    acc = None
    for h, c, at in quarters:
        term = dot(xg[0, :, at], last(h, c), ((1,), (1,)))
        acc = term if acc is None else acc + term
    part1[0:fpad, :] = acc
    red_ss = [new("send") for _ in range(2)]
    red_rs = [new("recv") for _ in range(2)]
    few, most = rb1.at[pl.ds(0, owners - 1)], rb1.at[pl.ds(0, owners)]
    with scope("red1"):
        for i, (k, dc) in enumerate(peers):
            peer_id, peer_owns = owner(k, dc)

            @pl.when(peer_owns)
            def _():
                send(part1.at[span(peer_id * rows, rows)], rb1.at[i], k, dc, red_ss[0], red_rs[0])

        @pl.when(owns)
        def _():
            mine = span(own_id * rows, rows)
            landed(rb1, red_rs[0])
            res1[mine, :] = part1[mine, :] + sum(rb1[i] for i in range(len(peers)))
            for k, dc in peers:
                send(res1.at[mine], res1.at[mine], k, dc, red_ss[1], red_rs[1])

    with scope("out1_wait"):
        @pl.when(owns)
        def _():
            landed(few, red_rs[1])

        @pl.when(jnp.logical_not(owns))
        def _():
            landed(most, red_rs[1])

    o1_ref[...] = res1[...]
    with scope("send_wait"):
        def drained(ref, ss):
            pltpu.make_async_copy(ref, ref, ssem.at[ss]).wait()

        for ref, ss in drains:
            drained(ref, ss)

        @pl.when(owns)
        def _():
            drained(few, red_ss[0])
            drained(rb1, red_ss[1])

        @pl.when(jnp.logical_not(owns))
        def _():
            drained(most, red_ss[0])
    assert used == {"send": ssem.shape[0], "recv": rsem.shape[0]}, used


def output_kernel(in1_ref, in2_ref, loss_ref, o1_ref, o2_ref):
    f_in, classes = o1_ref.shape[0], o2_ref.shape[0]
    o1_ref[...] = in1_ref[0:f_in, :]
    o2_ref[...] = in2_ref[0:classes, :]
    loss_ref[...] = in2_ref[classes:classes + 1, 0:1]


def solution(mesh):
    def local_step(adj_rows, features, w_one, w_two, labels, label_mask):
        nb, f_in = features.shape
        total = adj_rows.shape[1]
        hid, classes = w_two.shape
        cpad = 48
        lanes = 128
        fpad = 104
        frows = 112
        half = nb // 2
        nsend, nrecv = 12, 71
        anyspec = pl.BlockSpec(memory_space=pl.ANY)
        V = pltpu.VMEM
        dw1, dw2 = pl.pallas_call(
            functools.partial(step_kernel, nb, classes, f_in, cpad),
            out_shape=[V((frows, hid), F32), V((cpad, hid), F32)],
            in_specs=[anyspec] * 6,
            out_specs=[pl.BlockSpec(memory_space=pltpu.VMEM)] * 2,
            scratch_shapes=[
                V((total // nb, nb, nb), BF16), V((16, fpad, nb), BF16), V((2, hid, nb), BF16),
                V((nb, hid), F32), V((2, hid, nb), BF16), V((16, cpad, nb), BF16), V((nb, lanes), F32), V((2, cpad, nb), BF16),
                V((f_in, nb), BF16), V((f_in, hid), F32), V((classes, hid), F32), V((1, nb), jnp.int32), V((1, nb), jnp.int32),
                V((hid, fpad), BF16), V((hid, cpad), BF16), V((cpad, hid), BF16), V((lanes, hid), F32), V((lanes, hid), F32),
                V((8, cpad, half), F32), V((8, cpad, half), F32), V((8, cpad, half), F32), V((2, cpad, half), F32), V((4, cpad, half), F32),
                V((2, cpad, nb), BF16),
                V((8, hid, half), F32), V((8, hid, half), F32), V((8, hid, half), F32),
                V((2, hid, half), F32), V((4, hid, half), F32),
                V((frows, hid), F32), V((cpad, hid), F32), V((15, 16, hid), F32), V((cpad, hid // 2), F32),
                V((3, cpad // 2, hid // 2), F32), V((cpad, hid // 2), F32), V((2, cpad // 2, hid // 2), F32),
                V((frows, hid), F32), V((cpad, hid), F32),
                pltpu.SemaphoreType.DMA((9,)), pltpu.SemaphoreType.DMA((5,)),
                pltpu.SemaphoreType.DMA((nsend,)), pltpu.SemaphoreType.DMA((nrecv,)),
            ],
            compiler_params=pltpu.CompilerParams(collective_id=0, has_side_effects=True, vmem_limit_bytes=64 * 1000 * 1000),
            name="gcn_step",
        )(adj_rows, features.T, w_one, w_two.T, labels.reshape(1, nb), label_mask.reshape(1, nb))
        loss, dw1, dw2 = pl.pallas_call(
            output_kernel,
            out_shape=[jax.ShapeDtypeStruct((1, 1), F32), jax.ShapeDtypeStruct((f_in, hid), F32),
                       jax.ShapeDtypeStruct((classes, hid), F32)],
            name="outputs",
        )(*(pltpu.with_memory_space_constraint(v, pltpu.VMEM) for v in (dw1, dw2)))
        return loss.reshape(()), dw1, dw2.T

    row_spec = P(("nodes", "rep"))
    return jax.shard_map(local_step, mesh=mesh, in_specs=(P("nodes", None), P(("nodes", "rep"), None), P(), P(), row_spec, row_spec), out_specs=(P(), P(), P()), check_vma=False)
```

```python
import functools

import jax
import jax.numpy as jnp
from jax import lax
from jax.experimental import pallas as pl
from jax.experimental.pallas import tpu as pltpu
from jax.sharding import PartitionSpec as P

BF16 = jnp.bfloat16
F32 = jnp.float32
scope = jax.named_scope

ORDERS = ((1, 2, 4), (2, 4, 1), (4, 1, 2))
STAGES = (((0,) * 3,) + tuple(tuple(o[j] for o in ORDERS) for j in range(3))
          + tuple(tuple(o[a] + o[b] for o in ORDERS) for a, b in ((0, 1), (0, 2), (1, 2))) + ((7,) * 3,))
BACK = {key: slot for slot, key in enumerate(
    [(0, 0, 0), (0, 0, 1)] + [(0, k, dc) for k in (3, 1, 2) for dc in (1, 0)] + [(1, k, dc) for k in (3, 1, 2, 0) for dc in (1, 0)])}
COUNT_BASE = 32.0


def dot(a, b, dims=((1,), (0,))):
    return lax.dot_general(a, b, (dims, ((), ())), preferred_element_type=F32)


def step_kernel(nb, classes, f_in, cpad,
                a_hbm, x_hbm, w1_hbm, w2_hbm, lab_hbm, msk_hbm,
                o1_ref, o2_ref,
                abuf, xg, y1, z1, h1t, y2g, z2, g2,
                xraw, w1raw, w2raw, lab_ref, msk_ref, w1t_ref, w2_ref, w2t_ref, w1f, w2f,
                p2out, p2sib, p2sum, p2fwd, p2far, d2,
                p6out, p6sib, p6sum, p6fwd, p6far,
                part1, part2, rb1, rbc, rbz, sumc, sumz, res1, res2,
                asem, psem, ssem, rsem):
    r = lax.axis_index("rep")
    n = lax.axis_index("nodes")
    core = n % 2
    xc = (n // 2) % 2
    yc = n // 4
    hid = z1.shape[1]
    fpad = xg.shape[1]

    def flip(v, f):
        return 1 - v if f else v

    def coords(k, dc):
        rr = flip(r, k // 4)
        nn = flip(yc, (k // 2) % 2) * 4 + flip(xc, k % 2) * 2 + flip(core, dc)
        return rr, nn

    def block_id(k, dc):
        rr, nn = coords(k, dc)
        return nn * 2 + rr

    used = {"send": 0, "recv": 0}
    drains = []

    def new(kind):
        used[kind] += 1
        return used[kind] - 1

    def prepare(src, dst, k, dc, ss, rs):
        return pltpu.make_async_remote_copy(
            src_ref=src, dst_ref=dst, send_sem=ssem.at[ss], recv_sem=rsem.at[rs],
            device_id=coords(k, dc), device_id_type=pl.DeviceIdType.MESH)

    def send(*args):
        prepare(*args).start()

    def landed(ref, rs):
        pltpu.make_async_copy(ref, ref, rsem.at[rs]).wait()

    def drain(ref, ss):
        drains.append((ref, ss))

    peers = [(k, dc) for k in (7, 3, 5, 6, 1, 2, 4, 0) for dc in range(2) if (k, dc) != (0, 0)]

    pre = [pltpu.make_async_copy(src, dst, psem.at[i]) for i, (src, dst) in enumerate(
        ((x_hbm, xraw), (msk_hbm, msk_ref), (w1_hbm, w1raw), (w2_hbm, w2raw), (lab_hbm, lab_ref)))]
    for cp in pre:
        cp.start()
    barrier = pltpu.get_barrier_semaphore()
    near_peers = ((0, 1), (1, 0), (2, 0), (4, 0))
    for k, dc in near_peers:
        pl.semaphore_signal(barrier, inc=1, device_id=coords(k, dc), device_id_type=pl.DeviceIdType.MESH)
    z1[...] = jnp.zeros_like(z1)
    z2[...] = jnp.zeros_like(z2)
    part1[...] = jnp.zeros_like(part1)
    w1f[...] = jnp.zeros_like(w1f)
    w2f[...] = jnp.zeros_like(w2f)
    xg[0] = jnp.zeros((fpad, nb), BF16)
    with scope("entry_x"):
        pre[0].wait()
        pre[1].wait()

    third = (nb // 3 // 128 + 1) * 128
    cuts = [slice(0, third), slice(third, 2 * third), slice(2 * third, nb)]

    def a_load(rows, k, dc, slot, cut=slice(0, nb)):
        row = pl.multiple_of(rows * nb, nb)
        col = pl.multiple_of(block_id(k, dc) * nb + cut.start, 128)
        size = cut.stop - cut.start
        pltpu.make_async_copy(a_hbm.at[pl.ds(row, nb), pl.ds(col, size)], abuf.at[slot, :, cut], asem.at[0 if slot < 2 else (slot + 1) // 2]).start()

    def a_wait(base, count, sem):
        pltpu.make_async_copy(a_hbm.at[pl.ds(0, count * nb), pl.ds(0, nb)], a_hbm.at[pl.ds(0, count * nb), pl.ds(0, nb)], asem.at[sem]).wait()

    for slot in range(16):
        t, dc = slot // 2, slot % 2
        if t in (0, 7):
            a_load(r, STAGES[t][0], dc, slot)
        else:
            for p in range(3):
                a_load(r, STAGES[t][p], dc, slot, cuts[p])

    xg[0, 0:f_in, :] = xraw[...]
    count = jnp.sum(msk_ref[...].astype(F32), axis=1, keepdims=True)
    hi = jnp.floor(count * (1.0 / COUNT_BASE))
    lo = count - COUNT_BASE * hi
    row16 = lax.broadcasted_iota(jnp.int32, (8, 128), 0) + (fpad - 8)
    tail = xg[0, fpad - 8:fpad, 0:128].astype(F32)
    tail = jnp.where(row16 == f_in, hi, jnp.where(row16 == f_in + 1, lo, tail))
    xg[0, fpad - 8:fpad, 0:128] = tail.astype(BF16)
    with scope("entry_w"):
        for cp in pre[2:]:
            cp.wait()
    w1f[0:f_in, :] = w1raw[...]
    w1t_ref[...] = w1f[...].T[:, 0:fpad].astype(BF16)
    w2f[0:classes, :] = w2raw[...]
    w2t_ref[...] = w2f[0:cpad, :].astype(BF16)
    w2_ref[...] = w2f[...].T[:, 0:cpad].astype(BF16)
    with scope("entry_barrier"):
        pl.semaphore_wait(barrier, len(near_peers))

    def gather(buf, work, event, tail=None):
        ss = new("send")
        on = [new("recv") for _ in STAGES]
        ons = [new("recv") for _ in STAGES]

        def piece(slot, p):
            return buf.at[slot, :, cuts[p]]

        for j in range(3):
            for p, order in enumerate(ORDERS):
                send(piece(0, p), piece(2 * (1 + j), p), order[j], 0, ss, on[1 + j])
        sib = [prepare(buf.at[2 * t], buf.at[2 * t + 1], 0, 1, ss, ons[t]) for t in range(8)]
        sib[0].start()
        hops = {1: ((4, 1), (5, 2)), 2: ((6, 2),), 4: ((7, 2),)}
        onward = {t: [prepare(piece(2 * t, p), piece(2 * to, p), order[d], 0, ss, on[to]) for to, d in nxt for p, order in enumerate(ORDERS)]
                  for t, nxt in hops.items()}
        drain(buf.at[pl.ds(0, 15)], ss)

        def arrive(u):
            with scope(f"ev{u}"):
                landed(buf.at[0], on[u])
                for cp in onward.get(u, ()):
                    cp.start()
                sib[u].start()
                if u > 1:
                    landed(buf.at[0], ons[u - 1])

        with scope("ev0"):
            landed(buf.at[0], ons[0])
        work(0, 2)
        arrive(1)
        work(2, 1)


        @pl.loop(2, 8)
        def _(t):
            for u in range(2, 8):
                @pl.when(t == u)
                def _():
                    arrive(u)
                    event(u)
            with scope("pair"):
                work(2 * t - 1, 2)
        event(8)
        with scope("ev8"):
            landed(buf.at[0], ons[7])
        if tail:
            tail()
        else:
            work(15, 1)
        event(9)

    mrows = nb // 2

    def z1_work(base, count):
        a_wait(base, count, 0 if isinstance(base, int) and base == 0 else (base + 1) // 2)
        for j in range(count):
            y1[j] = dot(w1t_ref[...], xg[base + j]).astype(BF16)
        for m in range(0, nb, mrows):
            total = z1[m:m + mrows, :]
            for j in range(count):
                total = total + dot(abuf[base + j, m:m + mrows, :], y1[j], ((1,), (1,)))
            z1[m:m + mrows, :] = total

    gather(xg, z1_work, lambda t: None)

    with scope("h1y2"):
        for m in range(0, nb, 256):
            h1t[0, :, m:m + 256] = jnp.maximum(z1[m:m + 256, :], 0.0).T.astype(BF16)
        y2g[0] = dot(w2t_ref[...], h1t[0]).astype(BF16)

    def z2_work(base, count):
        for m in range(0, nb, mrows):
            total = z2[m:m + mrows, 0:cpad]
            for j in range(count):
                total = total + dot(abuf[base + j, m:m + mrows, :], y2g[base + j], ((1,), (1,)))
            z2[m:m + mrows, 0:cpad] = total

    chunk = hid // 4
    h1t_ss, h1t_rs = new("send"), new("recv")
    h1t_cps = [prepare(h1t.at[0, pl.ds(i * chunk, chunk)], h1t.at[1, pl.ds(i * chunk, chunk)], 4, 0, h1t_ss, h1t_rs) for i in range(4)]
    drain(h1t.at[0], h1t_ss)

    def z2_event(t):
        for (which, k, dc), slot in BACK.items():
            if slot > 1 and (slot + 1) // 2 == t - 1:
                a_load(flip(r, which), k, dc, slot)
        if t == 5:
            h1t_cps[0].start()

    tails = xg[0, fpad - 8:fpad, 0:128].astype(F32)
    for s in range(1, 16):
        tails = tails + xg[s, fpad - 8:fpad, 0:128].astype(F32)
    at_hi = f_in - (fpad - 8)
    total_m = COUNT_BASE * tails[at_hi:at_hi + 1, 0:1] + tails[at_hi + 1:at_hi + 2, 0:1]
    g2_rs, g2_ss = new("recv"), new("send")
    losses = []

    def z2_tail():
        for m in range(0, nb, mrows):
            at = slice(m, m + mrows)
            total = z2[at, 0:cpad]
            total = total + dot(abuf[15, at, :], y2g[15], ((1,), (1,)))
            z2[at, 0:cpad] = total
            z2t = z2[at, :].T[0:cpad, :]
            cls = lax.broadcasted_iota(jnp.int32, (cpad, mrows), 0)
            zm = jnp.where(cls < classes, z2t, -jnp.inf)
            zs = zm - jnp.max(zm, axis=0, keepdims=True)
            logp = zs - jnp.log(jnp.sum(jnp.exp(zs), axis=0, keepdims=True))
            hot = cls == lab_ref[:, at]
            mask_f = msk_ref[:, at].astype(F32)
            loss_v = -mask_f * jnp.sum(jnp.where(hot, logp, 0.0), axis=0, keepdims=True)
            losses.append(jnp.sum(loss_v, axis=1, keepdims=True))
            g2[0, :, at] = ((jnp.exp(logp) - hot.astype(F32)) * (mask_f / total_m)).astype(BF16)
            send(g2.at[0, :, at], g2.at[1, :, at], 4, 0, g2_ss, g2_rs)

    gather(y2g, z2_work, z2_event, z2_tail)
    drain(g2.at[0], g2_ss)
    loss_part = (losses[0] + losses[1]) / total_m
    for cp in h1t_cps[1:]:
        cp.start()

    half = nb // 2
    units = ((3, 0), (3, 1), (1, 0), (2, 1), (2, 0), (1, 1), (0, 0), (0, 1))

    def tree(name, g, out, sibb, summ, rfwd, rfar, early):
        sib_ss, ss = new("send"), new("send")
        sib_rs = [new("recv") for _ in range(3)]
        sibf_rs = {(h, c): new("recv") for h in range(2) for c in range(2)}
        f_rs = {(h, c): new("recv") for h in range(2) for c in range(2)}
        x_rs = new("recv")
        y_rs = [new("recv") for _ in range(2)]
        drain(out, sib_ss)
        drain(summ.at[pl.ds(0, 6)], ss)

        def cols(h):
            return slice(h * half, (h + 1) * half)

        def own(q, h, dc):
            return dot(g[0], abuf[BACK[0, q, dc], :, cols(h)])

        def partner(q, h, dc):
            return dot(g[1], abuf[BACK[1, q, dc], :, cols(h)])

        def partner_piece(i, dc, c):
            q, h = units[i]
            lo = h * half + c * half // 2
            return dot(g[1], abuf[BACK[1, q, dc], :, lo:lo + half // 2])

        def piece(i, c):
            return (i, slice(None), slice(c * half // 2, (c + 1) * half // 2))

        def first_dim(h):
            return 1 if h == 0 else 2

        def begin():
            for i in range(early):
                out[i] = own(*units[i], 1)
                summ[i] = own(*units[i], 0)

        def first_group(between, whole):
            def form(c):
                with scope(name + "_group"):
                    for i in range(2):
                        out[piece(i, c)] += partner_piece(i, 1, c)
                    for i in range(2):
                        send(out.at[piece(i, c)], sibb.at[piece(i, c)], 0, 1, sib_ss, sibf_rs[i, c])

            if whole:
                form(0)
                form(1)
            for c in range(2):
                if not whole:
                    form(c)
                with scope(name + "_group"):
                    for i in range(2):
                        summ[piece(i, c)] += partner_piece(i, 0, c)
                for i in range(2):
                    with scope(name + "_sib"):
                        landed(sibb.at[piece(i, c)], sibf_rs[i, c])
                    summ[piece(i, c)] += sibb[piece(i, c)]
                    send(summ.at[piece(i, c)], rfwd.at[piece(i, c)], first_dim(i), 0, ss, f_rs[i, c])
                if c == 0:
                    between()

        def group(j):
            pair = (2 * j, 2 * j + 1)
            with scope(name + "_group"):
                for i in pair:
                    if i < early:
                        out[i] += partner(*units[i], 1)
                    else:
                        out[i] = own(*units[i], 1) + partner(*units[i], 1)
                for i in pair:
                    send(out.at[i], sibb.at[i], 0, 1, sib_ss, sib_rs[j - 1])
                for i in pair:
                    if i < early:
                        summ[i] += partner(*units[i], 0)
                    else:
                        summ[i] = own(*units[i], 0) + partner(*units[i], 0)
            with scope(name + "_sib"):
                landed(sibb.at[pl.ds(2 * j, 2)], sib_rs[j - 1])
            for i in pair:
                q, h = units[i]
                summ[i] += sibb[i]
                if q == first_dim(h):
                    send(summ.at[i], rfar.at[h], first_dim(h), 0, ss, x_rs)

        def forward():
            for c in range(2):
                for h in range(2):
                    with scope(name + "_fwait"):
                        landed(rfwd.at[piece(h, c)], f_rs[h, c])
                    summ[piece(4 + h, c)] += rfwd[piece(h, c)]
                    send(summ.at[piece(4 + h, c)], rfar.at[piece(2 + h, c)], 3 - first_dim(h), 0, ss, y_rs[c])

        def collect():
            with scope(name + "_xwait"):
                landed(rfar.at[pl.ds(0, 2)], x_rs)
            for h in (0, 1):
                summ[6 + h] += rfar[h]

        def last(h, c):
            if h == 0:
                with scope(name + "_ywait"):
                    landed(rfar.at[0], y_rs[c])
            return (summ[piece(6 + h, c)] + rfar[piece(2 + h, c)]).astype(BF16)

        return begin, first_group, group, forward, collect, last

    begin, first_group, group, forward, collect, last = tree("p2", g2, p2out, p2sib, p2sum, p2fwd, p2far, 8)
    with scope("p2own"):
        for sem in range(1, 5):
            a_wait(0, 1 if sem == 1 else 2, sem)
        begin()
    with scope("g2z_wait"):
        landed(g2.at[1], g2_rs)
        a_wait(0, 2, 5)
    first_group(lambda: None, whole=True)
    for sem in (6, 7):
        a_wait(0, 2, sem)
    group(1)
    group(2)
    forward()
    a_wait(0, 1, 8)
    group(3)
    collect()
    quarters = [(h, c, slice(h * half + c * half // 2, h * half + (c + 1) * half // 2)) for c in (0, 1) for h in (0, 1)]
    d2_rs, d2_ss = new("recv"), new("send")
    for h, c, at in quarters:
        d2[0, :, at] = last(h, c)
        send(d2.at[0, :, at], d2.at[1, :, at], 4, 0, d2_ss, d2_rs)
    drain(d2.at[0], d2_ss)

    g1 = y1

    def g1_of(i):
        g1[i] = jnp.where(h1t[i] > 0, dot(w2_ref[...], d2[i]), 0.0).astype(BF16)

    cls_row = lax.broadcasted_iota(jnp.int32, (cpad, hid), 0)
    part2[...] = jnp.where(cls_row == classes, loss_part, dot(d2[0], h1t[0], ((1,), (1,))))
    hc, hz = hid // 2, cpad // 2

    def span(start, size):
        return pl.ds(pl.multiple_of(start, size), size)

    w_ss = new("send")
    w_rs = [new("recv") for _ in range(6)]
    drain(p2out.at[0], w_ss)
    send(part2.at[:, span((1 - core) * hc, hc)], rbc, 0, 1, w_ss, w_rs[0])
    g1_of(0)

    begin, first_group, group, forward, collect, last = tree("p6", g1, p6out, p6sib, p6sum, p6fwd, p6far, 2)
    with scope("p6own"):
        begin()
    landed(rbc, w_rs[0])
    sumc[...] = part2[:, span(core * hc, hc)] + rbc[...]
    send(sumc.at[span((1 - r) * hz, hz)], rbz.at[0], 4, 0, w_ss, w_rs[1])
    with scope("d2z_wait"):
        landed(h1t.at[1], h1t_rs)
        landed(d2.at[1], d2_rs)
    with scope("g1b"):
        g1_of(1)

    def exchange_x():
        landed(rbz.at[0], w_rs[1])
        sumz[0] = sumc[span(r * hz, hz), :] + rbz[0]
        send(sumz.at[0], rbz.at[1], 1, 0, w_ss, w_rs[2])

    first_group(exchange_x, whole=False)
    group(1)
    group(2)
    with scope("exchange_y"):
        landed(rbz.at[1], w_rs[2])
    sumz[1] = sumz[0] + rbz[1]
    send(sumz.at[1], rbz.at[2], 2, 0, w_ss, w_rs[3])
    forward()
    group(3)
    collect()
    mine = (span(r * hz, hz), span(core * hc, hc))
    landed(rbz.at[2], w_rs[3])
    res2[mine] = sumz[1] + rbz[2]
    send(res2.at[mine], res2.at[mine], 4, 0, w_ss, w_rs[4])
    landed(rbz.at[0], w_rs[4])
    mine = (slice(None), span(core * hc, hc))
    send(res2.at[mine], res2.at[mine], 0, 1, w_ss, w_rs[5])
    landed(rbc, w_rs[5])
    o2_ref[...] = res2[...]

    rows = rb1.shape[1]
    owners = part1.shape[0] // rows

    def owner(k, dc):
        rr, nn = coords(k, dc)
        chip = rr * 4 + nn // 2
        return chip, jnp.logical_and(nn % 2 == 1, chip < owners)

    own_id, owns = owner(0, 0)

    acc = None
    for h, c, at in quarters:
        term = dot(xg[0, :, at], last(h, c), ((1,), (1,)))
        acc = term if acc is None else acc + term
    part1[0:fpad, :] = acc
    red_ss = [new("send") for _ in range(2)]
    red_rs = [new("recv") for _ in range(2)]
    few, most = rb1.at[pl.ds(0, owners - 1)], rb1.at[pl.ds(0, owners)]
    with scope("red1"):
        for i, (k, dc) in enumerate(peers):
            peer_id, peer_owns = owner(k, dc)

            @pl.when(peer_owns)
            def _():
                send(part1.at[span(peer_id * rows, rows)], rb1.at[i], k, dc, red_ss[0], red_rs[0])

        @pl.when(owns)
        def _():
            mine = span(own_id * rows, rows)
            landed(rb1, red_rs[0])
            res1[mine, :] = part1[mine, :] + sum(rb1[i] for i in range(len(peers)))
            for k, dc in peers:
                send(res1.at[mine], res1.at[mine], k, dc, red_ss[1], red_rs[1])

    with scope("out1_wait"):
        @pl.when(owns)
        def _():
            landed(few, red_rs[1])

        @pl.when(jnp.logical_not(owns))
        def _():
            landed(most, red_rs[1])

    o1_ref[...] = res1[...]
    with scope("send_wait"):
        def drained(ref, ss):
            pltpu.make_async_copy(ref, ref, ssem.at[ss]).wait()

        for ref, ss in drains:
            drained(ref, ss)

        @pl.when(owns)
        def _():
            drained(few, red_ss[0])
            drained(rb1, red_ss[1])

        @pl.when(jnp.logical_not(owns))
        def _():
            drained(most, red_ss[0])
    assert used == {"send": ssem.shape[0], "recv": rsem.shape[0]}, used


def output_kernel(in1_ref, in2_ref, loss_ref, o1_ref, o2_ref):
    f_in, classes = o1_ref.shape[0], o2_ref.shape[0]
    o1_ref[...] = in1_ref[0:f_in, :]
    o2_ref[...] = in2_ref[0:classes, :]
    loss_ref[...] = in2_ref[classes:classes + 1, 0:1]


def solution(mesh):
    def local_step(adj_rows, features, w_one, w_two, labels, label_mask):
        nb, f_in = features.shape
        total = adj_rows.shape[1]
        hid, classes = w_two.shape
        cpad = 48
        lanes = 128
        fpad = 104
        frows = 112
        half = nb // 2
        nsend, nrecv = 12, 71
        anyspec = pl.BlockSpec(memory_space=pl.ANY)
        V = pltpu.VMEM
        dw1, dw2 = pl.pallas_call(
            functools.partial(step_kernel, nb, classes, f_in, cpad),
            out_shape=[V((frows, hid), F32), V((cpad, hid), F32)],
            in_specs=[anyspec] * 6,
            out_specs=[pl.BlockSpec(memory_space=pltpu.VMEM)] * 2,
            scratch_shapes=[
                V((total // nb, nb, nb), BF16), V((16, fpad, nb), BF16), V((2, hid, nb), BF16),
                V((nb, hid), F32), V((2, hid, nb), BF16), V((16, cpad, nb), BF16), V((nb, lanes), F32), V((2, cpad, nb), BF16),
                V((f_in, nb), BF16), V((f_in, hid), F32), V((classes, hid), F32), V((1, nb), jnp.int32), V((1, nb), jnp.int32),
                V((hid, fpad), BF16), V((hid, cpad), BF16), V((cpad, hid), BF16), V((lanes, hid), F32), V((lanes, hid), F32),
                V((8, cpad, half), F32), V((8, cpad, half), F32), V((8, cpad, half), F32), V((2, cpad, half), F32), V((4, cpad, half), F32),
                V((2, cpad, nb), BF16),
                V((8, hid, half), F32), V((8, hid, half), F32), V((8, hid, half), F32),
                V((2, hid, half), F32), V((4, hid, half), F32),
                V((frows, hid), F32), V((cpad, hid), F32), V((15, 16, hid), F32), V((cpad, hid // 2), F32),
                V((3, cpad // 2, hid // 2), F32), V((cpad, hid // 2), F32), V((2, cpad // 2, hid // 2), F32),
                V((frows, hid), F32), V((cpad, hid), F32),
                pltpu.SemaphoreType.DMA((9,)), pltpu.SemaphoreType.DMA((5,)),
                pltpu.SemaphoreType.DMA((nsend,)), pltpu.SemaphoreType.DMA((nrecv,)),
            ],
            compiler_params=pltpu.CompilerParams(collective_id=0, has_side_effects=True, vmem_limit_bytes=64 * 1000 * 1000),
            name="gcn_step",
        )(adj_rows, features.T, w_one, w_two.T, labels.reshape(1, nb), label_mask.reshape(1, nb))
        loss, dw1, dw2 = pl.pallas_call(
            output_kernel,
            out_shape=[jax.ShapeDtypeStruct((1, 1), F32), jax.ShapeDtypeStruct((f_in, hid), F32),
                       jax.ShapeDtypeStruct((classes, hid), F32)],
            name="outputs",
        )(*(pltpu.with_memory_space_constraint(v, pltpu.VMEM) for v in (dw1, dw2)))
        return loss.reshape(()), dw1, dw2.T

    row_spec = P(("nodes", "rep"))
    return jax.shard_map(local_step, mesh=mesh, in_specs=(P("nodes", None), P(("nodes", "rep"), None), P(), P(), row_spec, row_spec), out_specs=(P(), P(), P()), check_vma=False)
```

```python
import functools

import jax
import jax.numpy as jnp
from jax import lax
from jax.experimental import pallas as pl
from jax.experimental.pallas import tpu as pltpu
from jax.sharding import PartitionSpec as P

BF16 = jnp.bfloat16
F32 = jnp.float32
scope = jax.named_scope

ORDERS = ((1, 2, 4), (2, 4, 1), (4, 1, 2))
STAGES = (((0,) * 3,) + tuple(tuple(o[j] for o in ORDERS) for j in range(3))
          + tuple(tuple(o[a] + o[b] for o in ORDERS) for a, b in ((0, 1), (0, 2), (1, 2))) + ((7,) * 3,))
BACK = {key: slot for slot, key in enumerate(
    [(0, 0, 0), (0, 0, 1)] + [(0, k, dc) for k in (3, 1, 2) for dc in (1, 0)] + [(1, k, dc) for k in (3, 1, 2, 0) for dc in (1, 0)])}
COUNT_BASE = 32.0


def dot(a, b, dims=((1,), (0,))):
    return lax.dot_general(a, b, (dims, ((), ())), preferred_element_type=F32)


def step_kernel(nb, classes, f_in, cpad,
                a_hbm, x_hbm, w1_hbm, w2_hbm, lab_hbm, msk_hbm,
                o1_ref, o2_ref,
                abuf, xg, y1, z1, h1t, y2g, z2, g2,
                xraw, w1raw, w2raw, lab_ref, msk_ref, w1t_ref, w2_ref, w2t_ref, w1f, w2f,
                p2out, p2sib, p2sum, p2fwd, p2far, d2,
                p6out, p6sib, p6sum, p6fwd, p6far,
                part1, part2, rb1, rbc, rbz, sumc, sumz, res1, res2,
                asem, psem, ssem, rsem):
    r = lax.axis_index("rep")
    n = lax.axis_index("nodes")
    core = n % 2
    xc = (n // 2) % 2
    yc = n // 4
    hid = z1.shape[1]
    fpad = xg.shape[1]

    def flip(v, f):
        return 1 - v if f else v

    def coords(k, dc):
        rr = flip(r, k // 4)
        nn = flip(yc, (k // 2) % 2) * 4 + flip(xc, k % 2) * 2 + flip(core, dc)
        return rr, nn

    def block_id(k, dc):
        rr, nn = coords(k, dc)
        return nn * 2 + rr

    used = {"send": 0, "recv": 0}
    drains = []

    def new(kind):
        used[kind] += 1
        return used[kind] - 1

    def prepare(src, dst, k, dc, ss, rs):
        return pltpu.make_async_remote_copy(
            src_ref=src, dst_ref=dst, send_sem=ssem.at[ss], recv_sem=rsem.at[rs],
            device_id=coords(k, dc), device_id_type=pl.DeviceIdType.MESH)

    def send(*args):
        prepare(*args).start()

    def landed(ref, rs):
        pltpu.make_async_copy(ref, ref, rsem.at[rs]).wait()

    def drain(ref, ss):
        drains.append((ref, ss))

    peers = [(k, dc) for k in (7, 3, 5, 6, 1, 2, 4, 0) for dc in range(2) if (k, dc) != (0, 0)]

    pre = [pltpu.make_async_copy(src, dst, psem.at[i]) for i, (src, dst) in enumerate(
        ((x_hbm, xraw), (msk_hbm, msk_ref), (w1_hbm, w1raw), (w2_hbm, w2raw), (lab_hbm, lab_ref)))]
    for cp in pre:
        cp.start()
    barrier = pltpu.get_barrier_semaphore()
    near_peers = ((0, 1), (1, 0), (2, 0), (4, 0))
    for k, dc in near_peers:
        pl.semaphore_signal(barrier, inc=1, device_id=coords(k, dc), device_id_type=pl.DeviceIdType.MESH)
    z1[...] = jnp.zeros_like(z1)
    z2[...] = jnp.zeros_like(z2)
    part1[...] = jnp.zeros_like(part1)
    w1f[...] = jnp.zeros_like(w1f)
    w2f[...] = jnp.zeros_like(w2f)
    xg[0] = jnp.zeros((fpad, nb), BF16)
    with scope("entry_x"):
        pre[0].wait()
        pre[1].wait()

    third = (nb // 3 // 128 + 1) * 128
    cuts = [slice(0, third), slice(third, 2 * third), slice(2 * third, nb)]

    def a_load(rows, k, dc, slot, cut=slice(0, nb)):
        row = pl.multiple_of(rows * nb, nb)
        col = pl.multiple_of(block_id(k, dc) * nb + cut.start, 128)
        size = cut.stop - cut.start
        pltpu.make_async_copy(a_hbm.at[pl.ds(row, nb), pl.ds(col, size)], abuf.at[slot, :, cut], asem.at[0 if slot < 2 else (slot + 1) // 2]).start()

    def a_wait(base, count, sem):
        pltpu.make_async_copy(a_hbm.at[pl.ds(0, count * nb), pl.ds(0, nb)], a_hbm.at[pl.ds(0, count * nb), pl.ds(0, nb)], asem.at[sem]).wait()

    for slot in range(16):
        t, dc = slot // 2, slot % 2
        if t in (0, 7):
            a_load(r, STAGES[t][0], dc, slot)
        else:
            for p in range(3):
                a_load(r, STAGES[t][p], dc, slot, cuts[p])

    xg[0, 0:f_in, :] = xraw[...]
    count = jnp.sum(msk_ref[...].astype(F32), axis=1, keepdims=True)
    hi = jnp.floor(count * (1.0 / COUNT_BASE))
    lo = count - COUNT_BASE * hi
    row16 = lax.broadcasted_iota(jnp.int32, (8, 128), 0) + (fpad - 8)
    tail = xg[0, fpad - 8:fpad, 0:128].astype(F32)
    tail = jnp.where(row16 == f_in, hi, jnp.where(row16 == f_in + 1, lo, tail))
    xg[0, fpad - 8:fpad, 0:128] = tail.astype(BF16)
    with scope("entry_w"):
        for cp in pre[2:]:
            cp.wait()
    w1f[0:f_in, :] = w1raw[...]
    w1t_ref[...] = w1f[...].T[:, 0:fpad].astype(BF16)
    w2f[0:classes, :] = w2raw[...]
    w2t_ref[...] = w2f[0:cpad, :].astype(BF16)
    w2_ref[...] = w2f[...].T[:, 0:cpad].astype(BF16)
    with scope("entry_barrier"):
        pl.semaphore_wait(barrier, len(near_peers))

    def gather(buf, work, event, tail=None):
        ss = new("send")
        on = [new("recv") for _ in STAGES]
        ons = [new("recv") for _ in STAGES]

        def piece(slot, p):
            return buf.at[slot, :, cuts[p]]

        for j in range(3):
            for p, order in enumerate(ORDERS):
                send(piece(0, p), piece(2 * (1 + j), p), order[j], 0, ss, on[1 + j])
        sib = [prepare(buf.at[2 * t], buf.at[2 * t + 1], 0, 1, ss, ons[t]) for t in range(8)]
        sib[0].start()
        hops = {1: ((4, 1), (5, 2)), 2: ((6, 2),), 4: ((7, 2),)}
        onward = {t: [prepare(piece(2 * t, p), piece(2 * to, p), order[d], 0, ss, on[to]) for to, d in nxt for p, order in enumerate(ORDERS)]
                  for t, nxt in hops.items()}
        drain(buf.at[pl.ds(0, 15)], ss)

        def arrive(u):
            with scope(f"ev{u}"):
                landed(buf.at[0], on[u])
                for cp in onward.get(u, ()):
                    cp.start()
                sib[u].start()
                if u > 1:
                    landed(buf.at[0], ons[u - 1])

        with scope("ev0"):
            landed(buf.at[0], ons[0])
        work(0, 2)
        arrive(1)
        work(2, 1)


        @pl.loop(2, 8)
        def _(t):
            for u in range(2, 8):
                @pl.when(t == u)
                def _():
                    arrive(u)
                    event(u)
            with scope("pair"):
                work(2 * t - 1, 2)
        event(8)
        with scope("ev8"):
            landed(buf.at[0], ons[7])
        if tail:
            tail()
        else:
            work(15, 1)
        event(9)

    mrows = nb // 2

    def z1_work(base, count):
        a_wait(base, count, 0 if isinstance(base, int) and base == 0 else (base + 1) // 2)
        for j in range(count):
            y1[j] = dot(w1t_ref[...], xg[base + j]).astype(BF16)
        for m in range(0, nb, mrows):
            total = z1[m:m + mrows, :]
            for j in range(count):
                total = total + dot(abuf[base + j, m:m + mrows, :], y1[j], ((1,), (1,)))
            z1[m:m + mrows, :] = total

    gather(xg, z1_work, lambda t: None)

    with scope("h1y2"):
        for m in range(0, nb, 256):
            h1t[0, :, m:m + 256] = jnp.maximum(z1[m:m + 256, :], 0.0).T.astype(BF16)
        y2g[0] = dot(w2t_ref[...], h1t[0]).astype(BF16)

    def z2_work(base, count):
        for m in range(0, nb, mrows):
            total = z2[m:m + mrows, 0:cpad]
            for j in range(count):
                total = total + dot(abuf[base + j, m:m + mrows, :], y2g[base + j], ((1,), (1,)))
            z2[m:m + mrows, 0:cpad] = total

    chunk = hid // 4
    h1t_ss, h1t_rs = new("send"), new("recv")
    h1t_cps = [prepare(h1t.at[0, pl.ds(i * chunk, chunk)], h1t.at[1, pl.ds(i * chunk, chunk)], 4, 0, h1t_ss, h1t_rs) for i in range(4)]
    drain(h1t.at[0], h1t_ss)

    def z2_event(t):
        for (which, k, dc), slot in BACK.items():
            if slot > 1 and (slot + 1) // 2 == t - 1:
                a_load(flip(r, which), k, dc, slot)
        if t == 5:
            h1t_cps[0].start()

    tails = xg[0, fpad - 8:fpad, 0:128].astype(F32)
    for s in range(1, 16):
        tails = tails + xg[s, fpad - 8:fpad, 0:128].astype(F32)
    at_hi = f_in - (fpad - 8)
    total_m = COUNT_BASE * tails[at_hi:at_hi + 1, 0:1] + tails[at_hi + 1:at_hi + 2, 0:1]
    g2_rs, g2_ss = new("recv"), new("send")
    losses = []

    def z2_tail():
        for m in range(0, nb, mrows):
            at = slice(m, m + mrows)
            total = z2[at, 0:cpad]
            total = total + dot(abuf[15, at, :], y2g[15], ((1,), (1,)))
            z2[at, 0:cpad] = total
            z2t = z2[at, :].T[0:cpad, :]
            cls = lax.broadcasted_iota(jnp.int32, (cpad, mrows), 0)
            zm = jnp.where(cls < classes, z2t, -jnp.inf)
            zs = zm - jnp.max(zm, axis=0, keepdims=True)
            logp = zs - jnp.log(jnp.sum(jnp.exp(zs), axis=0, keepdims=True))
            hot = cls == lab_ref[:, at]
            mask_f = msk_ref[:, at].astype(F32)
            loss_v = -mask_f * jnp.sum(jnp.where(hot, logp, 0.0), axis=0, keepdims=True)
            losses.append(jnp.sum(loss_v, axis=1, keepdims=True))
            g2[0, :, at] = ((jnp.exp(logp) - hot.astype(F32)) * (mask_f / total_m)).astype(BF16)
            send(g2.at[0, :, at], g2.at[1, :, at], 4, 0, g2_ss, g2_rs)

    gather(y2g, z2_work, z2_event, z2_tail)
    drain(g2.at[0], g2_ss)
    loss_part = (losses[0] + losses[1]) / total_m
    for cp in h1t_cps[1:]:
        cp.start()

    half = nb // 2
    units = ((3, 0), (3, 1), (1, 0), (2, 1), (2, 0), (1, 1), (0, 0), (0, 1))

    def tree(name, g, out, sibb, summ, rfwd, rfar, early):
        sib_ss, ss = new("send"), new("send")
        sib_rs = [new("recv") for _ in range(3)]
        sibf_rs = {(h, c): new("recv") for h in range(2) for c in range(2)}
        f_rs = {(h, c): new("recv") for h in range(2) for c in range(2)}
        x_rs = new("recv")
        y_rs = [new("recv") for _ in range(2)]
        drain(out, sib_ss)
        drain(summ.at[pl.ds(0, 6)], ss)

        def cols(h):
            return slice(h * half, (h + 1) * half)

        def own(q, h, dc):
            return dot(g[0], abuf[BACK[0, q, dc], :, cols(h)])

        def partner(q, h, dc):
            return dot(g[1], abuf[BACK[1, q, dc], :, cols(h)])

        def partner_piece(i, dc, c):
            q, h = units[i]
            lo = h * half + c * half // 2
            return dot(g[1], abuf[BACK[1, q, dc], :, lo:lo + half // 2])

        def piece(i, c):
            return (i, slice(None), slice(c * half // 2, (c + 1) * half // 2))

        def first_dim(h):
            return 1 if h == 0 else 2

        def begin():
            for i in range(early):
                out[i] = own(*units[i], 1)
                summ[i] = own(*units[i], 0)

        def first_group(between, whole):
            def form(c):
                with scope(name + "_group"):
                    for i in range(2):
                        out[piece(i, c)] += partner_piece(i, 1, c)
                    for i in range(2):
                        send(out.at[piece(i, c)], sibb.at[piece(i, c)], 0, 1, sib_ss, sibf_rs[i, c])

            if whole:
                form(0)
                form(1)
            for c in range(2):
                if not whole:
                    form(c)
                with scope(name + "_group"):
                    for i in range(2):
                        summ[piece(i, c)] += partner_piece(i, 0, c)
                for i in range(2):
                    with scope(name + "_sib"):
                        landed(sibb.at[piece(i, c)], sibf_rs[i, c])
                    summ[piece(i, c)] += sibb[piece(i, c)]
                    send(summ.at[piece(i, c)], rfwd.at[piece(i, c)], first_dim(i), 0, ss, f_rs[i, c])
                if c == 0:
                    between()

        def group_out(j):
            pair = (2 * j, 2 * j + 1)
            with scope(name + "_group"):
                for i in pair:
                    if i < early:
                        out[i] += partner(*units[i], 1)
                    else:
                        out[i] = own(*units[i], 1) + partner(*units[i], 1)
                for i in pair:
                    send(out.at[i], sibb.at[i], 0, 1, sib_ss, sib_rs[j - 1])

        def group(j, formed=False):
            pair = (2 * j, 2 * j + 1)
            if not formed:
                group_out(j)
            with scope(name + "_group"):
                for i in pair:
                    if i < early:
                        summ[i] += partner(*units[i], 0)
                    else:
                        summ[i] = own(*units[i], 0) + partner(*units[i], 0)
            with scope(name + "_sib"):
                landed(sibb.at[pl.ds(2 * j, 2)], sib_rs[j - 1])
            for i in pair:
                q, h = units[i]
                summ[i] += sibb[i]
                if q == first_dim(h):
                    send(summ.at[i], rfar.at[h], first_dim(h), 0, ss, x_rs)

        def forward():
            for c in range(2):
                for h in range(2):
                    with scope(name + "_fwait"):
                        landed(rfwd.at[piece(h, c)], f_rs[h, c])
                    summ[piece(4 + h, c)] += rfwd[piece(h, c)]
                    send(summ.at[piece(4 + h, c)], rfar.at[piece(2 + h, c)], 3 - first_dim(h), 0, ss, y_rs[c])

        def collect():
            with scope(name + "_xwait"):
                landed(rfar.at[pl.ds(0, 2)], x_rs)
            for h in (0, 1):
                summ[6 + h] += rfar[h]

        def last(h, c):
            if h == 0:
                with scope(name + "_ywait"):
                    landed(rfar.at[0], y_rs[c])
            return (summ[piece(6 + h, c)] + rfar[piece(2 + h, c)]).astype(BF16)

        return begin, first_group, group_out, group, forward, collect, last

    begin, first_group, group_out, group, forward, collect, last = tree("p2", g2, p2out, p2sib, p2sum, p2fwd, p2far, 8)
    with scope("p2own"):
        for sem in range(1, 5):
            a_wait(0, 1 if sem == 1 else 2, sem)
        begin()
    with scope("g2z_wait"):
        landed(g2.at[1], g2_rs)
        a_wait(0, 2, 5)
    def next_outs():
        for sem in (6, 7):
            a_wait(0, 2, sem)
        group_out(1)

    first_group(next_outs, whole=True)
    group(1, formed=True)
    group(2)
    forward()
    a_wait(0, 1, 8)
    group(3)
    collect()
    quarters = [(h, c, slice(h * half + c * half // 2, h * half + (c + 1) * half // 2)) for c in (0, 1) for h in (0, 1)]
    d2_rs, d2_ss = new("recv"), new("send")
    for h, c, at in quarters:
        d2[0, :, at] = last(h, c)
        send(d2.at[0, :, at], d2.at[1, :, at], 4, 0, d2_ss, d2_rs)
    drain(d2.at[0], d2_ss)

    g1 = y1

    def g1_of(i):
        g1[i] = jnp.where(h1t[i] > 0, dot(w2_ref[...], d2[i]), 0.0).astype(BF16)

    cls_row = lax.broadcasted_iota(jnp.int32, (cpad, hid), 0)
    part2[...] = jnp.where(cls_row == classes, loss_part, dot(d2[0], h1t[0], ((1,), (1,))))
    hc, hz = hid // 2, cpad // 2

    def span(start, size):
        return pl.ds(pl.multiple_of(start, size), size)

    w_ss = new("send")
    w_rs = [new("recv") for _ in range(6)]
    drain(p2out.at[0], w_ss)
    send(part2.at[:, span((1 - core) * hc, hc)], rbc, 0, 1, w_ss, w_rs[0])
    g1_of(0)

    begin, first_group, _, group, forward, collect, last = tree("p6", g1, p6out, p6sib, p6sum, p6fwd, p6far, 2)
    with scope("p6own"):
        begin()
    landed(rbc, w_rs[0])
    sumc[...] = part2[:, span(core * hc, hc)] + rbc[...]
    send(sumc.at[span((1 - r) * hz, hz)], rbz.at[0], 4, 0, w_ss, w_rs[1])
    with scope("d2z_wait"):
        landed(h1t.at[1], h1t_rs)
        landed(d2.at[1], d2_rs)
    with scope("g1b"):
        g1_of(1)

    def exchange_x():
        landed(rbz.at[0], w_rs[1])
        sumz[0] = sumc[span(r * hz, hz), :] + rbz[0]
        send(sumz.at[0], rbz.at[1], 1, 0, w_ss, w_rs[2])

    first_group(exchange_x, whole=False)
    group(1)
    group(2)
    with scope("exchange_y"):
        landed(rbz.at[1], w_rs[2])
    sumz[1] = sumz[0] + rbz[1]
    send(sumz.at[1], rbz.at[2], 2, 0, w_ss, w_rs[3])
    forward()
    group(3)
    collect()
    mine = (span(r * hz, hz), span(core * hc, hc))
    landed(rbz.at[2], w_rs[3])
    res2[mine] = sumz[1] + rbz[2]
    send(res2.at[mine], res2.at[mine], 4, 0, w_ss, w_rs[4])
    landed(rbz.at[0], w_rs[4])
    mine = (slice(None), span(core * hc, hc))
    send(res2.at[mine], res2.at[mine], 0, 1, w_ss, w_rs[5])
    landed(rbc, w_rs[5])
    o2_ref[...] = res2[...]

    rows = rb1.shape[1]
    owners = part1.shape[0] // rows

    def owner(k, dc):
        rr, nn = coords(k, dc)
        chip = rr * 4 + nn // 2
        return chip, jnp.logical_and(nn % 2 == 1, chip < owners)

    own_id, owns = owner(0, 0)

    acc = None
    for h, c, at in quarters:
        term = dot(xg[0, :, at], last(h, c), ((1,), (1,)))
        acc = term if acc is None else acc + term
    part1[0:fpad, :] = acc
    red_ss = [new("send") for _ in range(2)]
    red_rs = [new("recv") for _ in range(2)]
    few, most = rb1.at[pl.ds(0, owners - 1)], rb1.at[pl.ds(0, owners)]
    with scope("red1"):
        for i, (k, dc) in enumerate(peers):
            peer_id, peer_owns = owner(k, dc)

            @pl.when(peer_owns)
            def _():
                send(part1.at[span(peer_id * rows, rows)], rb1.at[i], k, dc, red_ss[0], red_rs[0])

        @pl.when(owns)
        def _():
            mine = span(own_id * rows, rows)
            landed(rb1, red_rs[0])
            res1[mine, :] = part1[mine, :] + sum(rb1[i] for i in range(len(peers)))
            for k, dc in peers:
                send(res1.at[mine], res1.at[mine], k, dc, red_ss[1], red_rs[1])

    with scope("out1_wait"):
        @pl.when(owns)
        def _():
            landed(few, red_rs[1])

        @pl.when(jnp.logical_not(owns))
        def _():
            landed(most, red_rs[1])

    o1_ref[...] = res1[...]
    with scope("send_wait"):
        def drained(ref, ss):
            pltpu.make_async_copy(ref, ref, ssem.at[ss]).wait()

        for ref, ss in drains:
            drained(ref, ss)

        @pl.when(owns)
        def _():
            drained(few, red_ss[0])
            drained(rb1, red_ss[1])

        @pl.when(jnp.logical_not(owns))
        def _():
            drained(most, red_ss[0])
    assert used == {"send": ssem.shape[0], "recv": rsem.shape[0]}, used


def output_kernel(in1_ref, in2_ref, loss_ref, o1_ref, o2_ref):
    f_in, classes = o1_ref.shape[0], o2_ref.shape[0]
    o1_ref[...] = in1_ref[0:f_in, :]
    o2_ref[...] = in2_ref[0:classes, :]
    loss_ref[...] = in2_ref[classes:classes + 1, 0:1]


def solution(mesh):
    def local_step(adj_rows, features, w_one, w_two, labels, label_mask):
        nb, f_in = features.shape
        total = adj_rows.shape[1]
        hid, classes = w_two.shape
        cpad = 48
        lanes = 128
        fpad = 104
        frows = 112
        half = nb // 2
        nsend, nrecv = 12, 71
        anyspec = pl.BlockSpec(memory_space=pl.ANY)
        V = pltpu.VMEM
        dw1, dw2 = pl.pallas_call(
            functools.partial(step_kernel, nb, classes, f_in, cpad),
            out_shape=[V((frows, hid), F32), V((cpad, hid), F32)],
            in_specs=[anyspec] * 6,
            out_specs=[pl.BlockSpec(memory_space=pltpu.VMEM)] * 2,
            scratch_shapes=[
                V((total // nb, nb, nb), BF16), V((16, fpad, nb), BF16), V((2, hid, nb), BF16),
                V((nb, hid), F32), V((2, hid, nb), BF16), V((16, cpad, nb), BF16), V((nb, lanes), F32), V((2, cpad, nb), BF16),
                V((f_in, nb), BF16), V((f_in, hid), F32), V((classes, hid), F32), V((1, nb), jnp.int32), V((1, nb), jnp.int32),
                V((hid, fpad), BF16), V((hid, cpad), BF16), V((cpad, hid), BF16), V((lanes, hid), F32), V((lanes, hid), F32),
                V((8, cpad, half), F32), V((8, cpad, half), F32), V((8, cpad, half), F32), V((2, cpad, half), F32), V((4, cpad, half), F32),
                V((2, cpad, nb), BF16),
                V((8, hid, half), F32), V((8, hid, half), F32), V((8, hid, half), F32),
                V((2, hid, half), F32), V((4, hid, half), F32),
                V((frows, hid), F32), V((cpad, hid), F32), V((15, 16, hid), F32), V((cpad, hid // 2), F32),
                V((3, cpad // 2, hid // 2), F32), V((cpad, hid // 2), F32), V((2, cpad // 2, hid // 2), F32),
                V((frows, hid), F32), V((cpad, hid), F32),
                pltpu.SemaphoreType.DMA((9,)), pltpu.SemaphoreType.DMA((5,)),
                pltpu.SemaphoreType.DMA((nsend,)), pltpu.SemaphoreType.DMA((nrecv,)),
            ],
            compiler_params=pltpu.CompilerParams(collective_id=0, has_side_effects=True, vmem_limit_bytes=64 * 1000 * 1000),
            name="gcn_step",
        )(adj_rows, features.T, w_one, w_two.T, labels.reshape(1, nb), label_mask.reshape(1, nb))
        loss, dw1, dw2 = pl.pallas_call(
            output_kernel,
            out_shape=[jax.ShapeDtypeStruct((1, 1), F32), jax.ShapeDtypeStruct((f_in, hid), F32),
                       jax.ShapeDtypeStruct((classes, hid), F32)],
            name="outputs",
        )(*(pltpu.with_memory_space_constraint(v, pltpu.VMEM) for v in (dw1, dw2)))
        return loss.reshape(()), dw1, dw2.T

    row_spec = P(("nodes", "rep"))
    return jax.shard_map(local_step, mesh=mesh, in_specs=(P("nodes", None), P(("nodes", "rep"), None), P(), P(), row_spec, row_spec), out_specs=(P(), P(), P()), check_vma=False)
```
